128 devices in a mesh: data: 1, seq: 128 (over z, y, x, core).
Axes of the slice: x: 4, y: 4, z: 4, core: 2. Of those that a mesh axis runs over, the one named last changes fastest.
Arguments:
- dec_in: bfloat16 [4096, 384], P(('data', 'seq'))
- memory: bfloat16 [131072, 384], P(('data', 'seq'))
- mem_len: int32 [1], P('data')
- grad_out: float32 [4096, 384], P(('data', 'seq'))
- norm_attn: bfloat16 [384], replicated
- wq_cross: bfloat16 [384, 6, 64], replicated
- wk_cross: bfloat16 [384, 6, 64], replicated
- wv_cross: bfloat16 [384, 6, 64], replicated
- wo_cross: bfloat16 [6, 64, 384], replicated
- norm_mlp: bfloat16 [384], replicated
- w_gate: bfloat16 [384, 1536], replicated
- w_up: bfloat16 [384, 1536], replicated
- w_down: bfloat16 [1536, 384], replicated
Outputs:
- output 1: float32 [4096, 384], P(('data', 'seq'))
- output 2: float32 [131072, 384], P(('data', 'seq'))
- output 3: float32 [384], P('data')
- output 4: float32 [384, 6, 64], P('data')
- output 5: float32 [384, 6, 64], P('data')
- output 6: float32 [384, 6, 64], P('data')
- output 7: float32 [6, 64, 384], P('data')
- output 8: float32 [384], P('data')
- output 9: float32 [384, 1536], P('data')
- output 10: float32 [384, 1536], P('data')
- output 11: float32 [1536, 384], P('data')
All inputs are finite; a program needn't handle non-finite values.
Results may differ from the reference program's by a relative error of at most 0.0157402.
Values are sent between devices in bfloat16 or wider.
A program may use at most 1 GiB of HBM per device.

```python
import functools
import jax
import jax.numpy as jnp
from jax import lax

TQ = 4096
TM = 131072
D = 384
HEADS = 6
KV_HEADS = 6
HEAD = 64
FF = 1536
QBLK = 32
SEGMENTS = 16


def setup_inputs(seed: int = 0, part: int = 0) -> dict:
    part_keys = jax.random.split(jax.random.fold_in(jax.random.key(seed), part), 5)
    shared_keys = jax.random.split(jax.random.key(seed + 1), 11)
    inv_width = D ** -0.5

    def normal_draw(key, shape, spread):
        return spread * jax.random.normal(key, shape, jnp.float32)

    topics = normal_draw(part_keys[1], (SEGMENTS, D), 1.0)
    memory = normal_draw(part_keys[2], (TM, D), 0.6) + 0.8 * jnp.repeat(topics, TM // SEGMENTS, axis=0)
    quarter = TM // 4
    mem_len = jax.random.randint(part_keys[3], (1,), quarter, TM - quarter + 1, dtype=jnp.int32)
    return {
        'dec_in': normal_draw(part_keys[0], (TQ, D), 1.0).astype(jnp.bfloat16),
        'memory': memory.astype(jnp.bfloat16),
        'mem_len': mem_len,
        'grad_out': normal_draw(part_keys[4], (TQ, D), 1.0),
        'norm_attn': (1.0 + normal_draw(shared_keys[0], (D,), 0.3)).astype(jnp.bfloat16),
        'wq_cross': normal_draw(shared_keys[1], (D, HEADS, HEAD), 1.2 * inv_width).astype(jnp.bfloat16),
        'wk_cross': normal_draw(shared_keys[2], (D, KV_HEADS, HEAD), 1.2 * inv_width).astype(jnp.bfloat16),
        'wv_cross': normal_draw(shared_keys[3], (D, KV_HEADS, HEAD), inv_width).astype(jnp.bfloat16),
        'wo_cross': normal_draw(shared_keys[4], (HEADS, HEAD, D), 1.5 * inv_width).astype(jnp.bfloat16),
        'norm_mlp': (1.0 + normal_draw(shared_keys[5], (D,), 0.3)).astype(jnp.bfloat16),
        'w_gate': normal_draw(shared_keys[6], (D, FF), inv_width).astype(jnp.bfloat16),
        'w_up': normal_draw(shared_keys[7], (D, FF), inv_width).astype(jnp.bfloat16),
        'w_down': normal_draw(shared_keys[8], (FF, D), FF ** -0.5).astype(jnp.bfloat16),
    }


def to_bf16(tensor):
    return tensor + lax.stop_gradient(tensor.astype(jnp.bfloat16).astype(jnp.float32) - tensor)


def rms_norm(tensor, gain):
    mean_sq = jnp.mean(tensor * tensor, axis=-1, keepdims=True)
    return tensor * lax.rsqrt(mean_sq + 1e-6) * gain


def layer_forward(valid_mask, dec_in, memory, norm_attn, wq_cross, wk_cross, wv_cross, wo_cross, norm_mlp, w_gate, w_up, w_down):
    normed = to_bf16(rms_norm(dec_in, norm_attn))
    dec_query = to_bf16(jnp.einsum('td,dhe->the', normed, wq_cross))
    dec_query = dec_query.reshape(TQ // QBLK, QBLK, KV_HEADS, HEADS // KV_HEADS, HEAD)
    mem_keys = to_bf16(jnp.einsum('td,dke->tke', memory, wk_cross))
    mem_vals = to_bf16(jnp.einsum('td,dke->tke', memory, wv_cross))

    def block_attention(query_block):
        scores = jnp.einsum('qkge,tke->qkgt', query_block, mem_keys) * (HEAD ** -0.5)
        scores = jnp.where(valid_mask, scores, -1e30)
        attn_prob = jax.nn.softmax(scores, axis=-1)
        return jnp.einsum('qkgt,tke->qkge', attn_prob, mem_vals)

    attended = to_bf16(lax.map(jax.checkpoint(block_attention), dec_query).reshape(TQ, HEADS, HEAD))
    hidden = to_bf16(dec_in + jnp.einsum('the,hed->td', attended, wo_cross))
    normed_mlp = to_bf16(rms_norm(hidden, norm_mlp))
    gate_pre = jnp.dot(normed_mlp, w_gate, preferred_element_type=jnp.float32)
    up_pre = jnp.dot(normed_mlp, w_up, preferred_element_type=jnp.float32)
    mlp_act = to_bf16(jax.nn.silu(gate_pre) * up_pre)
    return hidden + jnp.dot(mlp_act, w_down, preferred_element_type=jnp.float32)


def reference(dec_in, memory, mem_len, grad_out, norm_attn, wq_cross, wk_cross, wv_cross, wo_cross, norm_mlp, w_gate, w_up, w_down):
    valid_mask = jnp.arange(TM) < mem_len[0]
    primals = [tensor.astype(jnp.float32) for tensor in (dec_in, memory, norm_attn, wq_cross, wk_cross, wv_cross, wo_cross, norm_mlp, w_gate, w_up, w_down)]
    _, pullback = jax.vjp(functools.partial(layer_forward, valid_mask), *primals)
    (g_dec, g_mem, g_norm_attn, g_wq, g_wk, g_wv, g_wo, g_norm_mlp, g_gate, g_up, g_down) = pullback(grad_out.astype(jnp.float32))
    return (g_dec, g_mem, g_norm_attn, g_wq, g_wk, g_wv, g_wo, g_norm_mlp, g_gate, g_up, g_down)
```

```python
import functools

import jax
import jax.numpy as jnp
from jax import lax
from jax.experimental import pallas as pl
from jax.experimental.pallas import tpu as pltpu
from jax.sharding import PartitionSpec as P

F32 = jnp.float32
BF16 = jnp.bfloat16
MESH = pl.DeviceIdType.MESH
VMEM_LIMIT = 62 * 1024 * 1024
NEG = -1e30
ORDERS = ((0, 1, 2), (2, 0, 1), (1, 2, 0))
PARTS = 3
TILE = 128


def rms_norm(tensor, gain):
    mean_sq = jnp.mean(tensor * tensor, axis=-1, keepdims=True)
    return tensor * lax.rsqrt(mean_sq + 1e-6) * gain


def gated_unit(gate_pre, up_pre):
    return jax.nn.silu(gate_pre) * up_pre


class Place:
    def __init__(self, n):
        self.n = n
        me = lax.axis_index("seq")
        self.me = me
        self.core = lax.rem(me, 2)
        x = lax.rem(me // 2, n)
        y = lax.rem(me // (2 * n), n)
        z = me // (2 * n * n)
        self.coord = (z, y, x)
        self.stride = (2 * n * n, 2 * n, 2)

    def along(self, axis, k):
        here = self.coord[axis]
        return self.me + (lax.rem(here + k, self.n) - here) * self.stride[axis]

    def other_core(self):
        return self.me + 1 - 2 * self.core

    def to(self, k):
        return {"seq": k}

    def barrier(self):
        sem = pltpu.get_barrier_semaphore()
        for axis in range(3):
            for k in range(1, self.n):
                pl.semaphore_signal(sem, inc=1, device_id=self.to(self.along(axis, k)), device_id_type=MESH)
        pl.semaphore_signal(sem, inc=1, device_id=self.to(self.other_core()), device_id_type=MESH)
        pl.semaphore_wait(sem, 3 * (self.n - 1) + 1)


def rcopy(src, dst, send, recv, device):
    return pltpu.make_async_remote_copy(src_ref=src, dst_ref=dst, send_sem=send, recv_sem=recv,
                                        device_id={"seq": device}, device_id_type=MESH)


def lanes(start, size):
    return pl.ds(pl.multiple_of(start, TILE), size)


def gather_kernel(n, has_stats, *refs):
    if has_stats:
        x_ref, s_ref, out_ref, sout_ref, rows, srows, send, recv, ssend, srecv, csend, crecv = refs
    else:
        x_ref, out_ref, rows, send, recv, csend, crecv = refs
    at = Place(n)
    r = TILE // n
    at.barrier()
    pairs = [(0, x_ref, rows, out_ref)]
    if has_stats:
        pairs.append((1, s_ref, srows, sout_ref))

    def sems(kind):
        return (send, recv) if kind == 0 else (ssend, srecv)

    copies = {}
    for p in range(PARTS):
        a3 = ORDERS[p][2]
        mine = pl.ds(pl.multiple_of(at.coord[a3] * r, r), r)
        for kind, src, dst, _ in pairs:
            snd, rcv = sems(kind)
            for k in range(1, n):
                c = rcopy(src.at[p], dst.at[p, mine, :], snd.at[0, p, k - 1], rcv.at[0, p, k - 1], at.along(a3, k))
                c.start()
                copies[0, p, kind, k] = c
            dst[p, mine, :] = src[p]
    for p in range(PARTS):
        a1, a2, _ = ORDERS[p]
        base = ((at.core * n + at.coord[a1]) * n + at.coord[a2]) * TILE
        for kind, _, dst, full in pairs:
            for k in range(1, n):
                copies[0, p, kind, k].wait()
            block = dst[p].astype(F32).T
            full[p, :, lanes(base, TILE)] = block[:full.shape[1]].astype(full.dtype)
    for stage in (1, 2):
        for p in range(PARTS):
            a1, a2, _ = ORDERS[p]
            if stage == 1:
                axis, width = a2, TILE
                base = ((at.core * n + at.coord[a1]) * n + at.coord[a2]) * TILE
            else:
                axis, width = a1, TILE * n
                base = (at.core * n + at.coord[a1]) * n * TILE
                for kind, *_ in pairs:
                    for k in range(1, n):
                        copies[1, p, kind, k].wait()
            for kind, _, _, full in pairs:
                snd, rcv = sems(kind)
                view = full.at[p, :, lanes(base, width)]
                for k in range(1, n):
                    c = rcopy(view, view, snd.at[stage, p, k - 1], rcv.at[stage, p, k - 1], at.along(axis, k))
                    c.start()
                    copies[stage, p, kind, k] = c
    final = []
    for p in range(PARTS):
        for kind, _, _, full in pairs:
            for k in range(1, n):
                copies[2, p, kind, k].wait()
            width = n * n * TILE
            view = full.at[p, :, lanes(at.core * width, width)]
            c = rcopy(view, view, csend.at[kind, p], crecv.at[kind, p], at.other_core())
            c.start()
            final.append(c)
    for c in final:
        c.wait()


def all_gather_t(n, cid, rows, stats=None):
    total = 2 * n * n * TILE
    r = TILE // n
    has = stats is not None
    vm = pl.BlockSpec(memory_space=pltpu.VMEM)
    outs = [jax.ShapeDtypeStruct((PARTS, TILE, total), BF16)]
    scratch = [pltpu.VMEM((PARTS, TILE, TILE), BF16)]
    args = [rows]
    sem = pltpu.SemaphoreType.DMA
    if has:
        outs.append(jax.ShapeDtypeStruct((PARTS, 8, total), F32))
        scratch.append(pltpu.VMEM((PARTS, TILE, TILE), F32))
        args.append(stats)
    scratch += [sem((3, PARTS, n - 1)), sem((3, PARTS, n - 1))]
    if has:
        scratch += [sem((3, PARTS, n - 1)), sem((3, PARTS, n - 1))]
    scratch += [sem((2, PARTS)), sem((2, PARTS))]
    res = pl.pallas_call(
        functools.partial(gather_kernel, n, has),
        out_shape=tuple(outs), in_specs=[vm] * len(args), out_specs=(vm,) * len(outs),
        scratch_shapes=scratch, name="gather_stats" if has else "gather_q",
        compiler_params=pltpu.CompilerParams(collective_id=cid, has_side_effects=True, vmem_limit_bytes=VMEM_LIMIT),
    )(*args)
    return res if has else res[0]


def merge(blocks, rows_axis):
    take = (lambda b, i, j: b[i:j]) if rows_axis == 0 else (lambda b, i, j: b[:, i:j])
    half = TILE // 2
    outs, maxes, sums = [], [], []
    for h in range(2):
        ms = [take(b, TILE + h, TILE + h + 1) for b in blocks]
        m = functools.reduce(jnp.maximum, ms)
        ws = [jnp.exp(v - m) for v in ms]
        o = sum(take(b, half * h, half * h + half) * w for b, w in zip(blocks, ws))
        l = sum(take(b, TILE + 2 + h, TILE + 3 + h) * w for b, w in zip(blocks, ws))
        outs.append(o)
        maxes.append(m)
        sums.append(l)
    return outs, maxes + sums


def scatter_kernel(n, with_stats, x_ref, *refs):
    if with_stats:
        o_ref, st_ref, buf0, acc0, buf1, acc1, buf2, acc2, buf3, csend, crecv, send, recv = refs
    else:
        o_ref, buf0, acc0, buf1, acc1, buf2, acc2, buf3, csend, crecv, send, recv = refs
    at = Place(n)
    r = TILE // n
    at.barrier()
    half = n * n * TILE

    def combine(dst, p, col, blocks):
        vals = blocks
        if with_stats:
            outs, stats = merge(vals, 0)
            dst[p, 0:TILE // 2, col] = outs[0]
            dst[p, TILE // 2:TILE, col] = outs[1]
            dst[p, TILE:TILE + 8, col] = jnp.concatenate(stats + [jnp.zeros_like(stats[0])] * 4, axis=0)
        else:
            dst[p, :, col] = functools.reduce(jnp.add, vals)

    first = []
    for p in range(PARTS):
        c = rcopy(x_ref.at[p, :, lanes((1 - at.core) * half, half)], buf0.at[p], csend.at[p], crecv.at[p], at.other_core())
        c.start()
        first.append(c)
    copies = {}
    for p in range(PARTS):
        a1 = ORDERS[p][0]
        first[p].wait()
        step = n * TILE
        for j in range(n):
            combine(acc0, p, pl.ds(j * step, step),
                    [x_ref[p, :, lanes(at.core * half + j * step, step)], buf0[p, :, j * step:(j + 1) * step]])
        for k in range(1, n):
            there = lax.rem(at.coord[a1] + k, n)
            c = rcopy(acc0.at[p, :, lanes(there * step, step)], buf1.at[p, k - 1],
                      send.at[0, p, k - 1], recv.at[0, p, k - 1], at.along(a1, k))
            c.start()
            copies[0, p, k] = c
    for p in range(PARTS):
        a1, a2, _ = ORDERS[p]
        for k in range(1, n):
            copies[0, p, k].wait()
        mine = at.coord[a1] * n * TILE
        for j in range(n):
            col = slice(j * TILE, (j + 1) * TILE)
            combine(acc1, p, pl.ds(j * TILE, TILE),
                    [acc0[p, :, lanes(mine + j * TILE, TILE)]] + [buf1[p, k, :, col] for k in range(n - 1)])
        for k in range(1, n):
            there = lax.rem(at.coord[a2] + k, n)
            c = rcopy(acc1.at[p, :, lanes(there * TILE, TILE)], buf2.at[p, k - 1],
                      send.at[1, p, k - 1], recv.at[1, p, k - 1], at.along(a2, k))
            c.start()
            copies[1, p, k] = c
    for p in range(PARTS):
        _, a2, a3 = ORDERS[p]
        for k in range(1, n):
            copies[1, p, k].wait()
        blocks = [acc1[p, :, lanes(at.coord[a2] * TILE, TILE)]] + [buf2[p, k] for k in range(n - 1)]
        if with_stats:
            outs, stats = merge(blocks, 0)
            acc2[p, :, 0:TILE] = jnp.concatenate(outs, axis=0).T
            tail = jnp.concatenate(stats + [jnp.zeros((TILE - 4, TILE), F32)], axis=0)
            acc2[p, :, TILE:2 * TILE] = tail.T
        else:
            acc2[p] = functools.reduce(jnp.add, blocks).T
        for k in range(1, n):
            there = lax.rem(at.coord[a3] + k, n)
            c = rcopy(acc2.at[p, pl.ds(pl.multiple_of(there * r, r), r), :], buf3.at[p, k - 1],
                      send.at[2, p, k - 1], recv.at[2, p, k - 1], at.along(a3, k))
            c.start()
            copies[2, p, k] = c
    for p in range(PARTS):
        a3 = ORDERS[p][2]
        for k in range(1, n):
            copies[2, p, k].wait()
        blocks = [acc2[p, pl.ds(pl.multiple_of(at.coord[a3] * r, r), r), :]] + [buf3[p, k] for k in range(n - 1)]
        if with_stats:
            outs, (m0, m1, l0, l1) = merge(blocks, 1)
            o_ref[p] = jnp.concatenate([outs[0] / l0, outs[1] / l1], axis=1)
            col = lax.broadcasted_iota(jnp.int32, (r, TILE), 1)
            st_ref[p] = jnp.where(col == 0, m0 + jnp.log(l0), jnp.where(col == 1, m1 + jnp.log(l1), 0.0))
        else:
            o_ref[p] = functools.reduce(jnp.add, blocks)


def reduce_scatter_t(n, cid, x, with_stats):
    rows = x.shape[1]
    r = TILE // n
    wide = 2 * TILE if with_stats else TILE
    vm = pl.BlockSpec(memory_space=pltpu.VMEM)
    sem = pltpu.SemaphoreType.DMA
    half = n * n * TILE
    outs = [jax.ShapeDtypeStruct((PARTS, r, TILE), F32)] * (2 if with_stats else 1)
    scratch = [
        pltpu.VMEM((PARTS, rows, half), F32), pltpu.VMEM((PARTS, rows, half), F32),
        pltpu.VMEM((PARTS, n - 1, rows, n * TILE), F32), pltpu.VMEM((PARTS, rows, n * TILE), F32),
        pltpu.VMEM((PARTS, n - 1, rows, TILE), F32), pltpu.VMEM((PARTS, TILE, wide), F32),
        pltpu.VMEM((PARTS, n - 1, r, wide), F32),
        sem((PARTS,)), sem((PARTS,)), sem((3, PARTS, n - 1)), sem((3, PARTS, n - 1)),
    ]
    res = pl.pallas_call(
        functools.partial(scatter_kernel, n, with_stats),
        out_shape=tuple(outs), in_specs=[vm], out_specs=(vm,) * len(outs), scratch_shapes=scratch,
        name="scatter_out" if with_stats else "scatter_dq",
        compiler_params=pltpu.CompilerParams(collective_id=cid, has_side_effects=True, vmem_limit_bytes=VMEM_LIMIT),
    )(x)
    return res if with_stats else res[0]


QB = 256


def aux_rows(rows, width):
    pad = jnp.zeros((64 - len(rows), width), F32)
    return jnp.concatenate(list(rows) + [pad], axis=0).astype(BF16)


def split3(v):
    hi = v.astype(BF16).astype(F32)
    mid = (v - hi).astype(BF16).astype(F32)
    lo = (v - hi - mid).astype(BF16).astype(F32)
    return [hi, mid, lo]


def fwd_kernel(q_ref, k_ref, vt_ref, o_ref):
    total = q_ref.shape[2]
    half = TILE // 2
    one = jnp.ones((1, QB), F32)
    aux = aux_rows([one], QB)

    def body(b, _):
        col = pl.ds(pl.multiple_of(b * QB, QB), QB)
        for p in range(PARTS):
            maxes, sums = [], []
            for j in range(2):
                qa = jnp.concatenate([q_ref[p, half * j:half * (j + 1), col], aux], axis=0)
                s = jnp.dot(k_ref[2 * p + j], qa, preferred_element_type=F32)
                m = jnp.max(s, axis=0, keepdims=True)
                e = jnp.exp(s - m)
                l = jnp.sum(e, axis=0, keepdims=True)
                o_ref[p, half * j:half * (j + 1), col] = jnp.dot(
                    vt_ref[p, half * j:half * (j + 1), :], e.astype(BF16), preferred_element_type=F32)
                maxes.append(m)
                sums.append(l)
            o_ref[p, TILE:TILE + 8, col] = jnp.concatenate(maxes + sums + [jnp.zeros((4, QB), F32)], axis=0)
        return 0

    lax.fori_loop(0, total // QB, body, 0)


def attention_fwd(q_t, k_aug, v_t):
    total, keys = q_t.shape[2], k_aug.shape[1]
    vm = pl.BlockSpec(memory_space=pltpu.VMEM)
    return pl.pallas_call(
        fwd_kernel, out_shape=jax.ShapeDtypeStruct((PARTS, TILE + 8, total), F32),
        in_specs=[vm] * 3, out_specs=vm, name="attention_fwd",
        cost_estimate=pl.CostEstimate(flops=4 * 384 * total * keys, bytes_accessed=12_000_000, transcendentals=6 * total * keys),
        compiler_params=pltpu.CompilerParams(vmem_limit_bytes=VMEM_LIMIT),
    )(q_t, k_aug, v_t)


def bwd_kernel(q_ref, do_ref, st_ref, k_ref, v_ref, kt_ref, dq_ref, dk_ref, dv_ref):
    total = q_ref.shape[2]
    half = TILE // 2
    one = jnp.ones((1, QB), F32)
    zero = jnp.zeros((1, QB), F32)
    blank = jnp.zeros((half, QB), BF16)
    nt = (((1,), (1,)), ((), ()))
    dk_ref[...] = jnp.zeros_like(dk_ref)
    dv_ref[...] = jnp.zeros_like(dv_ref)

    def body(b, _):
        col = pl.ds(pl.multiple_of(b * QB, QB), QB)
        for p in range(PARTS):
            probs, dscores, dos, qs = [], [], [], []
            for j in range(2):
                qh = q_ref[p, half * j:half * (j + 1), col]
                doh = do_ref[p, half * j:half * (j + 1), col]
                lse = st_ref[p, j:j + 1, col]
                delta = st_ref[p, 2 + j:3 + j, col]
                qa = jnp.concatenate([qh, aux_rows([one] + split3(-lse), QB)], axis=0)
                da = jnp.concatenate([doh, aux_rows([zero] + split3(-delta), QB)], axis=0)
                e = jnp.exp(jnp.dot(k_ref[2 * p + j], qa, preferred_element_type=F32))
                dp = jnp.dot(v_ref[2 * p + j], da, preferred_element_type=F32)
                ds = (e * dp).astype(BF16)
                probs.append(e.astype(BF16))
                dscores.append(ds)
                order = (lambda a: [a, blank]) if j == 0 else (lambda a: [blank, a])
                dos.append(jnp.concatenate(order(doh), axis=0))
                qs.append(jnp.concatenate(order(qh), axis=0))
                dq_ref[p, half * j:half * (j + 1), col] = 0.125 * jnp.dot(
                    kt_ref[p, half * j:half * (j + 1), :], ds, preferred_element_type=F32)
            dv_ref[p] += (lax.dot_general(probs[0], dos[0], nt, preferred_element_type=F32)
                          + lax.dot_general(probs[1], dos[1], nt, preferred_element_type=F32))
            dk_ref[p] += (lax.dot_general(dscores[0], qs[0], nt, preferred_element_type=F32)
                          + lax.dot_general(dscores[1], qs[1], nt, preferred_element_type=F32))
        return 0

    lax.fori_loop(0, total // QB, body, 0)


def attention_bwd(q_t, do_t, stats, k_aug, v_aug, k_t):
    total, keys = q_t.shape[2], k_aug.shape[1]
    vm = pl.BlockSpec(memory_space=pltpu.VMEM)
    acc = jax.ShapeDtypeStruct((PARTS, keys, TILE), F32)
    return pl.pallas_call(
        bwd_kernel, out_shape=(jax.ShapeDtypeStruct((PARTS, TILE, total), F32), acc, acc),
        in_specs=[vm] * 6, out_specs=(vm,) * 3, name="attention_bwd",
        cost_estimate=pl.CostEstimate(flops=10 * 384 * total * keys, bytes_accessed=20_000_000, transcendentals=6 * total * keys),
        compiler_params=pltpu.CompilerParams(vmem_limit_bytes=VMEM_LIMIT),
    )(q_t, do_t, stats, k_aug, v_aug, k_t)


def solution(mesh):
    group = mesh.shape['seq']
    n = round((group // 2) ** (1 / 3))
    row_spec = P(('data', 'seq'), None)
    weight_spec = P()
    part_vec = P('data')
    part_mat = P('data', None)
    part_cube = P('data', None, None)

    def by_part(a):
        return jnp.transpose(a.reshape(a.shape[0], PARTS, TILE), (1, 0, 2))

    def by_row(a):
        return jnp.transpose(a, (1, 0, 2)).reshape(a.shape[1], PARTS * TILE)

    def device_step(dec_in, memory, mem_len, grad_out, norm_attn, wq_cross, wk_cross, wv_cross, wo_cross, norm_mlp, w_gate, w_up, w_down):
        q_rows, model_dim = dec_in.shape
        m_rows = memory.shape[0]
        heads, head_dim = wq_cross.shape[1], wq_cross.shape[2]
        wide = heads * head_dim
        wq, wk, wv = (w.reshape(model_dim, wide) for w in (wq_cross, wk_cross, wv_cross))
        wo = wo_cross.reshape(wide, model_dim)
        mem_pos = lax.axis_index('seq') * m_rows + jnp.arange(m_rows)
        bias = jnp.where(mem_pos < mem_len[0], 0.0, NEG).astype(BF16)

        x_in = dec_in.astype(F32)
        normed_f, norm_pull = jax.vjp(rms_norm, x_in, norm_attn.astype(F32))
        normed = normed_f.astype(BF16)
        local_query = jnp.dot(normed, wq, preferred_element_type=F32).astype(BF16) * jnp.asarray(head_dim ** -0.5, BF16)
        q_t = all_gather_t(n, 0, by_part(local_query))

        mem_keys = jnp.dot(memory, wk, preferred_element_type=F32).astype(BF16)
        mem_vals = jnp.dot(memory, wv, preferred_element_type=F32).astype(BF16)
        k_t = mem_keys.T.reshape(PARTS, TILE, m_rows)
        v_t = mem_vals.T.reshape(PARTS, TILE, m_rows)
        ones = jnp.ones((m_rows, 3), BF16)
        aux_k = jnp.concatenate([bias[:, None], ones, jnp.zeros((m_rows, 60), BF16)], axis=1)
        aux_v = jnp.concatenate([jnp.zeros((m_rows, 1), BF16), ones, jnp.zeros((m_rows, 60), BF16)], axis=1)

        def augment(a, aux):
            return jnp.stack([jnp.concatenate([a[:, head_dim * h:head_dim * (h + 1)], aux], axis=1) for h in range(heads)])

        k_aug = augment(mem_keys, aux_k)
        v_aug = augment(mem_vals, aux_v)

        partial = attention_fwd(q_t, k_aug, v_t)
        out_parts, lse = reduce_scatter_t(n, 1, partial, True)
        attended_f = by_row(out_parts)

        attended = attended_f.astype(BF16)
        hidden_f = x_in + jnp.dot(attended, wo, preferred_element_type=F32)
        hidden = hidden_f.astype(BF16)
        normed_mlp_f, mlp_norm_pull = jax.vjp(rms_norm, hidden.astype(F32), norm_mlp.astype(F32))
        normed_mlp = normed_mlp_f.astype(BF16)
        gate_pre = jnp.dot(normed_mlp, w_gate, preferred_element_type=F32)
        up_pre = jnp.dot(normed_mlp, w_up, preferred_element_type=F32)
        mlp_f, gated_pull = jax.vjp(gated_unit, gate_pre, up_pre)
        mlp_act = mlp_f.astype(BF16)

        grad_top = grad_out.astype(BF16)
        g_down = jnp.einsum('qf,qd->fd', mlp_act, grad_top, preferred_element_type=F32)
        grad_act = jnp.einsum('qd,fd->qf', grad_top, w_down, preferred_element_type=F32)
        grad_gate, grad_up = gated_pull(grad_act)
        grad_gate_b = grad_gate.astype(BF16)
        grad_up_b = grad_up.astype(BF16)
        g_gate = jnp.einsum('qd,qf->df', normed_mlp, grad_gate_b, preferred_element_type=F32)
        g_up = jnp.einsum('qd,qf->df', normed_mlp, grad_up_b, preferred_element_type=F32)
        grad_normed_mlp = (jnp.einsum('qf,df->qd', grad_gate_b, w_gate, preferred_element_type=F32)
                           + jnp.einsum('qf,df->qd', grad_up_b, w_up, preferred_element_type=F32))
        grad_hidden_norm, g_norm_mlp = mlp_norm_pull(grad_normed_mlp)
        grad_hidden = grad_out + grad_hidden_norm
        grad_hidden_b = grad_hidden.astype(BF16)
        g_wo = jnp.einsum('qe,qd->ed', attended, grad_hidden_b, preferred_element_type=F32).reshape(heads, head_dim, model_dim)
        grad_attended = jnp.einsum('qd,ed->qe', grad_hidden_b, wo, preferred_element_type=F32)
        delta = jnp.sum((grad_attended * attended_f).reshape(q_rows, PARTS, 2, head_dim), axis=-1)
        delta = jnp.transpose(delta, (1, 0, 2))
        stats_in = jnp.concatenate([lse[:, :, 0:2], delta, jnp.zeros((PARTS, q_rows, TILE - 4), F32)], axis=2)
        do_t, stats = all_gather_t(n, 2, by_part(grad_attended.astype(BF16)), stats_in)

        early = lax.psum((g_wo, g_norm_mlp, g_gate, g_up, g_down), 'seq')

        dq_part, dk, dv = attention_bwd(q_t, do_t, stats, k_aug, v_aug, k_t)
        grad_query_b = by_row(reduce_scatter_t(n, 3, dq_part, False)).astype(BF16)

        g_wq = jnp.einsum('td,te->de', normed, grad_query_b, preferred_element_type=F32)
        grad_normed = jnp.einsum('te,de->td', grad_query_b, wq, preferred_element_type=F32)
        grad_x_norm, g_norm_attn = norm_pull(grad_normed)
        g_dec = grad_hidden + grad_x_norm
        dk_b = by_row(dk.astype(BF16))
        dv_b = by_row(dv.astype(BF16))
        g_wk = jnp.einsum('td,te->de', memory, dk_b, preferred_element_type=F32)
        g_wv = jnp.einsum('td,te->de', memory, dv_b, preferred_element_type=F32)
        g_mem = (jnp.einsum('te,de->td', dk_b, wk, preferred_element_type=F32)
                 + jnp.einsum('te,de->td', dv_b, wv, preferred_element_type=F32))
        late = lax.psum((g_norm_attn, g_wq, g_wk, g_wv), 'seq')
        cube = (model_dim, heads, head_dim)
        g_wo, g_norm_mlp, g_gate, g_up, g_down = early
        g_norm_attn, g_wq, g_wk, g_wv = late
        return (g_dec, g_mem, g_norm_attn, g_wq.reshape(cube), g_wk.reshape(cube), g_wv.reshape(cube),
                g_wo, g_norm_mlp, g_gate, g_up, g_down)

    return jax.shard_map(device_step, mesh=mesh,
                         in_specs=(row_spec, row_spec, part_vec, row_spec) + (weight_spec,) * 9,
                         out_specs=(row_spec, row_spec, part_vec, part_cube, part_cube, part_cube, part_cube, part_vec, part_mat, part_mat, part_mat),
                         check_vma=False)
```

```python
import functools

import jax
import jax.numpy as jnp
from jax import lax
from jax.experimental import pallas as pl
from jax.experimental.pallas import tpu as pltpu
from jax.sharding import PartitionSpec as P

F32 = jnp.float32
BF16 = jnp.bfloat16
MESH = pl.DeviceIdType.MESH
VMEM_LIMIT = 62 * 1024 * 1024
NEG = -1e30
ORDERS = ((0, 1, 2), (2, 0, 1), (1, 2, 0))
PARTS = 3
TILE = 128


def rms_norm(tensor, gain):
    mean_sq = jnp.mean(tensor * tensor, axis=-1, keepdims=True)
    return tensor * lax.rsqrt(mean_sq + 1e-6) * gain


def gated_unit(gate_pre, up_pre):
    return jax.nn.silu(gate_pre) * up_pre


class Place:
    def __init__(self, n):
        self.n = n
        me = lax.axis_index("seq")
        self.me = me
        self.core = lax.rem(me, 2)
        x = lax.rem(me // 2, n)
        y = lax.rem(me // (2 * n), n)
        z = me // (2 * n * n)
        self.coord = (z, y, x)
        self.stride = (2 * n * n, 2 * n, 2)

    def along(self, axis, k):
        here = self.coord[axis]
        return self.me + (lax.rem(here + k, self.n) - here) * self.stride[axis]

    def other_core(self):
        return self.me + 1 - 2 * self.core

    def to(self, k):
        return {"seq": k}

    def barrier(self):
        sem = pltpu.get_barrier_semaphore()
        for axis in range(3):
            for k in range(1, self.n):
                pl.semaphore_signal(sem, inc=1, device_id=self.to(self.along(axis, k)), device_id_type=MESH)
        pl.semaphore_signal(sem, inc=1, device_id=self.to(self.other_core()), device_id_type=MESH)
        pl.semaphore_wait(sem, 3 * (self.n - 1) + 1)


def rcopy(src, dst, send, recv, device):
    return pltpu.make_async_remote_copy(src_ref=src, dst_ref=dst, send_sem=send, recv_sem=recv,
                                        device_id={"seq": device}, device_id_type=MESH)


def lanes(start, size):
    return pl.ds(pl.multiple_of(start, TILE), size)


def gather_kernel(n, has_stats, *refs):
    if has_stats:
        x_ref, s_ref, out_ref, sout_ref, rows, srows, send, recv, ssend, srecv, csend, crecv = refs
    else:
        x_ref, out_ref, rows, send, recv, csend, crecv = refs
    at = Place(n)
    r = TILE // n
    at.barrier()
    pairs = [(0, x_ref, rows, out_ref)]
    if has_stats:
        pairs.append((1, s_ref, srows, sout_ref))

    def sems(kind):
        return (send, recv) if kind == 0 else (ssend, srecv)

    copies = {}
    for p in range(PARTS):
        a3 = ORDERS[p][2]
        mine = pl.ds(pl.multiple_of(at.coord[a3] * r, r), r)
        for kind, src, dst, _ in pairs:
            snd, rcv = sems(kind)
            for k in range(1, n):
                c = rcopy(src.at[p], dst.at[p, mine, :], snd.at[0, p, k - 1], rcv.at[0, p, k - 1], at.along(a3, k))
                c.start()
                copies[0, p, kind, k] = c
            dst[p, mine, :] = src[p]
    for p in range(PARTS):
        a1, a2, _ = ORDERS[p]
        base = ((at.core * n + at.coord[a1]) * n + at.coord[a2]) * TILE
        for kind, _, dst, full in pairs:
            for k in range(1, n):
                copies[0, p, kind, k].wait()
            block = dst[p].astype(F32).T
            full[p, :, lanes(base, TILE)] = block[:full.shape[1]].astype(full.dtype)
    for stage in (1, 2):
        for p in range(PARTS):
            a1, a2, _ = ORDERS[p]
            if stage == 1:
                axis, width = a2, TILE
                base = ((at.core * n + at.coord[a1]) * n + at.coord[a2]) * TILE
            else:
                axis, width = a1, TILE * n
                base = (at.core * n + at.coord[a1]) * n * TILE
                for kind, *_ in pairs:
                    for k in range(1, n):
                        copies[1, p, kind, k].wait()
            for kind, _, _, full in pairs:
                snd, rcv = sems(kind)
                view = full.at[p, :, lanes(base, width)]
                for k in range(1, n):
                    c = rcopy(view, view, snd.at[stage, p, k - 1], rcv.at[stage, p, k - 1], at.along(axis, k))
                    c.start()
                    copies[stage, p, kind, k] = c
    final = []
    for p in range(PARTS):
        for kind, _, _, full in pairs:
            for k in range(1, n):
                copies[2, p, kind, k].wait()
            width = n * n * TILE
            view = full.at[p, :, lanes(at.core * width, width)]
            c = rcopy(view, view, csend.at[kind, p], crecv.at[kind, p], at.other_core())
            c.start()
            final.append(c)
    for c in final:
        c.wait()


def all_gather_t(n, cid, rows, stats=None):
    total = 2 * n * n * TILE
    r = TILE // n
    has = stats is not None
    vm = pl.BlockSpec(memory_space=pltpu.VMEM)
    outs = [jax.ShapeDtypeStruct((PARTS, TILE, total), BF16)]
    scratch = [pltpu.VMEM((PARTS, TILE, TILE), BF16)]
    args = [rows]
    sem = pltpu.SemaphoreType.DMA
    if has:
        outs.append(jax.ShapeDtypeStruct((PARTS, 8, total), F32))
        scratch.append(pltpu.VMEM((PARTS, TILE, TILE), F32))
        args.append(stats)
    scratch += [sem((3, PARTS, n - 1)), sem((3, PARTS, n - 1))]
    if has:
        scratch += [sem((3, PARTS, n - 1)), sem((3, PARTS, n - 1))]
    scratch += [sem((2, PARTS)), sem((2, PARTS))]
    res = pl.pallas_call(
        functools.partial(gather_kernel, n, has),
        out_shape=tuple(outs), in_specs=[vm] * len(args), out_specs=(vm,) * len(outs),
        scratch_shapes=scratch, name="gather_stats" if has else "gather_q",
        compiler_params=pltpu.CompilerParams(collective_id=cid, has_side_effects=True, vmem_limit_bytes=VMEM_LIMIT),
    )(*args)
    return res if has else res[0]


def merge(blocks, rows_axis):
    take = (lambda b, i, j: b[i:j]) if rows_axis == 0 else (lambda b, i, j: b[:, i:j])
    half = TILE // 2
    outs, maxes, sums = [], [], []
    for h in range(2):
        ms = [take(b, TILE + h, TILE + h + 1) for b in blocks]
        m = functools.reduce(jnp.maximum, ms)
        ws = [jnp.exp(v - m) for v in ms]
        o = sum(take(b, half * h, half * h + half) * w for b, w in zip(blocks, ws))
        l = sum(take(b, TILE + 2 + h, TILE + 3 + h) * w for b, w in zip(blocks, ws))
        outs.append(o)
        maxes.append(m)
        sums.append(l)
    return outs, maxes + sums


class Scatter:
    def __init__(self, n, at, with_stats, bufs):
        self.n, self.at, self.with_stats = n, at, with_stats
        (self.far, self.near, self.buf0, self.buf1, self.acc1, self.buf2, self.acc2, self.buf3,
         self.csend, self.crecv, self.send, self.recv) = bufs
        self.step = n * TILE

    @staticmethod
    def scratch(n, rows, wide):
        sem = pltpu.SemaphoreType.DMA
        half = n * n * TILE
        r = TILE // n
        return [
            pltpu.VMEM((PARTS, rows, half), F32), pltpu.VMEM((PARTS, rows, half), F32), pltpu.VMEM((PARTS, rows, half), F32),
            pltpu.VMEM((PARTS, n - 1, rows, n * TILE), F32), pltpu.VMEM((PARTS, rows, n * TILE), F32),
            pltpu.VMEM((PARTS, n - 1, rows, TILE), F32), pltpu.VMEM((PARTS, TILE, wide), F32),
            pltpu.VMEM((PARTS, n - 1, r, wide), F32),
            sem((PARTS, n)), sem((PARTS, n)), sem((3, PARTS, n - 1)), sem((3, PARTS, n - 1)),
        ]

    def chunk(self, p, k):
        return lax.rem(self.at.coord[ORDERS[p][0]] + k, self.n)

    def combine(self, dst, p, col, vals):
        if self.with_stats:
            outs, stats = merge(vals, 0)
            dst[p, 0:TILE // 2, col] = outs[0]
            dst[p, TILE // 2:TILE, col] = outs[1]
            dst[p, TILE:TILE + 8, col] = jnp.concatenate(stats + [jnp.zeros_like(stats[0])] * 4, axis=0)
        else:
            dst[p, :, col] = functools.reduce(jnp.add, vals)

    def core_copy(self, p, k):
        view = (p, slice(None), lanes(self.chunk(p, k) * self.step, self.step))
        return rcopy(self.far.at[view], self.buf0.at[view], self.csend.at[p, k], self.crecv.at[p, k], self.at.other_core())

    def first_copy(self, p, k):
        return rcopy(self.near.at[p, :, lanes(self.chunk(p, k) * self.step, self.step)], self.buf1.at[p, k - 1],
                     self.send.at[0, p, k - 1], self.recv.at[0, p, k - 1], self.at.along(ORDERS[p][0], k))

    def far_done(self, k):
        for p in range(PARTS):
            self.core_copy(p, k).start()

    def near_done(self, k):
        for p in range(PARTS):
            self.core_copy(p, k).wait()

            def fold(j, _, p=p):
                col = lanes(self.chunk(p, k) * self.step + j * TILE, TILE)
                self.combine(self.near, p, col, [self.near[p, :, col], self.buf0[p, :, col]])
                return 0

            lax.fori_loop(0, self.n, fold, 0)

            @pl.when(k > 0)
            def _(p=p):
                self.first_copy(p, k).start()

    def finish(self, o_ref, st_ref=None):
        n, at = self.n, self.at
        r = TILE // n
        copies = {}
        for p in range(PARTS):
            a1, a2, _ = ORDERS[p]
            for k in range(1, n):
                self.first_copy(p, k).wait()
            mine = at.coord[a1] * n * TILE
            for j in range(n):
                col = slice(j * TILE, (j + 1) * TILE)
                self.combine(self.acc1, p, pl.ds(j * TILE, TILE),
                             [self.near[p, :, lanes(mine + j * TILE, TILE)]] + [self.buf1[p, k, :, col] for k in range(n - 1)])
            for k in range(1, n):
                there = lax.rem(at.coord[a2] + k, n)
                c = rcopy(self.acc1.at[p, :, lanes(there * TILE, TILE)], self.buf2.at[p, k - 1],
                          self.send.at[1, p, k - 1], self.recv.at[1, p, k - 1], at.along(a2, k))
                c.start()
                copies[1, p, k] = c
        for p in range(PARTS):
            _, a2, a3 = ORDERS[p]
            for k in range(1, n):
                copies[1, p, k].wait()
            blocks = [self.acc1[p, :, lanes(at.coord[a2] * TILE, TILE)]] + [self.buf2[p, k] for k in range(n - 1)]
            if self.with_stats:
                outs, stats = merge(blocks, 0)
                self.acc2[p, :, 0:TILE] = jnp.concatenate(outs, axis=0).T
                tail = jnp.concatenate(stats + [jnp.zeros((TILE - 4, TILE), F32)], axis=0)
                self.acc2[p, :, TILE:2 * TILE] = tail.T
            else:
                self.acc2[p] = functools.reduce(jnp.add, blocks).T
            for k in range(1, n):
                there = lax.rem(at.coord[a3] + k, n)
                c = rcopy(self.acc2.at[p, pl.ds(pl.multiple_of(there * r, r), r), :], self.buf3.at[p, k - 1],
                          self.send.at[2, p, k - 1], self.recv.at[2, p, k - 1], at.along(a3, k))
                c.start()
                copies[2, p, k] = c
        for p in range(PARTS):
            a3 = ORDERS[p][2]
            for k in range(1, n):
                copies[2, p, k].wait()
            blocks = [self.acc2[p, pl.ds(pl.multiple_of(at.coord[a3] * r, r), r), :]] + [self.buf3[p, k] for k in range(n - 1)]
            if self.with_stats:
                outs, (m0, m1, l0, l1) = merge(blocks, 1)
                o_ref[p] = jnp.concatenate([outs[0] / l0, outs[1] / l1], axis=1)
                col = lax.broadcasted_iota(jnp.int32, (r, TILE), 1)
                st_ref[p] = jnp.where(col == 0, m0 + jnp.log(l0), jnp.where(col == 1, m1 + jnp.log(l1), 0.0))
            else:
                o_ref[p] = functools.reduce(jnp.add, blocks)


def rows_of(start, size):
    return pl.ds(pl.multiple_of(start, 8), size)


class Wide:
    def __init__(self, shape, n):
        self.part, self.cols = shape[0] // PARTS, shape[1]
        self.r1, self.r2, self.c3 = self.part // 2, self.part // 2 // n, shape[1] // n
        self.l1, self.l2, self.l3 = (self.r1, self.cols), (self.r2, self.cols), (self.r2, self.c3)

    def full1(self, p, c):
        return rows_of(self.part * p + self.r1 * c, self.r1), slice(None)

    def full2(self, p, c, a):
        return rows_of(self.part * p + self.r1 * c + self.r2 * a, self.r2), slice(None)

    def full3(self, p, c, a, b):
        return rows_of(self.part * p + self.r1 * c + self.r2 * a, self.r2), lanes(self.c3 * b, self.c3)

    def in1(self, a):
        return rows_of(self.r2 * a, self.r2), slice(None)

    def in2(self, b):
        return slice(None), lanes(self.c3 * b, self.c3)


class Tall(Wide):
    def __init__(self, shape, n):
        super().__init__(shape, n)
        self.r3 = self.r2 // n
        self.l3 = (self.r3, self.cols)

    def full3(self, p, c, a, b):
        return rows_of(self.part * p + self.r1 * c + self.r2 * a + self.r3 * b, self.r3), slice(None)

    def in2(self, b):
        return rows_of(self.r3 * b, self.r3), slice(None)


class Stack:
    def __init__(self, shape, n):
        w, rows, cols = shape
        self.part, self.w3 = rows // PARTS, w // n
        self.r1, self.r2 = self.part // 2, self.part // 2 // n
        self.l1, self.l2, self.l3 = (w, self.r1, cols), (w, self.r2, cols), (self.w3, self.r2, cols)

    def full1(self, p, c):
        return slice(None), rows_of(self.part * p + self.r1 * c, self.r1), slice(None)

    def full2(self, p, c, a):
        return slice(None), rows_of(self.part * p + self.r1 * c + self.r2 * a, self.r2), slice(None)

    def full3(self, p, c, a, b):
        return pl.ds(self.w3 * b, self.w3), rows_of(self.part * p + self.r1 * c + self.r2 * a, self.r2), slice(None)

    def in1(self, a):
        return slice(None), rows_of(self.r2 * a, self.r2), slice(None)

    def in2(self, b):
        return pl.ds(self.w3 * b, self.w3), slice(None), slice(None)


REDUCE_REFS = 15


class Reduce:
    def __init__(self, n, at, form, src, out, bufs):
        self.n, self.at, self.form, self.src, self.out = n, at, form, src, out
        (self.own, self.buf0, self.buf1, self.acc1, self.buf2, self.buf3, self.lsem,
         self.csend, self.crecv, self.send, self.recv, self.gsend, self.grecv, self.dsend, self.drecv) = bufs

    @staticmethod
    def scratch(n, form):
        sem = pltpu.SemaphoreType.DMA
        return [
            pltpu.VMEM((PARTS,) + form.l1, F32), pltpu.VMEM((PARTS,) + form.l1, F32),
            pltpu.VMEM((PARTS, n - 1) + form.l2, F32), pltpu.VMEM((PARTS,) + form.l2, F32),
            pltpu.VMEM((PARTS, n - 1) + form.l3, F32), pltpu.VMEM((PARTS, n) + form.l3, F32),
            sem((PARTS,)), sem((PARTS,)), sem((PARTS,)), sem((3, PARTS, n - 1)), sem((3, PARTS, n - 1)),
            sem((2, PARTS, n - 1)), sem((2, PARTS, n - 1)), sem((PARTS,)), sem((PARTS,)),
        ]

    def spots(self, p):
        a1, a2, a3 = ORDERS[p]
        at = self.at
        return at.coord[a1], at.coord[a2], at.coord[a3]

    def copies(self, stage, p):
        at, n, form = self.at, self.n, self.form
        A1, A2, A3 = self.spots(p)
        a1, a2, a3 = ORDERS[p]
        c = at.core
        if stage == 0:
            return [rcopy(self.src.at[form.full1(p, 1 - c)], self.buf0.at[p], self.csend.at[p], self.crecv.at[p], at.other_core()),
                    pltpu.make_async_copy(self.src.at[form.full1(p, c)], self.own.at[p], self.lsem.at[p])]
        out = []
        if stage == 6:
            view = self.out.at[form.full1(p, c)]
            return [rcopy(view, view, self.dsend.at[p], self.drecv.at[p], at.other_core())]
        for k in range(1, n):
            if stage == 1:
                args = (self.own.at[p].at[form.in1(lax.rem(A1 + k, n))], self.buf1.at[p, k - 1], self.send.at[0, p, k - 1], self.recv.at[0, p, k - 1], at.along(a1, k))
            elif stage == 2:
                args = (self.acc1.at[p].at[form.in2(lax.rem(A2 + k, n))], self.buf2.at[p, k - 1], self.send.at[1, p, k - 1], self.recv.at[1, p, k - 1], at.along(a2, k))
            elif stage == 3:
                args = (self.buf3.at[p, A3], self.buf3.at[p, A3], self.send.at[2, p, k - 1], self.recv.at[2, p, k - 1], at.along(a3, k))
            elif stage == 4:
                view = self.out.at[form.full3(p, c, A1, A2)]
                args = (view, view, self.gsend.at[0, p, k - 1], self.grecv.at[0, p, k - 1], at.along(a2, k))
            else:
                view = self.out.at[form.full2(p, c, A1)]
                args = (view, view, self.gsend.at[1, p, k - 1], self.grecv.at[1, p, k - 1], at.along(a1, k))
            out.append(rcopy(*args))
        return out

    def advance(self, stage):
        form, n = self.form, self.n
        for p in range(PARTS):
            A1, A2, A3 = self.spots(p)
            if stage > 0:
                for c in self.copies(stage - 1, p):
                    c.wait()
            if stage == 1:
                self.own[p] = self.own[p] + self.buf0[p]
            elif stage == 2:
                self.acc1[p] = functools.reduce(jnp.add, [self.own[(p,) + form.in1(A1)]] + [self.buf1[p, k] for k in range(n - 1)])
            elif stage == 3:
                self.buf3[p, A3] = functools.reduce(jnp.add, [self.acc1[(p,) + form.in2(A2)]] + [self.buf2[p, k] for k in range(n - 1)])
            elif stage == 4:
                self.out[form.full3(p, self.at.core, A1, A2)] = functools.reduce(jnp.add, [self.buf3[p, k] for k in range(n)])
            if stage < 7:
                for c in self.copies(stage, p):
                    c.start()


QB = 256


def aux_rows(rows, width):
    pad = jnp.zeros((64 - len(rows), width), F32)
    return jnp.concatenate(list(rows) + [pad], axis=0).astype(BF16)


def split3(v):
    hi = v.astype(BF16).astype(F32)
    mid = (v - hi).astype(BF16).astype(F32)
    lo = (v - hi - mid).astype(BF16).astype(F32)
    return [hi, mid, lo]


def fold_rows(op, v, last):
    while v.shape[0] > 64:
        h = v.shape[0] // 2
        v = op(v[:h], v[h:])
    return last(v, axis=0, keepdims=True)


def blocks_loop(n, scatter, block, events):
    per = n * TILE // QB
    at = scatter.at

    def body(t, _):
        u = t // per
        k = n - 1 - u // 2
        near = lax.rem(u, 2)
        half = jnp.where(near == 1, at.core, 1 - at.core)
        for p in range(PARTS):
            inside = scatter.chunk(p, k) * (n * TILE) + lax.rem(t, per) * QB
            src = pl.multiple_of(half * (n * n * TILE) + inside, QB)
            block(p, pl.ds(src, QB), near, pl.ds(pl.multiple_of(inside, QB), QB))
        last = lax.rem(t, per) == per - 1

        @pl.when(last & (near == 0))
        def _():
            scatter.far_done(k)

        @pl.when(last & (near == 1))
        def _():
            scatter.near_done(k)

        for when, action in events:
            @pl.when(t == when)
            def _(action=action):
                action()
        return 0

    lax.fori_loop(0, 2 * n * per, body, 0)


def put(scatter, near, p, row, col, val):
    @pl.when(near == 1)
    def _():
        scatter.near[p, row, col] = val

    @pl.when(near == 0)
    def _():
        scatter.far[p, row, col] = val


def fwd_kernel(n, q_ref, k_ref, vt_ref, o_ref, st_ref, *bufs):
    half = TILE // 2
    one = jnp.ones((1, QB), F32)
    aux = aux_rows([one], QB)
    at = Place(n)
    at.barrier()
    scatter = Scatter(n, at, True, bufs)

    def block(p, src, near, dst):
        maxes, sums, outs = [], [], []
        for j in range(2):
            qa = jnp.concatenate([q_ref[p, half * j:half * (j + 1), src], aux], axis=0)
            s = jnp.dot(k_ref[2 * p + j], qa, preferred_element_type=F32)
            m = fold_rows(jnp.maximum, s, jnp.max)
            e = jnp.exp(s - m)
            sums.append(fold_rows(jnp.add, e, jnp.sum))
            outs.append(jnp.dot(vt_ref[p, half * j:half * (j + 1), :], e.astype(BF16), preferred_element_type=F32))
            maxes.append(m)
        val = jnp.concatenate(outs + maxes + sums + [jnp.zeros((4, QB), F32)], axis=0)
        put(scatter, near, p, slice(None), dst, val)

    blocks_loop(n, scatter, block, [])
    scatter.finish(o_ref, st_ref)


def attention_fwd(n, cid, q_t, k_aug, v_t):
    total, keys = q_t.shape[2], k_aug.shape[1]
    r = TILE // n
    vm = pl.BlockSpec(memory_space=pltpu.VMEM)
    return pl.pallas_call(
        functools.partial(fwd_kernel, n), out_shape=(jax.ShapeDtypeStruct((PARTS, r, TILE), F32),) * 2,
        in_specs=[vm] * 3, out_specs=(vm,) * 2, name="attention_fwd",
        scratch_shapes=Scatter.scratch(n, TILE + 8, 2 * TILE),
        cost_estimate=pl.CostEstimate(flops=4 * 384 * total * keys, bytes_accessed=12_000_000, transcendentals=6 * total * keys),
        compiler_params=pltpu.CompilerParams(collective_id=cid, has_side_effects=True, vmem_limit_bytes=VMEM_LIMIT),
    )(q_t, k_aug, v_t)


SCATTER_REFS = 12


def bwd_kernel(n, forms, q_ref, do_ref, st_ref, k_ref, v_ref, kt_ref, *refs):
    count = len(forms)
    grads, refs = refs[:count], refs[count:]
    dq_ref, dk_ref, dv_ref = refs[:3]
    sums, refs = refs[3:3 + count], refs[3 + count:]
    dk_acc, dv_acc = refs[:2]
    bufs, refs = refs[2:2 + SCATTER_REFS], refs[2 + SCATTER_REFS:]
    half = TILE // 2
    one = jnp.ones((1, QB), F32)
    zero = jnp.zeros((1, QB), F32)
    blank = jnp.zeros((half, QB), BF16)
    nt = (((1,), (1,)), ((), ()))
    at = Place(n)
    at.barrier()
    scatter = Scatter(n, at, False, bufs)
    reduces = [Reduce(n, at, form, grads[i], sums[i], refs[REDUCE_REFS * i:REDUCE_REFS * (i + 1)])
               for i, form in enumerate(forms)]

    def advance(stage):
        for red in reduces:
            red.advance(stage)

    advance(0)
    dk_acc[...] = jnp.zeros_like(dk_acc)
    dv_acc[...] = jnp.zeros_like(dv_acc)

    def block(p, src, near, dst):
        probs, dscores, dos, qs, dqs = [], [], [], [], []
        for j in range(2):
            qh = q_ref[p, half * j:half * (j + 1), src]
            doh = do_ref[p, half * j:half * (j + 1), src]
            lse = st_ref[p, j:j + 1, src]
            delta = st_ref[p, 2 + j:3 + j, src]
            qa = jnp.concatenate([qh, aux_rows([one] + split3(-lse), QB)], axis=0)
            da = jnp.concatenate([doh, aux_rows([zero] + split3(-delta), QB)], axis=0)
            e = jnp.exp(jnp.dot(k_ref[2 * p + j], qa, preferred_element_type=F32))
            dp = jnp.dot(v_ref[2 * p + j], da, preferred_element_type=F32)
            ds = (e * dp).astype(BF16)
            probs.append(e.astype(BF16))
            dscores.append(ds)
            order = (lambda a: [a, blank]) if j == 0 else (lambda a: [blank, a])
            dos.append(jnp.concatenate(order(doh), axis=0))
            qs.append(jnp.concatenate(order(qh), axis=0))
            dqs.append(0.125 * jnp.dot(kt_ref[p, half * j:half * (j + 1), :], ds, preferred_element_type=F32))
        dv_acc[p] += (lax.dot_general(probs[0], dos[0], nt, preferred_element_type=F32)
                      + lax.dot_general(probs[1], dos[1], nt, preferred_element_type=F32))
        dk_acc[p] += (lax.dot_general(dscores[0], qs[0], nt, preferred_element_type=F32)
                      + lax.dot_general(dscores[1], qs[1], nt, preferred_element_type=F32))
        put(scatter, near, p, slice(None), dst, jnp.concatenate(dqs, axis=0))

    trips = 2 * n * (n * TILE // QB)
    when = [min(w, trips - 1) for w in (1, trips // 2, trips // 2 + 1, trips // 2 + 2, trips // 2 + 3, max(trips // 2 + 3, trips - 2))]
    blocks_loop(n, scatter, block, [(w, functools.partial(advance, i + 1)) for i, w in enumerate(when)])
    for p in range(PARTS):
        dk_ref[:, p * TILE:(p + 1) * TILE] = dk_acc[p].astype(BF16)
        dv_ref[:, p * TILE:(p + 1) * TILE] = dv_acc[p].astype(BF16)
    scatter.finish(dq_ref)
    advance(7)


def attention_bwd(n, cid, q_t, do_t, stats, k_aug, v_aug, k_t, wide, tall):
    total, keys = q_t.shape[2], k_aug.shape[1]
    r = TILE // n
    forms = [Wide(a.shape, n) for a in wide] + [Tall(a.shape, n) for a in tall]
    grads = list(wide) + list(tall)
    vm = pl.BlockSpec(memory_space=pltpu.VMEM)
    flat = jax.ShapeDtypeStruct((keys, PARTS * TILE), BF16)
    acc = pltpu.VMEM((PARTS, keys, TILE), F32)
    outs = [jax.ShapeDtypeStruct((PARTS, r, TILE), F32), flat, flat] + [jax.ShapeDtypeStruct(a.shape, F32) for a in grads]
    scratch = [acc, acc] + Scatter.scratch(n, TILE, TILE)
    for form in forms:
        scratch += Reduce.scratch(n, form)
    return pl.pallas_call(
        functools.partial(bwd_kernel, n, forms), out_shape=tuple(outs),
        in_specs=[vm] * 6 + [pl.BlockSpec(memory_space=pl.ANY)] * len(grads), out_specs=(vm,) * len(outs), name="attention_bwd",
        scratch_shapes=scratch,
        cost_estimate=pl.CostEstimate(flops=10 * 384 * total * keys, bytes_accessed=20_000_000, transcendentals=6 * total * keys),
        compiler_params=pltpu.CompilerParams(collective_id=cid, has_side_effects=True, vmem_limit_bytes=VMEM_LIMIT),
    )(q_t, do_t, stats, k_aug, v_aug, k_t, *grads)


def reduce_kernel(n, form, src, small, out, small_out, slots, pair, ssend, srecv, *bufs):
    at = Place(n)
    at.barrier()
    red = Reduce(n, at, form, src, out, bufs)

    def small_copies(stage):
        if stage == 3:
            return [rcopy(pair.at[at.core], pair.at[at.core], ssend.at[3, 0], srecv.at[3, 0], at.other_core())]
        mine = slots.at[stage, at.coord[stage]]
        return [rcopy(mine, mine, ssend.at[stage, k - 1], srecv.at[stage, k - 1], at.along(stage, k)) for k in range(1, n)]

    red.advance(0)
    slots[0, at.coord[0]] = small[...]
    for c in small_copies(0):
        c.start()
    for stage in range(1, 8):
        red.advance(stage)
        if stage < 5:
            for c in small_copies(stage - 1):
                c.wait()
            if stage < 4:
                val = functools.reduce(jnp.add, [slots[stage - 1, k] for k in range(n)])
                if stage < 3:
                    slots[stage, at.coord[stage]] = val
                else:
                    pair[at.core] = val
                for c in small_copies(stage):
                    c.start()
            else:
                small_out[...] = pair[0] + pair[1]


def all_reduce_late(n, cid, stack, small):
    form = Stack(stack.shape, n)
    vm = pl.BlockSpec(memory_space=pltpu.VMEM)
    sem = pltpu.SemaphoreType.DMA
    return pl.pallas_call(
        functools.partial(reduce_kernel, n, form),
        out_shape=(jax.ShapeDtypeStruct(stack.shape, F32), jax.ShapeDtypeStruct(small.shape, F32)),
        in_specs=[pl.BlockSpec(memory_space=pl.ANY), vm], out_specs=(vm, vm), name="reduce_late",
        scratch_shapes=[pltpu.VMEM((3, n) + small.shape, F32), pltpu.VMEM((2,) + small.shape, F32),
                        sem((4, n - 1)), sem((4, n - 1))] + Reduce.scratch(n, form),
        compiler_params=pltpu.CompilerParams(collective_id=cid, has_side_effects=True, vmem_limit_bytes=VMEM_LIMIT),
    )(stack, small)


def solution(mesh):
    group = mesh.shape['seq']
    n = round((group // 2) ** (1 / 3))
    row_spec = P(('data', 'seq'), None)
    weight_spec = P()
    part_vec = P('data')
    part_mat = P('data', None)
    part_cube = P('data', None, None)

    def by_part(a):
        return jnp.transpose(a.reshape(a.shape[0], PARTS, TILE), (1, 0, 2))

    def by_row(a):
        return jnp.transpose(a, (1, 0, 2)).reshape(a.shape[1], PARTS * TILE)

    def device_step(dec_in, memory, mem_len, grad_out, norm_attn, wq_cross, wk_cross, wv_cross, wo_cross, norm_mlp, w_gate, w_up, w_down):
        q_rows, model_dim = dec_in.shape
        m_rows = memory.shape[0]
        heads, head_dim = wq_cross.shape[1], wq_cross.shape[2]
        wide = heads * head_dim
        wq, wk, wv = (w.reshape(model_dim, wide) for w in (wq_cross, wk_cross, wv_cross))
        wo = wo_cross.reshape(wide, model_dim)
        mem_pos = lax.axis_index('seq') * m_rows + jnp.arange(m_rows)
        bias = jnp.where(mem_pos < mem_len[0], 0.0, NEG).astype(BF16)

        x_in = dec_in.astype(F32)
        normed_f, norm_pull = jax.vjp(rms_norm, x_in, norm_attn.astype(F32))
        normed = normed_f.astype(BF16)
        local_query = jnp.dot(normed, wq, preferred_element_type=F32).astype(BF16) * jnp.asarray(head_dim ** -0.5, BF16)
        q_t = all_gather_t(n, 0, by_part(local_query))

        mem_keys = jnp.dot(memory, wk, preferred_element_type=F32).astype(BF16)
        mem_vals = jnp.dot(memory, wv, preferred_element_type=F32).astype(BF16)
        k_t = mem_keys.T.reshape(PARTS, TILE, m_rows)
        v_t = mem_vals.T.reshape(PARTS, TILE, m_rows)
        ones = jnp.ones((m_rows, 3), BF16)
        aux_k = jnp.concatenate([bias[:, None], ones, jnp.zeros((m_rows, 60), BF16)], axis=1)
        aux_v = jnp.concatenate([jnp.zeros((m_rows, 1), BF16), ones, jnp.zeros((m_rows, 60), BF16)], axis=1)

        def augment(a, aux):
            return jnp.stack([jnp.concatenate([a[:, head_dim * h:head_dim * (h + 1)], aux], axis=1) for h in range(heads)])

        k_aug = augment(mem_keys, aux_k)
        v_aug = augment(mem_vals, aux_v)

        out_parts, lse = attention_fwd(n, 1, q_t, k_aug, v_t)
        attended_f = by_row(out_parts)

        attended = attended_f.astype(BF16)
        hidden_f = x_in + jnp.dot(attended, wo, preferred_element_type=F32)
        hidden = hidden_f.astype(BF16)
        normed_mlp_f, mlp_norm_pull = jax.vjp(rms_norm, hidden.astype(F32), norm_mlp.astype(F32))
        normed_mlp = normed_mlp_f.astype(BF16)
        gate_pre = jnp.dot(normed_mlp, w_gate, preferred_element_type=F32)
        up_pre = jnp.dot(normed_mlp, w_up, preferred_element_type=F32)
        mlp_f, gated_pull = jax.vjp(gated_unit, gate_pre, up_pre)
        mlp_act = mlp_f.astype(BF16)

        grad_top = grad_out.astype(BF16)
        g_down = jnp.einsum('qf,qd->fd', mlp_act, grad_top, preferred_element_type=F32)
        grad_act = jnp.einsum('qd,fd->qf', grad_top, w_down, preferred_element_type=F32)
        grad_gate, grad_up = gated_pull(grad_act)
        grad_gate_b = grad_gate.astype(BF16)
        grad_up_b = grad_up.astype(BF16)
        g_gate = jnp.einsum('qd,qf->df', normed_mlp, grad_gate_b, preferred_element_type=F32)
        g_up = jnp.einsum('qd,qf->df', normed_mlp, grad_up_b, preferred_element_type=F32)
        grad_normed_mlp = (jnp.einsum('qf,df->qd', grad_gate_b, w_gate, preferred_element_type=F32)
                           + jnp.einsum('qf,df->qd', grad_up_b, w_up, preferred_element_type=F32))
        grad_hidden_norm, g_norm_mlp = mlp_norm_pull(grad_normed_mlp)
        grad_hidden = grad_out + grad_hidden_norm
        grad_hidden_b = grad_hidden.astype(BF16)
        g_wo = jnp.einsum('qe,qd->ed', attended, grad_hidden_b, preferred_element_type=F32)
        grad_attended = jnp.einsum('qd,ed->qe', grad_hidden_b, wo, preferred_element_type=F32)
        delta = jnp.sum((grad_attended * attended_f).reshape(q_rows, PARTS, 2, head_dim), axis=-1)
        delta = jnp.transpose(delta, (1, 0, 2))
        stats_in = jnp.concatenate([lse[:, :, 0:2], delta, jnp.zeros((PARTS, q_rows, TILE - 4), F32)], axis=2)
        do_t, stats = all_gather_t(n, 2, by_part(grad_attended.astype(BF16)), stats_in)

        dq_parts, dk_b, dv_b, g_gate, g_up, g_down = attention_bwd(
            n, 3, q_t, do_t, stats, k_aug, v_aug, k_t, (g_gate, g_up), (g_down,))
        grad_query_b = by_row(dq_parts).astype(BF16)

        g_wq = jnp.einsum('td,te->de', normed, grad_query_b, preferred_element_type=F32)
        grad_normed = jnp.einsum('te,de->td', grad_query_b, wq, preferred_element_type=F32)
        grad_x_norm, g_norm_attn = norm_pull(grad_normed)
        g_dec = grad_hidden + grad_x_norm
        g_wk = jnp.einsum('td,te->de', memory, dk_b, preferred_element_type=F32)
        g_wv = jnp.einsum('td,te->de', memory, dv_b, preferred_element_type=F32)
        g_mem = (jnp.einsum('te,de->td', dk_b, wk, preferred_element_type=F32)
                 + jnp.einsum('te,de->td', dv_b, wv, preferred_element_type=F32))
        small = jnp.concatenate([g_norm_attn[None], g_norm_mlp[None], jnp.zeros((6, model_dim), F32)], axis=0)
        late, small = all_reduce_late(n, 4, jnp.stack([g_wq, g_wk, g_wv, g_wo]), small)
        cube = (model_dim, heads, head_dim)
        g_wq, g_wk, g_wv = late[0], late[1], late[2]
        g_wo = late[3].reshape(heads, head_dim, model_dim)
        g_norm_attn, g_norm_mlp = small[0], small[1]
        return (g_dec, g_mem, g_norm_attn, g_wq.reshape(cube), g_wk.reshape(cube), g_wv.reshape(cube),
                g_wo, g_norm_mlp, g_gate, g_up, g_down)

    return jax.shard_map(device_step, mesh=mesh,
                         in_specs=(row_spec, row_spec, part_vec, row_spec) + (weight_spec,) * 9,
                         out_specs=(row_spec, row_spec, part_vec, part_cube, part_cube, part_cube, part_cube, part_vec, part_mat, part_mat, part_mat),
                         check_vma=False)
```

```python
import functools

import jax
import jax.numpy as jnp
from jax import lax
from jax.experimental import pallas as pl
from jax.experimental.pallas import tpu as pltpu
from jax.sharding import PartitionSpec as P

F32 = jnp.float32
BF16 = jnp.bfloat16
MESH = pl.DeviceIdType.MESH
VMEM_LIMIT = 62 * 1024 * 1024
NEG = -1e30
ORDERS = ((0, 1, 2), (2, 0, 1), (1, 2, 0))
PARTS = 3
TILE = 128


def rms_norm(tensor, gain):
    mean_sq = jnp.mean(tensor * tensor, axis=-1, keepdims=True)
    return tensor * lax.rsqrt(mean_sq + 1e-6) * gain


def gated_unit(gate_pre, up_pre):
    return jax.nn.silu(gate_pre) * up_pre


class Place:
    def __init__(self, n):
        self.n = n
        me = lax.axis_index("seq")
        self.me = me
        self.core = lax.rem(me, 2)
        x = lax.rem(me // 2, n)
        y = lax.rem(me // (2 * n), n)
        z = me // (2 * n * n)
        self.coord = (z, y, x)
        self.stride = (2 * n * n, 2 * n, 2)

    def along(self, axis, k):
        here = self.coord[axis]
        return self.me + (lax.rem(here + k, self.n) - here) * self.stride[axis]

    def other_core(self):
        return self.me + 1 - 2 * self.core

    def quarter(self):
        return self.me // (self.n ** 3 // 2)

    def mate(self, q):
        size = self.n ** 3 // 2
        return q * size + lax.rem(self.me, size)

    def to(self, k):
        return {"seq": k}

    def barrier(self):
        sem = pltpu.get_barrier_semaphore()
        for axis in range(3):
            for k in range(1, self.n):
                pl.semaphore_signal(sem, inc=1, device_id=self.to(self.along(axis, k)), device_id_type=MESH)
        pl.semaphore_signal(sem, inc=1, device_id=self.to(self.other_core()), device_id_type=MESH)
        extra = 0
        if self.n < 4:
            for k in range(1, 4):
                pl.semaphore_signal(sem, inc=1, device_id=self.to(self.mate(lax.rem(self.quarter() + k, 4))), device_id_type=MESH)
            extra = 3
        pl.semaphore_wait(sem, 3 * (self.n - 1) + 1 + extra)


def rcopy(src, dst, send, recv, device):
    return pltpu.make_async_remote_copy(src_ref=src, dst_ref=dst, send_sem=send, recv_sem=recv,
                                        device_id={"seq": device}, device_id_type=MESH)


def lanes(start, size):
    return pl.ds(pl.multiple_of(start, TILE), size)


def rows_of(start, size):
    return pl.ds(pl.multiple_of(start, 8), size)


class Gather:
    def __init__(self, n, at, src, full, bufs):
        self.n, self.at, self.src, self.full = n, at, src, full
        self.rows, self.send, self.recv, self.rsend, self.rrecv, self.csend, self.crecv = bufs
        self.copies = {}
        self.split = full.shape[1] == TILE and n == 4

    @staticmethod
    def scratch(n, dtype):
        sem = pltpu.SemaphoreType.DMA
        return [pltpu.VMEM((PARTS, TILE, TILE), dtype), sem((3, PARTS, n - 1)), sem((3, PARTS, n - 1)),
                sem((3, PARTS, 2)), sem((3, PARTS, 2)), sem((PARTS,)), sem((PARTS,))]

    def begin(self):
        n, at = self.n, self.at
        r = TILE // n
        for p in range(PARTS):
            a3 = ORDERS[p][2]
            mine = rows_of(at.coord[a3] * r, r)
            for k in range(1, n):
                c = rcopy(self.src.at[p], self.rows.at[p, mine, :], self.send.at[0, p, k - 1], self.recv.at[0, p, k - 1], at.along(a3, k))
                c.start()
                self.copies[0, p, k] = c
            self.rows[p, mine, :] = self.src[p]

    def turn(self):
        at, n = self.at, self.n
        for p in range(PARTS):
            a1, a2, _ = ORDERS[p]
            for k in range(1, n):
                self.copies[0, p, k].wait()
            block = self.rows[p].astype(F32).T
            base = ((at.core * n + at.coord[a1]) * n + at.coord[a2]) * TILE
            self.full[p, :, lanes(base, TILE)] = block[:self.full.shape[1]].astype(self.full.dtype)

    def place(self, stage, p, back):
        at, n = self.at, self.n
        a1, a2, _ = ORDERS[p]
        if stage == 1:
            spot = lax.rem(at.coord[a2] + n - back, n)
            return a2, lanes(((at.core * n + at.coord[a1]) * n + spot) * TILE, TILE)
        spot = lax.rem(at.coord[a1] + n - back, n)
        return a1, lanes((at.core * n + spot) * n * TILE, n * TILE)

    def spread(self, stage):
        n, at = self.n, self.at
        for p in range(PARTS):
            axis, cols = self.place(stage, p, 0)
            view = self.full.at[p, :, cols]
            for k in range(1, n):
                if self.split and k == 2:
                    continue
                c = rcopy(view, view, self.send.at[stage, p, k - 1], self.recv.at[stage, p, k - 1], at.along(axis, k))
                c.start()
                self.copies[stage, p, k] = c

    def settle(self, stage):
        n, at = self.n, self.at
        half = TILE // 2
        if not self.split:
            for p in range(PARTS):
                for k in range(1, n):
                    self.copies[stage, p, k].wait()
            return
        relays = []
        for p in range(PARTS):
            for k, i in ((1, 0), (3, 1)):
                self.copies[stage, p, k].wait_recv()
                axis, cols = self.place(stage, p, k)
                view = self.full.at[p, half * i:half * (i + 1), cols]
                c = rcopy(view, view, self.rsend.at[stage, p, i], self.rrecv.at[stage, p, i], at.along(axis, k))
                c.start()
                relays.append(c)
        for p in range(PARTS):
            for k in (1, 3):
                self.copies[stage, p, k].wait_send()
        for c in relays:
            c.wait()

    def swap(self):
        n, at = self.n, self.at
        width = n * n * TILE
        out = []
        for p in range(PARTS):
            view = self.full.at[p, :, lanes(at.core * width, width)]
            c = rcopy(view, view, self.csend.at[p], self.crecv.at[p], at.other_core())
            c.start()
            out.append(c)
        return out


GATHER_REFS = 7


def run_gathers(gathers, between=None):
    for g in gathers:
        g.begin()
    for g in gathers:
        g.turn()
        g.spread(1)
    for g in gathers:
        g.settle(1)
        g.spread(2)
    if between is not None:
        between()
    final = []
    for g in gathers:
        g.settle(2)
        final += g.swap()
    for c in final:
        c.wait()


def prepare_kernel(n, x_ref, mem_ref, wk_ref, wv_ref, auxk_ref, auxv_ref,
                   q_ref, keep_ref, k_ref, v_ref, kt_ref, vt_ref, *bufs):
    gbufs, (msend, mrecv) = bufs[:GATHER_REFS], bufs[GATHER_REFS:]
    at = Place(n)
    at.barrier()
    keep = keep_ref.shape[0]
    piece = keep // 3
    quarter = at.quarter()
    donor = quarter < 3

    def donate(q):
        return rcopy(mem_ref.at[pl.ds(keep, piece), :], keep_ref.at[pl.ds(q * piece, piece), :], msend, mrecv.at[q], at.mate(3))

    for q in range(3):
        @pl.when(quarter == q)
        def _(q=q):
            donate(q).start()

    def project():
        @pl.when(donor)
        def _():
            keep_ref[...] = mem_ref[0:keep, :]

        @pl.when(quarter == 3)
        def _():
            for q in range(3):
                donate(q).wait_recv()

        low = lax.broadcasted_iota(jnp.int32, (piece, TILE), 1) < TILE // 2

        def some(i, _):
            rows = pl.ds(pl.multiple_of(i * piece, piece), piece)
            m = keep_ref[rows, :]
            for w_ref, aux_ref, a_ref, t_ref in ((wk_ref, auxk_ref, k_ref, kt_ref), (wv_ref, auxv_ref, v_ref, vt_ref)):
                aux = aux_ref[rows, :].astype(F32)
                for p in range(PARTS):
                    b = jnp.dot(m, w_ref[:, p * TILE:(p + 1) * TILE], preferred_element_type=F32).astype(BF16).astype(F32)
                    a_ref[2 * p, rows, :] = jnp.where(low, b, aux).astype(BF16)
                    a_ref[2 * p + 1, rows, :] = jnp.where(low, aux, b).astype(BF16)
                    t_ref[p, :, rows] = b.T.astype(BF16)
            return 0

        for i in range(3):
            some(i, 0)

    run_gathers([Gather(n, at, x_ref, q_ref, gbufs)], project)
    for q in range(3):
        @pl.when(quarter == q)
        def _(q=q):
            donate(q).wait_send()


def prepare(n, cid, rows, memory, wk, wv, aux_k, aux_v):
    total = 2 * n * n * TILE
    keep, dim = aux_k.shape[0], memory.shape[1]
    vm = pl.BlockSpec(memory_space=pltpu.VMEM)
    sem = pltpu.SemaphoreType.DMA
    shape = jax.ShapeDtypeStruct
    outs = (shape((PARTS, TILE, total), BF16), shape((keep, dim), BF16), shape((2 * PARTS, keep, TILE), BF16),
            shape((2 * PARTS, keep, TILE), BF16), shape((PARTS, TILE, keep), BF16), shape((PARTS, TILE, keep), BF16))
    return pl.pallas_call(
        functools.partial(prepare_kernel, n), out_shape=outs, in_specs=[vm] * 6, out_specs=(vm,) * 6,
        scratch_shapes=Gather.scratch(n, BF16) + [sem(()), sem((3,))], name="prepare",
        compiler_params=pltpu.CompilerParams(collective_id=cid, has_side_effects=True, vmem_limit_bytes=VMEM_LIMIT),
    )(rows, memory, wk, wv, aux_k, aux_v)


def gather_kernel(n, x_ref, s_ref, out_ref, sout_ref, *bufs):
    at = Place(n)
    at.barrier()
    run_gathers([Gather(n, at, s_ref, sout_ref, bufs[GATHER_REFS:]), Gather(n, at, x_ref, out_ref, bufs[:GATHER_REFS])])


def all_gather_t(n, cid, rows, stats):
    total = 2 * n * n * TILE
    vm = pl.BlockSpec(memory_space=pltpu.VMEM)
    return pl.pallas_call(
        functools.partial(gather_kernel, n),
        out_shape=(jax.ShapeDtypeStruct((PARTS, TILE, total), BF16), jax.ShapeDtypeStruct((PARTS, 8, total), F32)),
        in_specs=[vm] * 2, out_specs=(vm,) * 2,
        scratch_shapes=Gather.scratch(n, BF16) + Gather.scratch(n, F32), name="gather_stats",
        compiler_params=pltpu.CompilerParams(collective_id=cid, has_side_effects=True, vmem_limit_bytes=VMEM_LIMIT),
    )(rows, stats)


def merge(blocks, rows_axis):
    take = (lambda b, i, j: b[i:j]) if rows_axis == 0 else (lambda b, i, j: b[:, i:j])
    half = TILE // 2
    outs, maxes, sums = [], [], []
    for h in range(2):
        ms = [take(b, TILE + h, TILE + h + 1) for b in blocks]
        m = functools.reduce(jnp.maximum, ms)
        ws = [jnp.exp(v - m) for v in ms]
        o = sum(take(b, half * h, half * h + half) * w for b, w in zip(blocks, ws))
        l = sum(take(b, TILE + 2 + h, TILE + 3 + h) * w for b, w in zip(blocks, ws))
        outs.append(o)
        maxes.append(m)
        sums.append(l)
    return outs, maxes + sums


class Scatter:
    def __init__(self, n, at, with_stats, bufs):
        self.n, self.at, self.with_stats = n, at, with_stats
        (self.far, self.near, self.buf0, self.buf1, self.acc1, self.buf2, self.acc2, self.buf3,
         self.csend, self.crecv, self.send, self.recv) = bufs
        self.step = n * TILE

    @staticmethod
    def scratch(n, rows, wide):
        sem = pltpu.SemaphoreType.DMA
        half = n * n * TILE
        r = TILE // n
        return [
            pltpu.VMEM((PARTS, rows, half), F32), pltpu.VMEM((PARTS, rows, half), F32), pltpu.VMEM((PARTS, rows, half), F32),
            pltpu.VMEM((PARTS, n - 1, rows, n * TILE), F32), pltpu.VMEM((PARTS, rows, n * TILE), F32),
            pltpu.VMEM((PARTS, n - 1, rows, TILE), F32), pltpu.VMEM((PARTS, TILE, wide), F32),
            pltpu.VMEM((PARTS, n - 1, r, wide), F32),
            sem((PARTS, n)), sem((PARTS, n)), sem((3, PARTS, n - 1)), sem((3, PARTS, n - 1)),
        ]

    def chunk(self, p, k):
        return lax.rem(self.at.coord[ORDERS[p][0]] + k, self.n)

    def combine(self, dst, p, col, vals):
        if self.with_stats:
            outs, stats = merge(vals, 0)
            dst[p, 0:TILE // 2, col] = outs[0]
            dst[p, TILE // 2:TILE, col] = outs[1]
            dst[p, TILE:TILE + 8, col] = jnp.concatenate(stats + [jnp.zeros_like(stats[0])] * 4, axis=0)
        else:
            dst[p, :, col] = functools.reduce(jnp.add, vals)

    def core_copy(self, p, k):
        view = (p, slice(None), lanes(self.chunk(p, k) * self.step, self.step))
        return rcopy(self.far.at[view], self.buf0.at[view], self.csend.at[p, k], self.crecv.at[p, k], self.at.other_core())

    def first_copy(self, p, k):
        return rcopy(self.near.at[p, :, lanes(self.chunk(p, k) * self.step, self.step)], self.buf1.at[p, k - 1],
                     self.send.at[0, p, k - 1], self.recv.at[0, p, k - 1], self.at.along(ORDERS[p][0], k))

    def far_done(self, k):
        for p in range(PARTS):
            self.core_copy(p, k).start()

    def near_done(self, k):
        for p in range(PARTS):
            self.core_copy(p, k).wait()

            def fold(j, _, p=p):
                col = lanes(self.chunk(p, k) * self.step + j * TILE, TILE)
                self.combine(self.near, p, col, [self.near[p, :, col], self.buf0[p, :, col]])
                return 0

            lax.fori_loop(0, self.n, fold, 0)

            @pl.when(k > 0)
            def _(p=p):
                self.first_copy(p, k).start()

    def finish(self, o_ref, st_ref=None):
        n, at = self.n, self.at
        r = TILE // n
        copies = {}
        for p in range(PARTS):
            a1, a2, _ = ORDERS[p]
            for k in range(1, n):
                self.first_copy(p, k).wait()
            mine = at.coord[a1] * n * TILE
            for j in range(n):
                col = slice(j * TILE, (j + 1) * TILE)
                self.combine(self.acc1, p, pl.ds(j * TILE, TILE),
                             [self.near[p, :, lanes(mine + j * TILE, TILE)]] + [self.buf1[p, k, :, col] for k in range(n - 1)])
            for k in range(1, n):
                there = lax.rem(at.coord[a2] + k, n)
                c = rcopy(self.acc1.at[p, :, lanes(there * TILE, TILE)], self.buf2.at[p, k - 1],
                          self.send.at[1, p, k - 1], self.recv.at[1, p, k - 1], at.along(a2, k))
                c.start()
                copies[1, p, k] = c
        for p in range(PARTS):
            _, a2, a3 = ORDERS[p]
            for k in range(1, n):
                copies[1, p, k].wait()
            blocks = [self.acc1[p, :, lanes(at.coord[a2] * TILE, TILE)]] + [self.buf2[p, k] for k in range(n - 1)]
            if self.with_stats:
                outs, stats = merge(blocks, 0)
                self.acc2[p, :, 0:TILE] = jnp.concatenate(outs, axis=0).T
                tail = jnp.concatenate(stats + [jnp.zeros((TILE - 4, TILE), F32)], axis=0)
                self.acc2[p, :, TILE:2 * TILE] = tail.T
            else:
                self.acc2[p] = functools.reduce(jnp.add, blocks).T
            for k in range(1, n):
                there = lax.rem(at.coord[a3] + k, n)
                c = rcopy(self.acc2.at[p, pl.ds(pl.multiple_of(there * r, r), r), :], self.buf3.at[p, k - 1],
                          self.send.at[2, p, k - 1], self.recv.at[2, p, k - 1], at.along(a3, k))
                c.start()
                copies[2, p, k] = c
        for p in range(PARTS):
            a3 = ORDERS[p][2]
            for k in range(1, n):
                copies[2, p, k].wait()
            blocks = [self.acc2[p, pl.ds(pl.multiple_of(at.coord[a3] * r, r), r), :]] + [self.buf3[p, k] for k in range(n - 1)]
            if self.with_stats:
                outs, (m0, m1, l0, l1) = merge(blocks, 1)
                o_ref[p] = jnp.concatenate([outs[0] / l0, outs[1] / l1], axis=1)
                col = lax.broadcasted_iota(jnp.int32, (r, TILE), 1)
                st_ref[p] = jnp.where(col == 0, m0 + jnp.log(l0), jnp.where(col == 1, m1 + jnp.log(l1), 0.0))
            else:
                o_ref[p] = functools.reduce(jnp.add, blocks)


class Wide:
    def __init__(self, shape, n):
        self.part, self.cols = shape[0] // PARTS, shape[1]
        self.r1, self.r2, self.c3 = self.part // 2, self.part // 2 // n, shape[1] // n
        self.l1, self.l2, self.l3 = (self.r1, self.cols), (self.r2, self.cols), (self.r2, self.c3)

    def full1(self, p, c):
        return rows_of(self.part * p + self.r1 * c, self.r1), slice(None)

    def full2(self, p, c, a):
        return rows_of(self.part * p + self.r1 * c + self.r2 * a, self.r2), slice(None)

    def full3(self, p, c, a, b):
        return rows_of(self.part * p + self.r1 * c + self.r2 * a, self.r2), lanes(self.c3 * b, self.c3)

    def in1(self, a):
        return rows_of(self.r2 * a, self.r2), slice(None)

    def in2(self, b):
        return slice(None), lanes(self.c3 * b, self.c3)


class Tall(Wide):
    def __init__(self, shape, n):
        super().__init__(shape, n)
        self.r3 = self.r2 // n
        self.l3 = (self.r3, self.cols)

    def full3(self, p, c, a, b):
        return rows_of(self.part * p + self.r1 * c + self.r2 * a + self.r3 * b, self.r3), slice(None)

    def in2(self, b):
        return rows_of(self.r3 * b, self.r3), slice(None)


class Stack:
    def __init__(self, shape, n):
        w, rows, cols = shape
        self.part, self.w3 = rows // PARTS, w // n
        self.r1, self.r2 = self.part // 2, self.part // 2 // n
        self.l1, self.l2, self.l3 = (w, self.r1, cols), (w, self.r2, cols), (self.w3, self.r2, cols)

    def full1(self, p, c):
        return slice(None), rows_of(self.part * p + self.r1 * c, self.r1), slice(None)

    def full2(self, p, c, a):
        return slice(None), rows_of(self.part * p + self.r1 * c + self.r2 * a, self.r2), slice(None)

    def full3(self, p, c, a, b):
        return pl.ds(self.w3 * b, self.w3), rows_of(self.part * p + self.r1 * c + self.r2 * a, self.r2), slice(None)

    def in1(self, a):
        return slice(None), rows_of(self.r2 * a, self.r2), slice(None)

    def in2(self, b):
        return pl.ds(self.w3 * b, self.w3), slice(None), slice(None)


REDUCE_REFS = 15


class Reduce:
    def __init__(self, n, at, form, src, out, bufs):
        self.n, self.at, self.form, self.src, self.out = n, at, form, src, out
        (self.own, self.buf0, self.buf1, self.acc1, self.buf2, self.buf3, self.lsem,
         self.csend, self.crecv, self.send, self.recv, self.gsend, self.grecv, self.dsend, self.drecv) = bufs

    @staticmethod
    def scratch(n, form):
        sem = pltpu.SemaphoreType.DMA
        return [
            pltpu.VMEM((PARTS,) + form.l1, F32), pltpu.VMEM((PARTS,) + form.l1, F32),
            pltpu.VMEM((PARTS, n - 1) + form.l2, F32), pltpu.VMEM((PARTS,) + form.l2, F32),
            pltpu.VMEM((PARTS, n - 1) + form.l3, F32), pltpu.VMEM((PARTS, n) + form.l3, F32),
            sem((PARTS,)), sem((PARTS,)), sem((PARTS,)), sem((3, PARTS, n - 1)), sem((3, PARTS, n - 1)),
            sem((2, PARTS, n - 1)), sem((2, PARTS, n - 1)), sem((PARTS,)), sem((PARTS,)),
        ]

    def spots(self, p):
        a1, a2, a3 = ORDERS[p]
        at = self.at
        return at.coord[a1], at.coord[a2], at.coord[a3]

    def copies(self, stage, p):
        at, n, form = self.at, self.n, self.form
        A1, A2, A3 = self.spots(p)
        a1, a2, a3 = ORDERS[p]
        c = at.core
        if stage == 0:
            return [rcopy(self.src.at[form.full1(p, 1 - c)], self.buf0.at[p], self.csend.at[p], self.crecv.at[p], at.other_core()),
                    pltpu.make_async_copy(self.src.at[form.full1(p, c)], self.own.at[p], self.lsem.at[p])]
        out = []
        if stage == 6:
            view = self.out.at[form.full1(p, c)]
            return [rcopy(view, view, self.dsend.at[p], self.drecv.at[p], at.other_core())]
        for k in range(1, n):
            if stage == 1:
                args = (self.own.at[p].at[form.in1(lax.rem(A1 + k, n))], self.buf1.at[p, k - 1], self.send.at[0, p, k - 1], self.recv.at[0, p, k - 1], at.along(a1, k))
            elif stage == 2:
                args = (self.acc1.at[p].at[form.in2(lax.rem(A2 + k, n))], self.buf2.at[p, k - 1], self.send.at[1, p, k - 1], self.recv.at[1, p, k - 1], at.along(a2, k))
            elif stage == 3:
                args = (self.buf3.at[p, A3], self.buf3.at[p, A3], self.send.at[2, p, k - 1], self.recv.at[2, p, k - 1], at.along(a3, k))
            elif stage == 4:
                view = self.out.at[form.full3(p, c, A1, A2)]
                args = (view, view, self.gsend.at[0, p, k - 1], self.grecv.at[0, p, k - 1], at.along(a2, k))
            else:
                view = self.out.at[form.full2(p, c, A1)]
                args = (view, view, self.gsend.at[1, p, k - 1], self.grecv.at[1, p, k - 1], at.along(a1, k))
            out.append(rcopy(*args))
        return out

    def advance(self, stage):
        form, n = self.form, self.n
        for p in range(PARTS):
            A1, A2, A3 = self.spots(p)
            if stage > 0:
                for c in self.copies(stage - 1, p):
                    c.wait()
            if stage == 1:
                self.own[p] = self.own[p] + self.buf0[p]
            elif stage == 2:
                self.acc1[p] = functools.reduce(jnp.add, [self.own[(p,) + form.in1(A1)]] + [self.buf1[p, k] for k in range(n - 1)])
            elif stage == 3:
                self.buf3[p, A3] = functools.reduce(jnp.add, [self.acc1[(p,) + form.in2(A2)]] + [self.buf2[p, k] for k in range(n - 1)])
            elif stage == 4:
                self.out[form.full3(p, self.at.core, A1, A2)] = functools.reduce(jnp.add, [self.buf3[p, k] for k in range(n)])
            if stage < 7:
                for c in self.copies(stage, p):
                    c.start()


QB = 256


def aux_rows(rows, width):
    pad = jnp.zeros((64 - len(rows), width), F32)
    return jnp.concatenate(list(rows) + [pad], axis=0).astype(BF16)


def split3(v):
    hi = v.astype(BF16).astype(F32)
    mid = (v - hi).astype(BF16).astype(F32)
    lo = (v - hi - mid).astype(BF16).astype(F32)
    return [hi, mid, lo]


def blocks_loop(n, scatter, blocks, events):
    per = n * TILE // QB
    at = scatter.at

    def body(t, _):
        u = t // per
        k = n - 1 - u // 2
        near = lax.rem(u, 2)
        half = jnp.where(near == 1, at.core, 1 - at.core)
        inside = [scatter.chunk(p, k) * (n * TILE) + lax.rem(t, per) * QB for p in range(PARTS)]
        srcs = [pl.ds(pl.multiple_of(half * (n * n * TILE) + i, QB), QB) for i in inside]
        blocks(srcs, near, [pl.ds(pl.multiple_of(i, QB), QB) for i in inside])
        last = lax.rem(t, per) == per - 1

        @pl.when(last & (near == 0))
        def _():
            scatter.far_done(k)

        @pl.when(last & (near == 1))
        def _():
            scatter.near_done(k)

        for when, action in events:
            @pl.when(t == when)
            def _(action=action):
                action()
        return 0

    lax.fori_loop(0, 2 * n * per, body, 0)


def put(scatter, near, p, row, col, val):
    @pl.when(near == 1)
    def _():
        scatter.near[p, row, col] = val

    @pl.when(near == 0)
    def _():
        scatter.far[p, row, col] = val


def beside(j, block, other):
    return jnp.concatenate([block, other] if j == 0 else [other, block], axis=0)


def shrink(op, v, rows):
    while v.shape[0] > rows:
        h = v.shape[0] // 2
        v = op(v[:h], v[h:])
    return v


KC = 256


def fwd_kernel(n, q_ref, k_ref, vt_ref, o_ref, st_ref, s_buf, *bufs):
    half = TILE // 2
    keys = k_ref.shape[1]
    kc = min(KC, keys // 3)
    chunks = keys // kc
    one = jnp.ones((1, QB), F32)
    aux = aux_rows([one], QB)
    at = Place(n)
    at.barrier()
    scatter = Scatter(n, at, True, bufs)

    def blocks(srcs, near, dsts):
        heads = [(p, j) for p in range(PARTS) for j in range(2)]

        def score(i, c, run):
            p, j = heads[i]
            qa = beside(j, q_ref[p, half * j:half * (j + 1), srcs[p]], aux)
            s = jnp.dot(k_ref[i, c * kc:(c + 1) * kc, :], qa, preferred_element_type=F32)
            s_buf[i % 2, c * kc:(c + 1) * kc, :] = s
            top = shrink(jnp.maximum, s, 16)
            return top if run is None else jnp.maximum(run, top)

        run = None
        for c in range(chunks):
            run = score(0, c, run)
        done = []
        for i, (p, j) in enumerate(heads):
            m = jnp.max(run, axis=0, keepdims=True)
            run, total, out = None, None, None
            for c in range(chunks):
                if i + 1 < len(heads):
                    run = score(i + 1, c, run)
                e = jnp.exp(s_buf[i % 2, c * kc:(c + 1) * kc, :] - m)
                part = shrink(jnp.add, e, 16)
                total = part if total is None else total + part
                o = jnp.dot(vt_ref[p, half * j:half * (j + 1), c * kc:(c + 1) * kc], e.astype(BF16), preferred_element_type=F32)
                out = o if out is None else out + o
            done.append((out, m, jnp.sum(total, axis=0, keepdims=True)))
            if j == 1:
                (o0, m0, l0), (o1, m1, l1) = done[-2:]
                val = jnp.concatenate([o0, o1, m0, m1, l0, l1, jnp.zeros((4, QB), F32)], axis=0)
                put(scatter, near, p, slice(None), dsts[p], val)

    blocks_loop(n, scatter, blocks, [])
    scatter.finish(o_ref, st_ref)


def attention_fwd(n, cid, q_t, k_aug, v_t):
    total, keys = q_t.shape[2], k_aug.shape[1]
    r = TILE // n
    vm = pl.BlockSpec(memory_space=pltpu.VMEM)
    return pl.pallas_call(
        functools.partial(fwd_kernel, n), out_shape=(jax.ShapeDtypeStruct((PARTS, r, TILE), F32),) * 2,
        in_specs=[vm] * 3, out_specs=(vm,) * 2, name="attention_fwd",
        scratch_shapes=[pltpu.VMEM((2, keys, QB), F32)] + Scatter.scratch(n, TILE + 8, 2 * TILE),
        cost_estimate=pl.CostEstimate(flops=4 * 384 * total * keys, bytes_accessed=12_000_000, transcendentals=6 * total * keys),
        compiler_params=pltpu.CompilerParams(collective_id=cid, has_side_effects=True, vmem_limit_bytes=VMEM_LIMIT),
    )(q_t, k_aug, v_t)


SCATTER_REFS = 12


def bwd_kernel(n, forms, q_ref, do_ref, st_ref, k_ref, v_ref, kt_ref, wk_ref, wv_ref, *refs):
    count = len(forms)
    grads, refs = refs[:count], refs[count:]
    dq_ref, dk_ref, dv_ref, dm_ref = refs[:4]
    sums, refs = refs[4:4 + count], refs[4 + count:]
    dk_acc, dv_acc, dm_buf, msend, mrecv = refs[:5]
    bufs, refs = refs[5:5 + SCATTER_REFS], refs[5 + SCATTER_REFS:]
    half = TILE // 2
    one = jnp.ones((1, QB), F32)
    zero = jnp.zeros((1, QB), F32)
    blank = jnp.zeros((half, QB), BF16)
    nt = (((1,), (1,)), ((), ()))
    at = Place(n)
    at.barrier()
    scatter = Scatter(n, at, False, bufs)
    reduces = [Reduce(n, at, form, grads[i], sums[i], refs[REDUCE_REFS * i:REDUCE_REFS * (i + 1)])
               for i, form in enumerate(forms)]

    def advance(stage):
        for red in reduces:
            red.advance(stage)

    advance(0)
    dk_acc[...] = jnp.zeros_like(dk_acc)
    dv_acc[...] = jnp.zeros_like(dv_acc)

    def block(p, src, near, dst):
        probs, dscores, dos, qs, dqs = [], [], [], [], []
        for j in range(2):
            qh = q_ref[p, half * j:half * (j + 1), src]
            doh = do_ref[p, half * j:half * (j + 1), src]
            lse = st_ref[p, j:j + 1, src]
            delta = st_ref[p, 2 + j:3 + j, src]
            qa = beside(j, qh, aux_rows([one] + split3(-lse), QB))
            da = beside(j, doh, aux_rows([zero] + split3(-delta), QB))
            e = jnp.exp(jnp.dot(k_ref[2 * p + j], qa, preferred_element_type=F32))
            dp = jnp.dot(v_ref[2 * p + j], da, preferred_element_type=F32)
            ds = (e * dp).astype(BF16)
            probs.append(e.astype(BF16))
            dscores.append(ds)
            dos.append(beside(j, doh, blank))
            qs.append(beside(j, qh, blank))
            dqs.append(0.125 * jnp.dot(kt_ref[p, half * j:half * (j + 1), :], ds, preferred_element_type=F32))
        dv_acc[p] += (lax.dot_general(probs[0], dos[0], nt, preferred_element_type=F32)
                      + lax.dot_general(probs[1], dos[1], nt, preferred_element_type=F32))
        dk_acc[p] += (lax.dot_general(dscores[0], qs[0], nt, preferred_element_type=F32)
                      + lax.dot_general(dscores[1], qs[1], nt, preferred_element_type=F32))
        put(scatter, near, p, slice(None), dst, jnp.concatenate(dqs, axis=0))

    trips = 2 * n * (n * TILE // QB)
    when = [min(w, trips - 1) for w in (1, trips // 2, trips // 2 + 1, trips // 2 + 2, trips // 2 + 3, max(trips // 2 + 3, trips - 2))]

    def blocks(srcs, near, dsts):
        for p in range(PARTS):
            block(p, srcs[p], near, dsts[p])

    blocks_loop(n, scatter, blocks, [(w, functools.partial(advance, i + 1)) for i, w in enumerate(when)])
    for p in range(PARTS):
        dk_ref[:, p * TILE:(p + 1) * TILE] = dk_acc[p].astype(BF16)
        dv_ref[:, p * TILE:(p + 1) * TILE] = dv_acc[p].astype(BF16)

    keep = dk_ref.shape[0]
    piece = keep // 3
    quarter = at.quarter()

    def give_back(q):
        return rcopy(dm_buf.at[pl.ds(q * piece, piece), :], dm_ref.at[pl.ds(keep, piece), :], msend.at[q], mrecv, at.mate(q))

    for i in range(3):
        rows = slice(i * piece, (i + 1) * piece)
        dm_buf[rows, :] = (lax.dot_general(dk_ref[rows, :], wk_ref[...], nt, preferred_element_type=F32)
                           + lax.dot_general(dv_ref[rows, :], wv_ref[...], nt, preferred_element_type=F32))

    @pl.when(quarter == 3)
    def _():
        for q in range(3):
            give_back(q).start()
        dm_ref[...] = jnp.zeros_like(dm_ref)

    @pl.when(quarter < 3)
    def _():
        dm_ref[0:keep, :] = dm_buf[...]

    scatter.finish(dq_ref)
    advance(7)

    @pl.when(quarter == 3)
    def _():
        for q in range(3):
            give_back(q).wait_send()

    @pl.when(quarter < 3)
    def _():
        give_back(0).wait_recv()


def attention_bwd(n, cid, m_rows, q_t, do_t, stats, k_aug, v_aug, k_t, wk, wv, wide, tall):
    total, keys = q_t.shape[2], k_aug.shape[1]
    r = TILE // n
    forms = [Wide(a.shape, n) for a in wide] + [Tall(a.shape, n) for a in tall]
    grads = list(wide) + list(tall)
    vm = pl.BlockSpec(memory_space=pltpu.VMEM)
    flat = jax.ShapeDtypeStruct((keys, PARTS * TILE), BF16)
    acc = pltpu.VMEM((PARTS, keys, TILE), F32)
    sem = pltpu.SemaphoreType.DMA
    outs = [jax.ShapeDtypeStruct((PARTS, r, TILE), F32), flat, flat, jax.ShapeDtypeStruct((m_rows, wk.shape[0]), F32)] + [jax.ShapeDtypeStruct(a.shape, F32) for a in grads]
    scratch = [acc, acc, pltpu.VMEM((keys, wk.shape[0]), F32), sem((3,)), sem(())] + Scatter.scratch(n, TILE, TILE)
    for form in forms:
        scratch += Reduce.scratch(n, form)
    return pl.pallas_call(
        functools.partial(bwd_kernel, n, forms), out_shape=tuple(outs),
        in_specs=[vm] * 8 + [pl.BlockSpec(memory_space=pl.ANY)] * len(grads), out_specs=(vm,) * len(outs), name="attention_bwd",
        scratch_shapes=scratch,
        cost_estimate=pl.CostEstimate(flops=10 * 384 * total * keys, bytes_accessed=20_000_000, transcendentals=6 * total * keys),
        compiler_params=pltpu.CompilerParams(collective_id=cid, has_side_effects=True, vmem_limit_bytes=VMEM_LIMIT),
    )(q_t, do_t, stats, k_aug, v_aug, k_t, wk, wv, *grads)


def reduce_kernel(n, form, src, small, out, small_out, slots, pair, ssend, srecv, *bufs):
    at = Place(n)
    at.barrier()
    red = Reduce(n, at, form, src, out, bufs)

    def small_copies(stage):
        if stage == 3:
            return [rcopy(pair.at[at.core], pair.at[at.core], ssend.at[3, 0], srecv.at[3, 0], at.other_core())]
        mine = slots.at[stage, at.coord[stage]]
        return [rcopy(mine, mine, ssend.at[stage, k - 1], srecv.at[stage, k - 1], at.along(stage, k)) for k in range(1, n)]

    red.advance(0)
    slots[0, at.coord[0]] = small[...]
    for c in small_copies(0):
        c.start()
    for stage in range(1, 8):
        red.advance(stage)
        if stage < 5:
            for c in small_copies(stage - 1):
                c.wait()
            if stage < 4:
                val = functools.reduce(jnp.add, [slots[stage - 1, k] for k in range(n)])
                if stage < 3:
                    slots[stage, at.coord[stage]] = val
                else:
                    pair[at.core] = val
                for c in small_copies(stage):
                    c.start()
            else:
                small_out[...] = pair[0] + pair[1]


def all_reduce_late(n, cid, stack, small):
    form = Stack(stack.shape, n)
    vm = pl.BlockSpec(memory_space=pltpu.VMEM)
    sem = pltpu.SemaphoreType.DMA
    return pl.pallas_call(
        functools.partial(reduce_kernel, n, form),
        out_shape=(jax.ShapeDtypeStruct(stack.shape, F32), jax.ShapeDtypeStruct(small.shape, F32)),
        in_specs=[pl.BlockSpec(memory_space=pl.ANY), vm], out_specs=(vm, vm), name="reduce_late",
        scratch_shapes=[pltpu.VMEM((3, n) + small.shape, F32), pltpu.VMEM((2,) + small.shape, F32),
                        sem((4, n - 1)), sem((4, n - 1))] + Reduce.scratch(n, form),
        compiler_params=pltpu.CompilerParams(collective_id=cid, has_side_effects=True, vmem_limit_bytes=VMEM_LIMIT),
    )(stack, small)


def solution(mesh):
    group = mesh.shape['seq']
    n = round((group // 2) ** (1 / 3))
    row_spec = P(('data', 'seq'), None)
    weight_spec = P()
    part_vec = P('data')
    part_mat = P('data', None)
    part_cube = P('data', None, None)

    def by_part(a):
        return jnp.transpose(a.reshape(a.shape[0], PARTS, TILE), (1, 0, 2))

    def by_row(a):
        return jnp.transpose(a, (1, 0, 2)).reshape(a.shape[1], PARTS * TILE)

    def device_step(dec_in, memory, mem_len, grad_out, norm_attn, wq_cross, wk_cross, wv_cross, wo_cross, norm_mlp, w_gate, w_up, w_down):
        q_rows, model_dim = dec_in.shape
        m_rows = memory.shape[0]
        heads, head_dim = wq_cross.shape[1], wq_cross.shape[2]
        wide = heads * head_dim
        wq, wk, wv = (w.reshape(model_dim, wide) for w in (wq_cross, wk_cross, wv_cross))
        wo = wo_cross.reshape(wide, model_dim)
        keep, piece, size = m_rows * 3 // 4, m_rows // 4, group // 4
        me = lax.axis_index('seq')
        slot = jnp.arange(keep)
        own_pos = me * m_rows + slot
        given_pos = ((slot // piece) * size + me % size) * m_rows + keep + slot % piece
        mem_pos = jnp.where(me // size == 3, given_pos, own_pos)
        bias = jnp.where(mem_pos < mem_len[0], 0.0, NEG)[:, None]
        lane = jnp.arange(TILE)[None, :] % head_dim
        flag = jnp.where((lane >= 1) & (lane <= 3), 1.0, 0.0)
        aux_k = jnp.where(lane == 0, bias, flag).astype(BF16)
        aux_v = jnp.broadcast_to(flag, aux_k.shape).astype(BF16)

        x_in = dec_in.astype(F32)
        normed_f, norm_pull = jax.vjp(rms_norm, x_in, norm_attn.astype(F32))
        normed = normed_f.astype(BF16)
        local_query = jnp.dot(normed, wq, preferred_element_type=F32).astype(BF16) * jnp.asarray(head_dim ** -0.5, BF16)
        q_t, kept, k_aug, v_aug, k_t, v_t = prepare(n, 0, by_part(local_query), memory, wk, wv, aux_k, aux_v)
        out_parts, lse = attention_fwd(n, 1, q_t, k_aug, v_t)
        attended_f = by_row(out_parts)

        attended = attended_f.astype(BF16)
        hidden_f = x_in + jnp.dot(attended, wo, preferred_element_type=F32)
        hidden = hidden_f.astype(BF16)
        normed_mlp_f, mlp_norm_pull = jax.vjp(rms_norm, hidden.astype(F32), norm_mlp.astype(F32))
        normed_mlp = normed_mlp_f.astype(BF16)
        gate_pre = jnp.dot(normed_mlp, w_gate, preferred_element_type=F32)
        up_pre = jnp.dot(normed_mlp, w_up, preferred_element_type=F32)
        mlp_f, gated_pull = jax.vjp(gated_unit, gate_pre, up_pre)
        mlp_act = mlp_f.astype(BF16)

        grad_top = grad_out.astype(BF16)
        g_down = jnp.einsum('qf,qd->fd', mlp_act, grad_top, preferred_element_type=F32)
        grad_act = jnp.einsum('qd,fd->qf', grad_top, w_down, preferred_element_type=F32)
        grad_gate, grad_up = gated_pull(grad_act)
        grad_gate_b = grad_gate.astype(BF16)
        grad_up_b = grad_up.astype(BF16)
        g_gate = jnp.einsum('qd,qf->df', normed_mlp, grad_gate_b, preferred_element_type=F32)
        g_up = jnp.einsum('qd,qf->df', normed_mlp, grad_up_b, preferred_element_type=F32)
        grad_normed_mlp = (jnp.einsum('qf,df->qd', grad_gate_b, w_gate, preferred_element_type=F32)
                           + jnp.einsum('qf,df->qd', grad_up_b, w_up, preferred_element_type=F32))
        grad_hidden_norm, g_norm_mlp = mlp_norm_pull(grad_normed_mlp)
        grad_hidden = grad_out + grad_hidden_norm
        grad_hidden_b = grad_hidden.astype(BF16)
        g_wo = jnp.einsum('qe,qd->ed', attended, grad_hidden_b, preferred_element_type=F32)
        grad_attended = jnp.einsum('qd,ed->qe', grad_hidden_b, wo, preferred_element_type=F32)
        delta = jnp.sum((grad_attended * attended_f).reshape(q_rows, PARTS, 2, head_dim), axis=-1)
        delta = jnp.transpose(delta, (1, 0, 2))
        stats_in = jnp.concatenate([lse[:, :, 0:2], delta, jnp.zeros((PARTS, q_rows, TILE - 4), F32)], axis=2)
        do_t, stats = all_gather_t(n, 2, by_part(grad_attended.astype(BF16)), stats_in)

        dq_parts, dk_b, dv_b, g_mem, g_gate, g_up, g_down = attention_bwd(
            n, 3, m_rows, q_t, do_t, stats, k_aug, v_aug, k_t, wk, wv, (g_gate, g_up), (g_down,))
        grad_query_b = by_row(dq_parts).astype(BF16)

        g_wq = jnp.einsum('td,te->de', normed, grad_query_b, preferred_element_type=F32)
        grad_normed = jnp.einsum('te,de->td', grad_query_b, wq, preferred_element_type=F32)
        grad_x_norm, g_norm_attn = norm_pull(grad_normed)
        g_dec = grad_hidden + grad_x_norm
        g_wk = jnp.einsum('td,te->de', kept, dk_b, preferred_element_type=F32)
        g_wv = jnp.einsum('td,te->de', kept, dv_b, preferred_element_type=F32)
        small = jnp.concatenate([g_norm_attn[None], g_norm_mlp[None], jnp.zeros((6, model_dim), F32)], axis=0)
        late, small = all_reduce_late(n, 4, jnp.stack([g_wq, g_wk, g_wv, g_wo]), small)
        cube = (model_dim, heads, head_dim)
        g_wq, g_wk, g_wv = late[0], late[1], late[2]
        g_wo = late[3].reshape(heads, head_dim, model_dim)
        g_norm_attn, g_norm_mlp = small[0], small[1]
        return (g_dec, g_mem, g_norm_attn, g_wq.reshape(cube), g_wk.reshape(cube), g_wv.reshape(cube),
                g_wo, g_norm_mlp, g_gate, g_up, g_down)

    return jax.shard_map(device_step, mesh=mesh,
                         in_specs=(row_spec, row_spec, part_vec, row_spec) + (weight_spec,) * 9,
                         out_specs=(row_spec, row_spec, part_vec, part_cube, part_cube, part_cube, part_cube, part_vec, part_mat, part_mat, part_mat),
                         check_vma=False)
```

```python
import functools

import jax
import jax.numpy as jnp
from jax import lax
from jax.experimental import pallas as pl
from jax.experimental.pallas import tpu as pltpu
from jax.sharding import PartitionSpec as P

F32 = jnp.float32
BF16 = jnp.bfloat16
MESH = pl.DeviceIdType.MESH
VMEM_LIMIT = 62 * 1024 * 1024
NEG = -1e30
ORDERS = ((0, 1, 2), (2, 0, 1), (1, 2, 0))
PARTS = 3
TILE = 128
HALF = TILE // 2
ALL = slice(None)


def rms_norm(tensor, gain):
    mean_sq = jnp.mean(tensor * tensor, axis=-1, keepdims=True)
    return tensor * lax.rsqrt(mean_sq + 1e-6) * gain


def gated_unit(gate_pre, up_pre):
    return jax.nn.silu(gate_pre) * up_pre


class Place:
    def __init__(self, n):
        self.n = n
        me = lax.axis_index("seq")
        self.me = me
        self.core = lax.rem(me, 2)
        x = lax.rem(me // 2, n)
        y = lax.rem(me // (2 * n), n)
        z = me // (2 * n * n)
        self.coord = (z, y, x)
        self.stride = (2 * n * n, 2 * n, 2)

    def along(self, axis, k):
        here = self.coord[axis]
        return self.me + (lax.rem(here + k, self.n) - here) * self.stride[axis]

    def other_core(self):
        return self.me + 1 - 2 * self.core

    def quarter(self):
        return self.me // (self.n ** 3 // 2)

    def mate(self, q):
        size = self.n ** 3 // 2
        return q * size + lax.rem(self.me, size)

    def to(self, k):
        return {"seq": k}

    def barrier(self):
        sem = pltpu.get_barrier_semaphore()
        for axis in range(3):
            for k in range(1, self.n):
                pl.semaphore_signal(sem, inc=1, device_id=self.to(self.along(axis, k)), device_id_type=MESH)
        pl.semaphore_signal(sem, inc=1, device_id=self.to(self.other_core()), device_id_type=MESH)
        extra = 0
        if self.n < 4:
            for k in range(1, 4):
                pl.semaphore_signal(sem, inc=1, device_id=self.to(self.mate(lax.rem(self.quarter() + k, 4))), device_id_type=MESH)
            extra = 3
        pl.semaphore_wait(sem, 3 * (self.n - 1) + 1 + extra)


def rcopy(src, dst, send, recv, device):
    return pltpu.make_async_remote_copy(src_ref=src, dst_ref=dst, send_sem=send, recv_sem=recv,
                                        device_id={"seq": device}, device_id_type=MESH)


def lanes(start, size):
    return pl.ds(pl.multiple_of(start, TILE), size)


def rows_of(start, size):
    return pl.ds(pl.multiple_of(start, 8), size)


class Gather:
    def __init__(self, n, at, src, full, bufs):
        self.n, self.at, self.src, self.full = n, at, src, full
        self.rows, self.send, self.recv, self.csend, self.crecv = bufs
        self.copies = {}

    @staticmethod
    def scratch(n, dtype):
        sem = pltpu.SemaphoreType.DMA
        return [pltpu.VMEM((PARTS, TILE, TILE), dtype), sem((3, PARTS, n - 1)), sem((3, PARTS, n - 1)),
                sem((PARTS,)), sem((PARTS,))]

    def begin(self):
        n, at = self.n, self.at
        r = TILE // n
        for p in range(PARTS):
            a3 = ORDERS[p][2]
            mine = rows_of(at.coord[a3] * r, r)
            for k in range(1, n):
                c = rcopy(self.src.at[p], self.rows.at[p, mine, :], self.send.at[0, p, k - 1], self.recv.at[0, p, k - 1], at.along(a3, k))
                c.start()
                self.copies[0, p, k] = c
            self.rows[p, mine, :] = self.src[p]

    def turn(self):
        at, n = self.at, self.n
        for p in range(PARTS):
            a1, a2, _ = ORDERS[p]
            for k in range(1, n):
                self.copies[0, p, k].wait()
            block = self.rows[p].astype(F32).T
            base = ((at.core * n + at.coord[a1]) * n + at.coord[a2]) * TILE
            self.full[p, :, lanes(base, TILE)] = block[:self.full.shape[1]].astype(self.full.dtype)

    def place(self, stage, p, back):
        at, n = self.at, self.n
        a1, a2, _ = ORDERS[p]
        if stage == 1:
            spot = lax.rem(at.coord[a2] + n - back, n)
            return a2, lanes(((at.core * n + at.coord[a1]) * n + spot) * TILE, TILE)
        spot = lax.rem(at.coord[a1] + n - back, n)
        return a1, lanes((at.core * n + spot) * n * TILE, n * TILE)

    def spread(self, stage):
        n, at = self.n, self.at
        for p in range(PARTS):
            axis, cols = self.place(stage, p, 0)
            view = self.full.at[p, :, cols]
            for k in range(1, n):
                c = rcopy(view, view, self.send.at[stage, p, k - 1], self.recv.at[stage, p, k - 1], at.along(axis, k))
                c.start()
                self.copies[stage, p, k] = c

    def settle(self, stage):
        n = self.n
        for p in range(PARTS):
            for k in range(1, n):
                self.copies[stage, p, k].wait()

    def swap(self):
        n, at = self.n, self.at
        width = n * n * TILE
        out = []
        for p in range(PARTS):
            view = self.full.at[p, :, lanes(at.core * width, width)]
            c = rcopy(view, view, self.csend.at[p], self.crecv.at[p], at.other_core())
            c.start()
            out.append(c)
        return out


GATHER_REFS = 5


def run_gathers(gathers, between=None):
    for g in gathers:
        g.begin()
    for g in gathers:
        g.turn()
        g.spread(1)
    for g in gathers:
        g.settle(1)
        g.spread(2)
    if between is not None:
        between()
    final = []
    for g in gathers:
        g.settle(2)
        final += g.swap()
    for c in final:
        c.wait()


def merge(blocks, rows_axis):
    take = (lambda b, i, j: b[i:j]) if rows_axis == 0 else (lambda b, i, j: b[:, i:j])
    outs, maxes, sums = [], [], []
    for h in range(2):
        ms = [take(b, TILE + h, TILE + h + 1) for b in blocks]
        m = functools.reduce(jnp.maximum, ms)
        ws = [jnp.exp(v - m) for v in ms]
        o = sum(take(b, HALF * h, HALF * h + HALF) * w for b, w in zip(blocks, ws))
        l = sum(take(b, TILE + 2 + h, TILE + 3 + h) * w for b, w in zip(blocks, ws))
        outs.append(o)
        maxes.append(m)
        sums.append(l)
    return outs, maxes + sums


class Scatter:
    def __init__(self, n, at, with_stats, bufs):
        self.n, self.at, self.with_stats = n, at, with_stats
        (self.far, self.near, self.buf0, self.buf1, self.acc1, self.buf2, self.acc2, self.buf3, self.pass_buf,
         self.csend, self.crecv, self.send, self.recv, self.psend, self.precv) = bufs
        self.relay = n == 4
        self.step = n * TILE

    @staticmethod
    def scratch(n, rows, wide):
        sem = pltpu.SemaphoreType.DMA
        half = n * n * TILE
        r = TILE // n
        return [
            pltpu.VMEM((PARTS, rows, half), F32), pltpu.VMEM((PARTS, rows, half), F32), pltpu.VMEM((PARTS, rows, half), F32),
            pltpu.VMEM((PARTS, n - 1, rows, n * TILE), F32), pltpu.VMEM((PARTS, rows, n * TILE), F32),
            pltpu.VMEM((PARTS, n - 1, rows, TILE), F32), pltpu.VMEM((PARTS, TILE, wide), F32),
            pltpu.VMEM((PARTS, n - 1, r, wide), F32), pltpu.VMEM((PARTS, 2, rows, n * HALF), F32),
            sem((PARTS, n)), sem((PARTS, n)), sem((3, PARTS, n - 1)), sem((3, PARTS, n - 1)), sem((PARTS, 2)), sem((PARTS, 2)),
        ]

    def visit(self, i):
        if self.relay:
            return jnp.where(i == 0, 2, jnp.where(i == 1, 3, jnp.where(i == 2, 1, 0)))
        return self.n - 1 - i

    def pass_copy(self, p, i):
        width = self.step // 2
        return rcopy(self.near.at[p, :, lanes(self.chunk(p, 2) * self.step + i * width, width)], self.pass_buf.at[p, i],
                     self.psend.at[p, i], self.precv.at[p, i], self.at.along(ORDERS[p][0], 1 + 2 * i))

    def take_over(self, p, i):
        self.pass_copy(p, i).wait_recv()
        width = self.step // 2
        for j in range(width // TILE):
            col = lanes(self.chunk(p, 1 + 2 * i) * self.step + i * width + j * TILE, TILE)
            self.combine(self.near, p, col, [self.near[p, :, col], self.pass_buf[p, i, :, j * TILE:(j + 1) * TILE]])
        self.first_copy(p, 1 + 2 * i).start()

    def chunk(self, p, k):
        return lax.rem(self.at.coord[ORDERS[p][0]] + k, self.n)

    def combine(self, dst, p, col, vals):
        if self.with_stats:
            outs, stats = merge(vals, 0)
            dst[p, 0:HALF, col] = outs[0]
            dst[p, HALF:TILE, col] = outs[1]
            dst[p, TILE:TILE + 8, col] = jnp.concatenate(stats + [jnp.zeros_like(stats[0])] * 4, axis=0)
        else:
            dst[p, :, col] = functools.reduce(jnp.add, vals)

    def core_copy(self, p, k):
        view = (p, ALL, lanes(self.chunk(p, k) * self.step, self.step))
        return rcopy(self.far.at[view], self.buf0.at[view], self.csend.at[p, k], self.crecv.at[p, k], self.at.other_core())

    def first_copy(self, p, k):
        return rcopy(self.near.at[p, :, lanes(self.chunk(p, k) * self.step, self.step)], self.buf1.at[p, k - 1],
                     self.send.at[0, p, k - 1], self.recv.at[0, p, k - 1], self.at.along(ORDERS[p][0], k))

    def far_done(self, k):
        for p in range(PARTS):
            self.core_copy(p, k).start()

    def near_done(self, k):
        for p in range(PARTS):
            self.core_copy(p, k).wait()

            def fold(j, _, p=p):
                col = lanes(self.chunk(p, k) * self.step + j * TILE, TILE)
                self.combine(self.near, p, col, [self.near[p, :, col], self.buf0[p, :, col]])
                return 0

            lax.fori_loop(0, self.n, fold, 0)

            if self.relay:
                @pl.when(k == 2)
                def _(p=p):
                    for i in range(2):
                        self.pass_copy(p, i).start()

                for i in range(2):
                    @pl.when(k == 1 + 2 * i)
                    def _(p=p, i=i):
                        self.take_over(p, i)
            else:
                @pl.when(k > 0)
                def _(p=p):
                    self.first_copy(p, k).start()

    def finish(self, o_ref, st_ref=None):
        n, at = self.n, self.at
        r = TILE // n
        copies = {}
        for p in range(PARTS):
            a1, a2, _ = ORDERS[p]
            direct = (1, 3) if self.relay else range(1, n)
            for k in direct:
                self.first_copy(p, k).wait()
            if self.relay:
                for i in range(2):
                    self.pass_copy(p, i).wait_send()
            mine = at.coord[a1] * n * TILE
            for j in range(n):
                col = slice(j * TILE, (j + 1) * TILE)
                self.combine(self.acc1, p, pl.ds(j * TILE, TILE),
                             [self.near[p, :, lanes(mine + j * TILE, TILE)]] + [self.buf1[p, k - 1, :, col] for k in direct])
            for k in range(1, n):
                there = lax.rem(at.coord[a2] + k, n)
                c = rcopy(self.acc1.at[p, :, lanes(there * TILE, TILE)], self.buf2.at[p, k - 1],
                          self.send.at[1, p, k - 1], self.recv.at[1, p, k - 1], at.along(a2, k))
                c.start()
                copies[1, p, k] = c
        for p in range(PARTS):
            _, a2, a3 = ORDERS[p]
            for k in range(1, n):
                copies[1, p, k].wait()
            blocks = [self.acc1[p, :, lanes(at.coord[a2] * TILE, TILE)]] + [self.buf2[p, k] for k in range(n - 1)]
            if self.with_stats:
                outs, stats = merge(blocks, 0)
                self.acc2[p, :, 0:TILE] = jnp.concatenate(outs, axis=0).T
                tail = jnp.concatenate(stats + [jnp.zeros((TILE - 4, TILE), F32)], axis=0)
                self.acc2[p, :, TILE:2 * TILE] = tail.T
            else:
                self.acc2[p] = functools.reduce(jnp.add, blocks).T
            for k in range(1, n):
                there = lax.rem(at.coord[a3] + k, n)
                c = rcopy(self.acc2.at[p, pl.ds(pl.multiple_of(there * r, r), r), :], self.buf3.at[p, k - 1],
                          self.send.at[2, p, k - 1], self.recv.at[2, p, k - 1], at.along(a3, k))
                c.start()
                copies[2, p, k] = c
        for p in range(PARTS):
            a3 = ORDERS[p][2]
            for k in range(1, n):
                copies[2, p, k].wait()
            blocks = [self.acc2[p, pl.ds(pl.multiple_of(at.coord[a3] * r, r), r), :]] + [self.buf3[p, k] for k in range(n - 1)]
            if self.with_stats:
                outs, (m0, m1, l0, l1) = merge(blocks, 1)
                o_ref[p] = jnp.concatenate([outs[0] / l0, outs[1] / l1], axis=1)
                col = lax.broadcasted_iota(jnp.int32, (r, TILE), 1)
                st_ref[p] = jnp.where(col == 0, m0 + jnp.log(l0), jnp.where(col == 1, m1 + jnp.log(l1), 0.0))
            else:
                o_ref[p] = functools.reduce(jnp.add, blocks)


class Wide:
    def __init__(self, shape, n):
        self.part, self.cols = shape[0] // PARTS, shape[1]
        self.r1, self.r2, self.c3 = self.part // 2, self.part // 2 // n, shape[1] // n
        self.l1, self.l2, self.l3 = (self.r1, self.cols), (self.r2, self.cols), (self.r2, self.c3)

    def row(self, p, c, a):
        return self.part * p + self.r1 * c + self.r2 * a

    def full1(self, p, c):
        return rows_of(self.part * p + self.r1 * c, self.r1), ALL

    def full2(self, p, c, a):
        return rows_of(self.row(p, c, a), self.r2), ALL

    def half2(self, p, c, a, i):
        size = self.r2 // 2
        return rows_of(self.row(p, c, a) + i * size, size), ALL

    def hin1(self, a, i):
        size = self.r2 // 2
        return rows_of(self.r2 * a + i * size, size), ALL

    def full3(self, p, c, a, b):
        return rows_of(self.row(p, c, a), self.r2), lanes(self.c3 * b, self.c3)

    def in1(self, a):
        return rows_of(self.r2 * a, self.r2), ALL

    def in2(self, b):
        return ALL, lanes(self.c3 * b, self.c3)


class Tall(Wide):
    def __init__(self, shape, n):
        super().__init__(shape, n)
        self.r3 = self.r2 // n
        self.l3 = (self.r3, self.cols)

    def full3(self, p, c, a, b):
        return rows_of(self.row(p, c, a) + self.r3 * b, self.r3), ALL

    def in2(self, b):
        return rows_of(self.r3 * b, self.r3), ALL


class Stack:
    def __init__(self, shape, n):
        w, rows, cols = shape
        self.part, self.w3 = rows // PARTS, w // n
        self.r1, self.r2 = self.part // 2, self.part // 2 // n
        self.l1, self.l2, self.l3 = (w, self.r1, cols), (w, self.r2, cols), (self.w3, self.r2, cols)

    def full1(self, p, c):
        return ALL, rows_of(self.part * p + self.r1 * c, self.r1), ALL

    def row(self, p, c, a):
        return self.part * p + self.r1 * c + self.r2 * a

    def full2(self, p, c, a):
        return ALL, rows_of(self.row(p, c, a), self.r2), ALL

    def full3(self, p, c, a, b):
        return pl.ds(self.w3 * b, self.w3), rows_of(self.row(p, c, a), self.r2), ALL

    def in1(self, a):
        return ALL, rows_of(self.r2 * a, self.r2), ALL

    def in2(self, b):
        return pl.ds(self.w3 * b, self.w3), ALL, ALL


class Reduce:
    STAGES = ("core", "pass", "first", "second", "third", "back2", "back1", "relay", "swap")

    def __init__(self, n, at, form, src, out, bufs, relay):
        self.n, self.at, self.form, self.src, self.out = n, at, form, src, out
        self.relay = relay and n == 4
        self.stages = [v for v in self.STAGES if self.relay or v not in ("pass", "relay")]
        (self.own, self.buf0, self.buf1, self.acc1, self.buf2, self.buf3, self.lsem,
         self.csend, self.crecv, self.send, self.recv) = bufs

    @staticmethod
    def scratch(n, form):
        sem = pltpu.SemaphoreType.DMA
        kinds = len(Reduce.STAGES)
        return [
            pltpu.VMEM((PARTS,) + form.l1, F32), pltpu.VMEM((PARTS,) + form.l1, F32),
            pltpu.VMEM((PARTS, n - 1) + form.l2, F32), pltpu.VMEM((PARTS,) + form.l2, F32),
            pltpu.VMEM((PARTS, n - 1) + form.l3, F32), pltpu.VMEM((PARTS, n) + form.l3, F32),
            sem((PARTS,)), sem((PARTS,)), sem((PARTS,)), sem((kinds, PARTS, n - 1)), sem((kinds, PARTS, n - 1)),
        ]

    def spots(self, p):
        return [self.at.coord[a] for a in ORDERS[p]]

    def hold(self, p, i):
        return self.buf1.at[(p, 1)].at[self.form.hin1(0, i)]

    def copies(self, stage, p):
        at, n, form = self.at, self.n, self.form
        A1, A2, A3 = self.spots(p)
        a1, a2, a3 = ORDERS[p]
        c = at.core
        if stage == "core":
            return [rcopy(self.src.at[form.full1(p, 1 - c)], self.buf0.at[p], self.csend.at[p], self.crecv.at[p], at.other_core()),
                    pltpu.make_async_copy(self.src.at[form.full1(p, c)], self.own.at[p], self.lsem.at[p])]
        kind = self.STAGES.index(stage)
        out = []

        def add(src, dst, axis, k):
            out.append(rcopy(src, dst, self.send.at[kind, p, k - 1], self.recv.at[kind, p, k - 1], at.along(axis, k)))

        if stage == "swap":
            view = self.out.at[form.full1(p, c)]
            return [rcopy(view, view, self.send.at[kind, p, 0], self.recv.at[kind, p, 0], at.other_core())]
        steps = range(1, n)
        near = (1, n - 1) if self.relay else steps
        if stage == "pass":
            for i, k in enumerate(near):
                add(self.own.at[p].at[form.hin1(lax.rem(A1 + 2, n), i)], self.hold(p, i), a1, k)
        elif stage == "first":
            for k in near:
                add(self.own.at[p].at[form.in1(lax.rem(A1 + k, n))], self.buf1.at[p, k - 1], a1, k)
        elif stage == "second":
            for k in steps:
                add(self.acc1.at[p].at[form.in2(lax.rem(A2 + k, n))], self.buf2.at[p, k - 1], a2, k)
        elif stage == "third":
            for k in steps:
                add(self.buf3.at[p, A3], self.buf3.at[p, A3], a3, k)
        elif stage == "back2":
            view = self.out.at[form.full3(p, c, A1, A2)]
            for k in steps:
                add(view, view, a2, k)
        elif stage == "back1":
            view = self.out.at[form.full2(p, c, A1)]
            for k in near:
                add(view, view, a1, k)
        else:
            for i, k in enumerate(near):
                view = self.out.at[form.half2(p, c, lax.rem(A1 + n - k, n), i)]
                add(view, view, a1, k)
        return out

    def advance(self, step):
        form, n = self.form, self.n
        stage = self.stages[step] if step < len(self.stages) else None
        before = self.stages[step - 1]
        near = (0, n - 2) if self.relay else range(n - 1)
        for p in range(PARTS):
            A1, A2, A3 = self.spots(p)
            if step:
                for c in self.copies(before, p):
                    c.wait()
            own = self.own.at[p]
            if before == "core":
                own[...] += self.buf0[p]
            elif before == "pass":
                for i, k in enumerate((1, n - 1)):
                    own[form.hin1(lax.rem(A1 + k, n), i)] += self.hold(p, i)[...]
            elif before == "first":
                self.acc1[p] = functools.reduce(jnp.add, [own[form.in1(A1)]] + [self.buf1[p, k] for k in near])
            elif before == "second":
                self.buf3[p, A3] = functools.reduce(jnp.add, [self.acc1[(p,) + form.in2(A2)]] + [self.buf2[p, k] for k in range(n - 1)])
            elif before == "third":
                self.out[form.full3(p, self.at.core, A1, A2)] = functools.reduce(jnp.add, [self.buf3[p, k] for k in range(n)])
            if stage:
                for c in self.copies(stage, p):
                    c.start()

    def finish(self, step):
        for i in range(step, len(self.stages) + 1):
            self.advance(i)


REDUCE_REFS = 11


QB = 256


def aux_rows(rows, width):
    pad = jnp.zeros((64 - len(rows), width), F32)
    return jnp.concatenate(list(rows) + [pad], axis=0).astype(BF16)


def split3(v):
    hi = v.astype(BF16).astype(F32)
    mid = (v - hi).astype(BF16).astype(F32)
    lo = (v - hi - mid).astype(BF16).astype(F32)
    return [hi, mid, lo]


def blocks_loop(n, scatter, blocks, events):
    per = n * TILE // QB
    at = scatter.at

    def body(t, _):
        u = t // per
        k = scatter.visit(u // 2)
        near = lax.rem(u, 2)
        half = jnp.where(near == 1, at.core, 1 - at.core)
        inside = [scatter.chunk(p, k) * (n * TILE) + lax.rem(t, per) * QB for p in range(PARTS)]
        srcs = [pl.ds(pl.multiple_of(half * (n * n * TILE) + i, QB), QB) for i in inside]
        blocks(srcs, near, [pl.ds(pl.multiple_of(i, QB), QB) for i in inside])
        last = lax.rem(t, per) == per - 1

        @pl.when(last & (near == 0))
        def _():
            scatter.far_done(k)

        @pl.when(last & (near == 1))
        def _():
            scatter.near_done(k)

        for when, action in events:
            @pl.when(t == when)
            def _(action=action):
                action()
        return 0

    lax.fori_loop(0, 2 * n * per, body, 0)


def put(scatter, near, p, row, col, val):
    @pl.when(near == 1)
    def _():
        scatter.near[p, row, col] = val

    @pl.when(near == 0)
    def _():
        scatter.far[p, row, col] = val


def head(j):
    return slice(HALF * j, HALF * (j + 1))


def beside(j, block, other):
    return jnp.concatenate([block, other] if j == 0 else [other, block], axis=0)


def shrink(op, v, rows):
    while v.shape[0] > rows:
        h = v.shape[0] // 2
        v = op(v[:h], v[h:])
    return v


KC = 256


def fwd_kernel(n, x_ref, mem_ref, wk_ref, wv_ref, auxk_ref, auxv_ref, o_ref, st_ref, *refs):
    saved, refs = refs[:SAVED], refs[SAVED:]
    kept, refs = refs[:SAVED], refs[SAVED:]
    q_ref, keep_ref, k_ref, v_ref, kt_ref = kept
    vt_ref, s_buf, msend, mrecv, save_sem, *refs = refs
    gbufs, bufs = refs[:GATHER_REFS], refs[GATHER_REFS:]
    keys = k_ref.shape[1]
    piece = keys // 3
    kc = min(KC, piece)
    chunks = keys // kc
    at = Place(n)
    at.barrier()
    quarter = at.quarter()

    def donate(q):
        return rcopy(mem_ref.at[pl.ds(keys, piece), :], keep_ref.at[pl.ds(q * piece, piece), :], msend, mrecv.at[q], at.mate(3))

    def saves():
        return [pltpu.make_async_copy(a, b, save_sem.at[i]) for i, (a, b) in enumerate(zip(kept, saved))]

    for q in range(3):
        @pl.when(quarter == q)
        def _(q=q):
            donate(q).start()

    def project():
        @pl.when(quarter < 3)
        def _():
            keep_ref[...] = mem_ref[0:keys, :]

        @pl.when(quarter == 3)
        def _():
            for q in range(3):
                donate(q).wait_recv()

        low = lax.broadcasted_iota(jnp.int32, (piece, TILE), 1) < HALF
        for i in range(3):
            rows = pl.ds(i * piece, piece)
            m = keep_ref[rows, :]
            for w_ref, aux_ref, a_ref, t_ref in ((wk_ref, auxk_ref, k_ref, kt_ref), (wv_ref, auxv_ref, v_ref, vt_ref)):
                aux = aux_ref[rows, :].astype(F32)
                for p in range(PARTS):
                    b = jnp.dot(m, w_ref[:, p * TILE:(p + 1) * TILE], preferred_element_type=F32).astype(BF16).astype(F32)
                    a_ref[2 * p, rows, :] = jnp.where(low, b, aux).astype(BF16)
                    a_ref[2 * p + 1, rows, :] = jnp.where(low, aux, b).astype(BF16)
                    t_ref[p, :, rows] = b.T.astype(BF16)

    run_gathers([Gather(n, at, x_ref, q_ref, gbufs)], project)
    for q in range(3):
        @pl.when(quarter == q)
        def _(q=q):
            donate(q).wait_send()
    for c in saves():
        c.start()
    aux = aux_rows([jnp.ones((1, QB), F32)], QB)
    scatter = Scatter(n, at, True, bufs)

    def blocks(srcs, near, dsts):
        heads = [(p, j) for p in range(PARTS) for j in range(2)]

        def score(i, c, run):
            p, j = heads[i]
            qa = beside(j, q_ref[p, head(j), srcs[p]], aux)
            s = jnp.dot(k_ref[i, c * kc:(c + 1) * kc, :], qa, preferred_element_type=F32)
            s_buf[i % 2, c * kc:(c + 1) * kc, :] = s
            top = shrink(jnp.maximum, s, 16)
            return top if run is None else jnp.maximum(run, top)

        run = None
        for c in range(chunks):
            run = score(0, c, run)
        done = []
        for i, (p, j) in enumerate(heads):
            m = jnp.max(run, axis=0, keepdims=True)
            run, total, out = None, None, None
            for c in range(chunks):
                if i + 1 < len(heads):
                    run = score(i + 1, c, run)
                e = jnp.exp(s_buf[i % 2, c * kc:(c + 1) * kc, :] - m)
                part = shrink(jnp.add, e, 16)
                total = part if total is None else total + part
                o = jnp.dot(vt_ref[p, head(j), c * kc:(c + 1) * kc], e.astype(BF16), preferred_element_type=F32)
                out = o if out is None else out + o
            done.append((out, m, jnp.sum(total, axis=0, keepdims=True)))
            if j == 1:
                (o0, m0, l0), (o1, m1, l1) = done[-2:]
                val = jnp.concatenate([o0, o1, m0, m1, l0, l1, jnp.zeros((4, QB), F32)], axis=0)
                put(scatter, near, p, ALL, dsts[p], val)

    blocks_loop(n, scatter, blocks, [])
    scatter.finish(o_ref, st_ref)
    for c in saves():
        c.wait()


SAVED = 5


def attention_fwd(n, cid, rows, memory, wk, wv, aux_k, aux_v):
    total = 2 * n * n * TILE
    r = TILE // n
    keys, dim = aux_k.shape[0], memory.shape[1]
    vm, hbm = pl.BlockSpec(memory_space=pltpu.VMEM), pl.BlockSpec(memory_space=pl.ANY)
    sem = pltpu.SemaphoreType.DMA
    shapes = ((PARTS, TILE, total), (keys, dim), (2 * PARTS, keys, TILE), (2 * PARTS, keys, TILE), (PARTS, TILE, keys))
    scratch = [pltpu.VMEM(v, BF16) for v in shapes] + [pltpu.VMEM(shapes[-1], BF16), pltpu.VMEM((2, keys, QB), F32),
                                                       sem(()), sem((3,)), sem((SAVED,))]
    return pl.pallas_call(
        functools.partial(fwd_kernel, n),
        out_shape=(jax.ShapeDtypeStruct((PARTS, r, TILE), F32),) * 2 + tuple(jax.ShapeDtypeStruct(v, BF16) for v in shapes),
        in_specs=[vm] * 6, out_specs=(vm,) * 2 + (hbm,) * SAVED, name="attention_fwd",
        scratch_shapes=scratch + Gather.scratch(n, BF16) + Scatter.scratch(n, TILE + 8, 2 * TILE),
        compiler_params=pltpu.CompilerParams(collective_id=cid, has_side_effects=True, vmem_limit_bytes=VMEM_LIMIT),
    )(rows, memory, wk, wv, aux_k, aux_v)


SCATTER_REFS = 15


def bwd_kernel(n, forms, q_ref, x_ref, s_ref, k_ref, v_ref, kt_ref, *refs):
    count = len(forms)
    grads, refs = refs[:count], refs[count:]
    dq_ref, dk_ref, dv_ref, *refs = refs
    sums, refs = refs[:count], refs[count:]
    do_ref, st_ref, dk_acc, dv_acc, *refs = refs
    xbufs, refs = refs[:GATHER_REFS], refs[GATHER_REFS:]
    sbufs, refs = refs[:GATHER_REFS], refs[GATHER_REFS:]
    bufs, refs = refs[:SCATTER_REFS], refs[SCATTER_REFS:]
    one = jnp.ones((1, QB), F32)
    zero = jnp.zeros((1, QB), F32)
    blank = jnp.zeros((HALF, QB), BF16)
    nt = (((1,), (1,)), ((), ()))
    at = Place(n)
    at.barrier()
    scatter = Scatter(n, at, False, bufs)
    reduces = [Reduce(n, at, form, grads[i], sums[i], refs[REDUCE_REFS * i:REDUCE_REFS * (i + 1)], True)
               for i, form in enumerate(forms)]

    def advance(stage):
        for red in reduces:
            red.advance(stage)

    gathers = [Gather(n, at, s_ref, st_ref, sbufs), Gather(n, at, x_ref, do_ref, xbufs)]
    for g in gathers:
        g.begin()
    advance(0)
    dk_acc[...] = jnp.zeros_like(dk_acc)
    dv_acc[...] = jnp.zeros_like(dv_acc)
    for g in gathers:
        g.turn()
        g.spread(1)
    for g in gathers:
        g.settle(1)
        g.spread(2)
    advance(1)
    final = []
    for g in gathers:
        g.settle(2)
        final += g.swap()
    for c in final:
        c.wait()

    def block(p, src, near, dst):
        probs, dscores, dos, qs, dqs = [], [], [], [], []
        for j in range(2):
            qh = q_ref[p, head(j), src]
            doh = do_ref[p, head(j), src]
            lse = st_ref[p, j:j + 1, src]
            delta = st_ref[p, 2 + j:3 + j, src]
            qa = beside(j, qh, aux_rows([one] + split3(-lse), QB))
            da = beside(j, doh, aux_rows([zero] + split3(-delta), QB))
            e = jnp.exp(jnp.dot(k_ref[2 * p + j], qa, preferred_element_type=F32))
            dp = jnp.dot(v_ref[2 * p + j], da, preferred_element_type=F32)
            ds = (e * dp).astype(BF16)
            probs.append(e.astype(BF16))
            dscores.append(ds)
            dos.append(beside(j, doh, blank))
            qs.append(beside(j, qh, blank))
            dqs.append(0.125 * jnp.dot(kt_ref[p, head(j), :], ds, preferred_element_type=F32))
        dv_acc[p] += (lax.dot_general(probs[0], dos[0], nt, preferred_element_type=F32)
                      + lax.dot_general(probs[1], dos[1], nt, preferred_element_type=F32))
        dk_acc[p] += (lax.dot_general(dscores[0], qs[0], nt, preferred_element_type=F32)
                      + lax.dot_general(dscores[1], qs[1], nt, preferred_element_type=F32))
        put(scatter, near, p, ALL, dst, jnp.concatenate(dqs, axis=0))

    trips = 2 * n * (n * TILE // QB)
    when = [min(w, trips - 1) for w in ((0, 3, 5, 7, 9, 12, 14) if reduces[0].relay else (3, 5, 7, 9, 13))]

    def blocks(srcs, near, dsts):
        for p in range(PARTS):
            block(p, srcs[p], near, dsts[p])

    blocks_loop(n, scatter, blocks, [(w, functools.partial(advance, i + 2)) for i, w in enumerate(when)])
    for p in range(PARTS):
        dk_ref[:, p * TILE:(p + 1) * TILE] = dk_acc[p].astype(BF16)
        dv_ref[:, p * TILE:(p + 1) * TILE] = dv_acc[p].astype(BF16)

    scatter.finish(dq_ref)
    for red in reduces:
        red.finish(2 + len(when))


def attention_bwd(n, cid, q_t, do_rows, stats_rows, k_aug, v_aug, k_t, wide, tall):
    total, keys = q_t.shape[2], k_aug.shape[1]
    r = TILE // n
    forms = [Wide(a.shape, n) for a in wide] + [Tall(a.shape, n) for a in tall]
    grads = list(wide) + list(tall)
    vm = pl.BlockSpec(memory_space=pltpu.VMEM)
    flat = jax.ShapeDtypeStruct((keys, PARTS * TILE), BF16)
    acc = pltpu.VMEM((PARTS, keys, TILE), F32)
    outs = [jax.ShapeDtypeStruct((PARTS, r, TILE), F32), flat, flat] + [jax.ShapeDtypeStruct(a.shape, F32) for a in grads]
    scratch = [pltpu.VMEM((PARTS, TILE, total), BF16), pltpu.VMEM((PARTS, 8, total), F32),
               acc, acc]
    scratch += Gather.scratch(n, BF16) + Gather.scratch(n, F32) + Scatter.scratch(n, TILE, TILE)
    for form in forms:
        scratch += Reduce.scratch(n, form)
    return pl.pallas_call(
        functools.partial(bwd_kernel, n, forms), out_shape=tuple(outs),
        in_specs=[vm] * 6 + [pl.BlockSpec(memory_space=pl.ANY)] * len(grads), out_specs=(vm,) * len(outs), name="attention_bwd",
        scratch_shapes=scratch,
        cost_estimate=pl.CostEstimate(flops=10 * 384 * total * keys, bytes_accessed=20_000_000, transcendentals=6 * total * keys),
        compiler_params=pltpu.CompilerParams(collective_id=cid, has_side_effects=True, vmem_limit_bytes=VMEM_LIMIT),
    )(q_t, do_rows, stats_rows, k_aug, v_aug, k_t, *grads)


def reduce_kernel(n, form, src, small, dk_ref, dv_ref, wk_ref, wv_ref, out, small_out, dm_ref,
                  slots, pair, ssend, srecv, dm_buf, msend, mrecv, *bufs):
    at = Place(n)
    at.barrier()
    red = Reduce(n, at, form, src, out, bufs, False)
    keep = dk_ref.shape[0]
    piece = keep // 3
    quarter = at.quarter()
    nt = (((1,), (1,)), ((), ()))

    def give_back(q):
        return rcopy(dm_buf.at[pl.ds(q * piece, piece), :], dm_ref.at[pl.ds(keep, piece), :], msend.at[q], mrecv, at.mate(q))

    def memory_grad():
        for i in range(3):
            rows = slice(i * piece, (i + 1) * piece)
            dm_buf[rows, :] = (lax.dot_general(dk_ref[rows, :], wk_ref[...], nt, preferred_element_type=F32)
                               + lax.dot_general(dv_ref[rows, :], wv_ref[...], nt, preferred_element_type=F32))

        @pl.when(quarter == 3)
        def _():
            for q in range(3):
                give_back(q).start()
            dm_ref[...] = jnp.zeros_like(dm_ref)

        @pl.when(quarter < 3)
        def _():
            dm_ref[0:keep, :] = dm_buf[...]

    def small_copies(stage):
        if stage == 3:
            return [rcopy(pair.at[at.core], pair.at[at.core], ssend.at[3, 0], srecv.at[3, 0], at.other_core())]
        mine = slots.at[stage, at.coord[stage]]
        return [rcopy(mine, mine, ssend.at[stage, k - 1], srecv.at[stage, k - 1], at.along(stage, k)) for k in range(1, n)]

    red.advance(0)
    slots[0, at.coord[0]] = small[...]
    for c in small_copies(0):
        c.start()
    for stage in range(1, 8):
        red.advance(stage)
        if stage == 1:
            memory_grad()
        if stage < 5:
            for c in small_copies(stage - 1):
                c.wait()
            if stage < 4:
                val = functools.reduce(jnp.add, [slots[stage - 1, k] for k in range(n)])
                if stage < 3:
                    slots[stage, at.coord[stage]] = val
                else:
                    pair[at.core] = val
                for c in small_copies(stage):
                    c.start()
            else:
                small_out[...] = pair[0] + pair[1]

    @pl.when(quarter == 3)
    def _():
        for q in range(3):
            give_back(q).wait_send()

    @pl.when(quarter < 3)
    def _():
        give_back(0).wait_recv()


def all_reduce_late(n, cid, m_rows, stack, small, dk, dv, wk, wv):
    form = Stack(stack.shape, n)
    vm = pl.BlockSpec(memory_space=pltpu.VMEM)
    sem = pltpu.SemaphoreType.DMA
    return pl.pallas_call(
        functools.partial(reduce_kernel, n, form),
        out_shape=(jax.ShapeDtypeStruct(stack.shape, F32), jax.ShapeDtypeStruct(small.shape, F32),
                   jax.ShapeDtypeStruct((m_rows, wk.shape[0]), F32)),
        in_specs=[pl.BlockSpec(memory_space=pl.ANY)] + [vm] * 5, out_specs=(vm,) * 3, name="reduce_late",
        scratch_shapes=[pltpu.VMEM((3, n) + small.shape, F32), pltpu.VMEM((2,) + small.shape, F32),
                        sem((4, n - 1)), sem((4, n - 1)), pltpu.VMEM((dk.shape[0], wk.shape[0]), F32), sem((3,)), sem(())]
        + Reduce.scratch(n, form),
        compiler_params=pltpu.CompilerParams(collective_id=cid, has_side_effects=True, vmem_limit_bytes=VMEM_LIMIT // 2),
    )(stack, small, dk, dv, wk, wv)


def solution(mesh):
    group = mesh.shape['seq']
    n = round((group // 2) ** (1 / 3))
    row_spec = P(('data', 'seq'), None)
    weight_spec = P()
    part_vec = P('data')
    part_mat = P('data', None)
    part_cube = P('data', None, None)

    def by_part(a):
        return jnp.transpose(a.reshape(a.shape[0], PARTS, TILE), (1, 0, 2))

    def by_row(a):
        return jnp.transpose(a, (1, 0, 2)).reshape(a.shape[1], PARTS * TILE)

    def device_step(dec_in, memory, mem_len, grad_out, norm_attn, wq_cross, wk_cross, wv_cross, wo_cross, norm_mlp, w_gate, w_up, w_down):
        q_rows, model_dim = dec_in.shape
        m_rows = memory.shape[0]
        heads, head_dim = wq_cross.shape[1], wq_cross.shape[2]
        wide = heads * head_dim
        wq, wk, wv = (w.reshape(model_dim, wide) for w in (wq_cross, wk_cross, wv_cross))
        wo = wo_cross.reshape(wide, model_dim)
        keep, piece, size = m_rows * 3 // 4, m_rows // 4, group // 4
        me = lax.axis_index('seq')
        slot = jnp.arange(keep)
        own_pos = me * m_rows + slot
        given_pos = ((slot // piece) * size + me % size) * m_rows + keep + slot % piece
        mem_pos = jnp.where(me // size == 3, given_pos, own_pos)
        bias = jnp.where(mem_pos < mem_len[0], 0.0, NEG)[:, None]
        lane = jnp.arange(TILE)[None, :] % head_dim
        flag = jnp.where((lane >= 1) & (lane <= 3), 1.0, 0.0)
        aux_k = jnp.where(lane == 0, bias, flag).astype(BF16)
        aux_v = jnp.broadcast_to(flag, aux_k.shape).astype(BF16)

        x_in = dec_in.astype(F32)
        normed_f, norm_pull = jax.vjp(rms_norm, x_in, norm_attn.astype(F32))
        normed = normed_f.astype(BF16)
        local_query = jnp.dot(normed, wq, preferred_element_type=F32).astype(BF16) * jnp.asarray(head_dim ** -0.5, BF16)
        out_parts, lse, q_t, kept, k_aug, v_aug, k_t = attention_fwd(
            n, 1, by_part(local_query), memory, wk, wv, aux_k, aux_v)
        attended_f = by_row(out_parts)

        attended = attended_f.astype(BF16)
        hidden_f = x_in + jnp.dot(attended, wo, preferred_element_type=F32)
        hidden = hidden_f.astype(BF16)
        normed_mlp_f, mlp_norm_pull = jax.vjp(rms_norm, hidden.astype(F32), norm_mlp.astype(F32))
        normed_mlp = normed_mlp_f.astype(BF16)
        gate_pre = jnp.dot(normed_mlp, w_gate, preferred_element_type=F32)
        up_pre = jnp.dot(normed_mlp, w_up, preferred_element_type=F32)
        mlp_f, gated_pull = jax.vjp(gated_unit, gate_pre, up_pre)
        mlp_act = mlp_f.astype(BF16)

        grad_top = grad_out.astype(BF16)
        g_down = jnp.einsum('qf,qd->fd', mlp_act, grad_top, preferred_element_type=F32)
        grad_act = jnp.einsum('qd,fd->qf', grad_top, w_down, preferred_element_type=F32)
        grad_gate, grad_up = gated_pull(grad_act)
        grad_gate_b = grad_gate.astype(BF16)
        grad_up_b = grad_up.astype(BF16)
        g_gate = jnp.einsum('qd,qf->df', normed_mlp, grad_gate_b, preferred_element_type=F32)
        g_up = jnp.einsum('qd,qf->df', normed_mlp, grad_up_b, preferred_element_type=F32)
        grad_normed_mlp = (jnp.einsum('qf,df->qd', grad_gate_b, w_gate, preferred_element_type=F32)
                           + jnp.einsum('qf,df->qd', grad_up_b, w_up, preferred_element_type=F32))
        grad_hidden_norm, g_norm_mlp = mlp_norm_pull(grad_normed_mlp)
        grad_hidden = grad_out + grad_hidden_norm
        grad_hidden_b = grad_hidden.astype(BF16)
        g_wo = jnp.einsum('qe,qd->ed', attended, grad_hidden_b, preferred_element_type=F32)
        grad_attended = jnp.einsum('qd,ed->qe', grad_hidden_b, wo, preferred_element_type=F32)
        delta = jnp.sum((grad_attended * attended_f).reshape(q_rows, PARTS, 2, head_dim), axis=-1)
        delta = jnp.transpose(delta, (1, 0, 2))
        stats_in = jnp.concatenate([lse[:, :, 0:2], delta, jnp.zeros((PARTS, q_rows, TILE - 4), F32)], axis=2)

        dq_parts, dk_b, dv_b, g_gate, g_up, g_down = attention_bwd(
            n, 2, q_t, by_part(grad_attended.astype(BF16)), stats_in, k_aug, v_aug, k_t, (g_gate, g_up), (g_down,))
        grad_query_b = by_row(dq_parts).astype(BF16)

        g_wq = jnp.einsum('td,te->de', normed, grad_query_b, preferred_element_type=F32)
        grad_normed = jnp.einsum('te,de->td', grad_query_b, wq, preferred_element_type=F32)
        grad_x_norm, g_norm_attn = norm_pull(grad_normed)
        g_dec = grad_hidden + grad_x_norm
        g_wk = jnp.einsum('td,te->de', kept, dk_b, preferred_element_type=F32)
        g_wv = jnp.einsum('td,te->de', kept, dv_b, preferred_element_type=F32)
        small = jnp.concatenate([g_norm_attn[None], g_norm_mlp[None], jnp.zeros((6, model_dim), F32)], axis=0)
        late, small, g_mem = all_reduce_late(n, 3, m_rows, jnp.stack([g_wq, g_wk, g_wv, g_wo]), small, dk_b, dv_b, wk, wv)
        cube = (model_dim, heads, head_dim)
        g_wq, g_wk, g_wv = late[0], late[1], late[2]
        g_wo = late[3].reshape(heads, head_dim, model_dim)
        g_norm_attn, g_norm_mlp = small[0], small[1]
        return (g_dec, g_mem, g_norm_attn, g_wq.reshape(cube), g_wk.reshape(cube), g_wv.reshape(cube),
                g_wo, g_norm_mlp, g_gate, g_up, g_down)

    return jax.shard_map(device_step, mesh=mesh,
                         in_specs=(row_spec, row_spec, part_vec, row_spec) + (weight_spec,) * 9,
                         out_specs=(row_spec, row_spec, part_vec, part_cube, part_cube, part_cube, part_cube, part_vec, part_mat, part_mat, part_mat),
                         check_vma=False)
```

```python
import functools

import jax
import jax.numpy as jnp
from jax import lax
from jax.experimental import pallas as pl
from jax.experimental.pallas import tpu as pltpu
from jax.sharding import PartitionSpec as P

F32 = jnp.float32
BF16 = jnp.bfloat16
MESH = pl.DeviceIdType.MESH
VMEM_LIMIT = 62 * 1024 * 1024
NEG = -1e30
ORDERS = ((0, 1, 2), (2, 0, 1), (1, 2, 0))
PARTS = 3
TILE = 128
HALF = TILE // 2
ALL = slice(None)


def rms_norm(tensor, gain):
    mean_sq = jnp.mean(tensor * tensor, axis=-1, keepdims=True)
    return tensor * lax.rsqrt(mean_sq + 1e-6) * gain


def gated_unit(gate_pre, up_pre):
    return jax.nn.silu(gate_pre) * up_pre


class Place:
    def __init__(self, n):
        self.n = n
        me = lax.axis_index("seq")
        self.me = me
        self.core = lax.rem(me, 2)
        x = lax.rem(me // 2, n)
        y = lax.rem(me // (2 * n), n)
        z = me // (2 * n * n)
        self.coord = (z, y, x)
        self.stride = (2 * n * n, 2 * n, 2)

    def along(self, axis, k):
        here = self.coord[axis]
        return self.me + (lax.rem(here + k, self.n) - here) * self.stride[axis]

    def other_core(self):
        return self.me + 1 - 2 * self.core

    def quarter(self):
        return self.me // (self.n ** 3 // 2)

    def mate(self, q):
        size = self.n ** 3 // 2
        return q * size + lax.rem(self.me, size)

    def to(self, k):
        return {"seq": k}

    def barrier(self):
        sem = pltpu.get_barrier_semaphore()
        for axis in range(3):
            for k in range(1, self.n):
                pl.semaphore_signal(sem, inc=1, device_id=self.to(self.along(axis, k)), device_id_type=MESH)
        pl.semaphore_signal(sem, inc=1, device_id=self.to(self.other_core()), device_id_type=MESH)
        extra = 0
        if self.n < 4:
            for k in range(1, 4):
                pl.semaphore_signal(sem, inc=1, device_id=self.to(self.mate(lax.rem(self.quarter() + k, 4))), device_id_type=MESH)
            extra = 3
        pl.semaphore_wait(sem, 3 * (self.n - 1) + 1 + extra)


def rcopy(src, dst, send, recv, device):
    return pltpu.make_async_remote_copy(src_ref=src, dst_ref=dst, send_sem=send, recv_sem=recv,
                                        device_id={"seq": device}, device_id_type=MESH)


def lanes(start, size):
    return pl.ds(pl.multiple_of(start, TILE), size)


def rows_of(start, size):
    return pl.ds(pl.multiple_of(start, 8), size)


class Gather:
    def __init__(self, n, at, src, full, bufs):
        self.n, self.at, self.src, self.full = n, at, src, full
        self.rows, self.send, self.recv, self.csend, self.crecv = bufs
        self.copies = {}

    @staticmethod
    def scratch(n, dtype):
        sem = pltpu.SemaphoreType.DMA
        return [pltpu.VMEM((PARTS, TILE, TILE), dtype), sem((3, PARTS, n - 1)), sem((3, PARTS, n - 1)),
                sem((PARTS,)), sem((PARTS,))]

    def begin(self):
        n, at = self.n, self.at
        r = TILE // n
        for p in range(PARTS):
            a3 = ORDERS[p][2]
            mine = rows_of(at.coord[a3] * r, r)
            for k in range(1, n):
                c = rcopy(self.src.at[p], self.rows.at[p, mine, :], self.send.at[0, p, k - 1], self.recv.at[0, p, k - 1], at.along(a3, k))
                c.start()
                self.copies[0, p, k] = c
            self.rows[p, mine, :] = self.src[p]

    def turn(self):
        at, n = self.at, self.n
        for p in range(PARTS):
            a1, a2, _ = ORDERS[p]
            for k in range(1, n):
                self.copies[0, p, k].wait()
            block = self.rows[p].astype(F32).T
            base = ((at.core * n + at.coord[a1]) * n + at.coord[a2]) * TILE
            self.full[p, :, lanes(base, TILE)] = block[:self.full.shape[1]].astype(self.full.dtype)

    def place(self, stage, p, back):
        at, n = self.at, self.n
        a1, a2, _ = ORDERS[p]
        if stage == 1:
            spot = lax.rem(at.coord[a2] + n - back, n)
            return a2, lanes(((at.core * n + at.coord[a1]) * n + spot) * TILE, TILE)
        spot = lax.rem(at.coord[a1] + n - back, n)
        return a1, lanes((at.core * n + spot) * n * TILE, n * TILE)

    def spread(self, stage):
        n, at = self.n, self.at
        for p in range(PARTS):
            axis, cols = self.place(stage, p, 0)
            view = self.full.at[p, :, cols]
            for k in range(1, n):
                c = rcopy(view, view, self.send.at[stage, p, k - 1], self.recv.at[stage, p, k - 1], at.along(axis, k))
                c.start()
                self.copies[stage, p, k] = c

    def settle(self, stage):
        n = self.n
        for p in range(PARTS):
            for k in range(1, n):
                self.copies[stage, p, k].wait()

    def swap(self):
        n, at = self.n, self.at
        width = n * n * TILE
        out = []
        for p in range(PARTS):
            view = self.full.at[p, :, lanes(at.core * width, width)]
            c = rcopy(view, view, self.csend.at[p], self.crecv.at[p], at.other_core())
            c.start()
            out.append(c)
        return out


GATHER_REFS = 5


def run_gathers(gathers, hooks):
    for g in gathers:
        g.begin()
    hooks[0]()
    for g in gathers:
        g.turn()
        g.spread(1)
    hooks[1]()
    for g in gathers:
        g.settle(1)
        g.spread(2)
    hooks[2]()
    final = []
    for g in gathers:
        g.settle(2)
        final += g.swap()
    for c in final:
        c.wait()


def merge(blocks, rows_axis):
    take = (lambda b, i, j: b[i:j]) if rows_axis == 0 else (lambda b, i, j: b[:, i:j])
    outs, maxes, sums = [], [], []
    for h in range(2):
        ms = [take(b, TILE + h, TILE + h + 1) for b in blocks]
        m = functools.reduce(jnp.maximum, ms)
        ws = [jnp.exp(v - m) for v in ms]
        o = sum(take(b, HALF * h, HALF * h + HALF) * w for b, w in zip(blocks, ws))
        l = sum(take(b, TILE + 2 + h, TILE + 3 + h) * w for b, w in zip(blocks, ws))
        outs.append(o)
        maxes.append(m)
        sums.append(l)
    return outs, maxes + sums


class Scatter:
    def __init__(self, n, at, with_stats, bufs):
        self.n, self.at, self.with_stats = n, at, with_stats
        (self.far, self.near, self.buf0, self.buf1, self.acc1, self.buf2, self.acc2, self.buf3, self.pass_buf,
         self.csend, self.crecv, self.send, self.recv, self.psend, self.precv) = bufs
        self.relay = n == 4
        self.step = n * TILE

    @staticmethod
    def scratch(n, rows, wide):
        sem = pltpu.SemaphoreType.DMA
        half = n * n * TILE
        r = TILE // n
        return [
            pltpu.VMEM((PARTS, rows, half), F32), pltpu.VMEM((PARTS, rows, half), F32), pltpu.VMEM((PARTS, rows, half), F32),
            pltpu.VMEM((PARTS, n - 1, rows, n * TILE), F32), pltpu.VMEM((PARTS, rows, n * TILE), F32),
            pltpu.VMEM((PARTS, n - 1, rows, TILE), F32), pltpu.VMEM((PARTS, TILE, wide), F32),
            pltpu.VMEM((PARTS, n - 1, r, wide), F32), pltpu.VMEM((PARTS, 2, rows, n * HALF), F32),
            sem((PARTS, n)), sem((PARTS, n)), sem((3, PARTS, n - 1)), sem((3, PARTS, n - 1)), sem((PARTS, 2)), sem((PARTS, 2)),
        ]

    def visit(self, i):
        if self.relay:
            return jnp.where(i == 0, 2, jnp.where(i == 1, 3, jnp.where(i == 2, 1, 0)))
        return self.n - 1 - i

    def pass_copy(self, p, i):
        width = self.step // 2
        return rcopy(self.near.at[p, :, lanes(self.chunk(p, 2) * self.step + i * width, width)], self.pass_buf.at[p, i],
                     self.psend.at[p, i], self.precv.at[p, i], self.at.along(ORDERS[p][0], 1 + 2 * i))

    def take_over(self, p, i):
        self.pass_copy(p, i).wait_recv()
        width = self.step // 2
        for j in range(width // TILE):
            col = lanes(self.chunk(p, 1 + 2 * i) * self.step + i * width + j * TILE, TILE)
            self.combine(self.near, p, col, [self.near[p, :, col], self.pass_buf[p, i, :, j * TILE:(j + 1) * TILE]])
        self.first_copy(p, 1 + 2 * i).start()

    def chunk(self, p, k):
        return lax.rem(self.at.coord[ORDERS[p][0]] + k, self.n)

    def combine(self, dst, p, col, vals):
        if self.with_stats:
            outs, stats = merge(vals, 0)
            dst[p, 0:HALF, col] = outs[0]
            dst[p, HALF:TILE, col] = outs[1]
            dst[p, TILE:TILE + 8, col] = jnp.concatenate(stats + [jnp.zeros_like(stats[0])] * 4, axis=0)
        else:
            dst[p, :, col] = functools.reduce(jnp.add, vals)

    def core_copy(self, p, k):
        view = (p, ALL, lanes(self.chunk(p, k) * self.step, self.step))
        return rcopy(self.far.at[view], self.buf0.at[view], self.csend.at[p, k], self.crecv.at[p, k], self.at.other_core())

    def first_copy(self, p, k):
        return rcopy(self.near.at[p, :, lanes(self.chunk(p, k) * self.step, self.step)], self.buf1.at[p, k - 1],
                     self.send.at[0, p, k - 1], self.recv.at[0, p, k - 1], self.at.along(ORDERS[p][0], k))

    def far_done(self, k):
        for p in range(PARTS):
            self.core_copy(p, k).start()

    def near_done(self, k):
        for p in range(PARTS):
            self.core_copy(p, k).wait()

            def fold(j, _, p=p):
                col = lanes(self.chunk(p, k) * self.step + j * TILE, TILE)
                self.combine(self.near, p, col, [self.near[p, :, col], self.buf0[p, :, col]])
                return 0

            lax.fori_loop(0, self.n, fold, 0)

            if self.relay:
                @pl.when(k == 2)
                def _(p=p):
                    for i in range(2):
                        self.pass_copy(p, i).start()

                for i in range(2):
                    @pl.when(k == 1 + 2 * i)
                    def _(p=p, i=i):
                        self.take_over(p, i)
            else:
                @pl.when(k > 0)
                def _(p=p):
                    self.first_copy(p, k).start()

    def finish(self, o_ref, st_ref=None):
        n, at = self.n, self.at
        r = TILE // n
        copies = {}
        for p in range(PARTS):
            a1, a2, _ = ORDERS[p]
            direct = (1, 3) if self.relay else range(1, n)
            for k in direct:
                self.first_copy(p, k).wait()
            if self.relay:
                for i in range(2):
                    self.pass_copy(p, i).wait_send()
            mine = at.coord[a1] * n * TILE
            for j in range(n):
                col = slice(j * TILE, (j + 1) * TILE)
                self.combine(self.acc1, p, pl.ds(j * TILE, TILE),
                             [self.near[p, :, lanes(mine + j * TILE, TILE)]] + [self.buf1[p, k - 1, :, col] for k in direct])
            for k in range(1, n):
                there = lax.rem(at.coord[a2] + k, n)
                c = rcopy(self.acc1.at[p, :, lanes(there * TILE, TILE)], self.buf2.at[p, k - 1],
                          self.send.at[1, p, k - 1], self.recv.at[1, p, k - 1], at.along(a2, k))
                c.start()
                copies[1, p, k] = c
        for p in range(PARTS):
            _, a2, a3 = ORDERS[p]
            for k in range(1, n):
                copies[1, p, k].wait()
            blocks = [self.acc1[p, :, lanes(at.coord[a2] * TILE, TILE)]] + [self.buf2[p, k] for k in range(n - 1)]
            if self.with_stats:
                outs, stats = merge(blocks, 0)
                self.acc2[p, :, 0:TILE] = jnp.concatenate(outs, axis=0).T
                tail = jnp.concatenate(stats + [jnp.zeros((TILE - 4, TILE), F32)], axis=0)
                self.acc2[p, :, TILE:2 * TILE] = tail.T
            else:
                self.acc2[p] = functools.reduce(jnp.add, blocks).T
            for k in range(1, n):
                there = lax.rem(at.coord[a3] + k, n)
                c = rcopy(self.acc2.at[p, pl.ds(pl.multiple_of(there * r, r), r), :], self.buf3.at[p, k - 1],
                          self.send.at[2, p, k - 1], self.recv.at[2, p, k - 1], at.along(a3, k))
                c.start()
                copies[2, p, k] = c
        for p in range(PARTS):
            a3 = ORDERS[p][2]
            for k in range(1, n):
                copies[2, p, k].wait()
            blocks = [self.acc2[p, pl.ds(pl.multiple_of(at.coord[a3] * r, r), r), :]] + [self.buf3[p, k] for k in range(n - 1)]
            if self.with_stats:
                outs, (m0, m1, l0, l1) = merge(blocks, 1)
                o_ref[p] = jnp.concatenate([outs[0] / l0, outs[1] / l1], axis=1)
                col = lax.broadcasted_iota(jnp.int32, (r, TILE), 1)
                st_ref[p] = jnp.where(col == 0, m0 + jnp.log(l0), jnp.where(col == 1, m1 + jnp.log(l1), 0.0))
            else:
                o_ref[p] = functools.reduce(jnp.add, blocks)


class Wide:
    def __init__(self, shape, n):
        self.part, self.cols = shape[0] // PARTS, shape[1]
        self.r1, self.r2, self.c3 = self.part // 2, self.part // 2 // n, shape[1] // n
        self.l1, self.l2, self.l3 = (self.r1, self.cols), (self.r2, self.cols), (self.r2, self.c3)

    def row(self, p, c, a):
        return self.part * p + self.r1 * c + self.r2 * a

    def full1(self, p, c):
        return rows_of(self.part * p + self.r1 * c, self.r1), ALL

    def full2(self, p, c, a):
        return rows_of(self.row(p, c, a), self.r2), ALL

    def half2(self, p, c, a, i):
        size = self.r2 // 2
        return rows_of(self.row(p, c, a) + i * size, size), ALL

    def hin1(self, a, i):
        size = self.r2 // 2
        return rows_of(self.r2 * a + i * size, size), ALL

    def full3(self, p, c, a, b):
        return rows_of(self.row(p, c, a), self.r2), lanes(self.c3 * b, self.c3)

    def in1(self, a):
        return rows_of(self.r2 * a, self.r2), ALL

    def in2(self, b):
        return ALL, lanes(self.c3 * b, self.c3)


class Tall(Wide):
    def __init__(self, shape, n):
        super().__init__(shape, n)
        self.r3 = self.r2 // n
        self.l3 = (self.r3, self.cols)

    def full3(self, p, c, a, b):
        return rows_of(self.row(p, c, a) + self.r3 * b, self.r3), ALL

    def in2(self, b):
        return rows_of(self.r3 * b, self.r3), ALL


class Stack:
    def __init__(self, shape, n):
        w, rows, cols = shape
        self.part, self.w3 = rows // PARTS, w // n
        self.r1, self.r2 = self.part // 2, self.part // 2 // n
        self.l1, self.l2, self.l3 = (w, self.r1, cols), (w, self.r2, cols), (self.w3, self.r2, cols)

    def full1(self, p, c):
        return ALL, rows_of(self.part * p + self.r1 * c, self.r1), ALL

    def row(self, p, c, a):
        return self.part * p + self.r1 * c + self.r2 * a

    def full2(self, p, c, a):
        return ALL, rows_of(self.row(p, c, a), self.r2), ALL

    def full3(self, p, c, a, b):
        return pl.ds(self.w3 * b, self.w3), rows_of(self.row(p, c, a), self.r2), ALL

    def in1(self, a):
        return ALL, rows_of(self.r2 * a, self.r2), ALL

    def in2(self, b):
        return pl.ds(self.w3 * b, self.w3), ALL, ALL


class Reduce:
    STAGES = ("core", "pass", "first", "second", "third", "back2", "back1", "relay", "swap")

    def __init__(self, n, at, form, src, out, bufs, relay):
        self.n, self.at, self.form, self.src, self.out = n, at, form, src, out
        self.relay = relay and n == 4
        self.stages = [v for v in self.STAGES if self.relay or v not in ("pass", "relay")]
        (self.own, self.buf0, self.buf1, self.acc1, self.buf2, self.buf3, self.lsem,
         self.csend, self.crecv, self.send, self.recv) = bufs

    @staticmethod
    def scratch(n, form):
        sem = pltpu.SemaphoreType.DMA
        kinds = len(Reduce.STAGES)
        return [
            pltpu.VMEM((PARTS,) + form.l1, F32), pltpu.VMEM((PARTS,) + form.l1, F32),
            pltpu.VMEM((PARTS, n - 1) + form.l2, F32), pltpu.VMEM((PARTS,) + form.l2, F32),
            pltpu.VMEM((PARTS, n - 1) + form.l3, F32), pltpu.VMEM((PARTS, n) + form.l3, F32),
            sem((PARTS,)), sem((PARTS,)), sem((PARTS,)), sem((kinds, PARTS, n - 1)), sem((kinds, PARTS, n - 1)),
        ]

    def spots(self, p):
        return [self.at.coord[a] for a in ORDERS[p]]

    def hold(self, p, i):
        return self.buf1.at[(p, 1)].at[self.form.hin1(0, i)]

    def copies(self, stage, p):
        at, n, form = self.at, self.n, self.form
        A1, A2, A3 = self.spots(p)
        a1, a2, a3 = ORDERS[p]
        c = at.core
        if stage == "core":
            return [rcopy(self.src.at[form.full1(p, 1 - c)], self.buf0.at[p], self.csend.at[p], self.crecv.at[p], at.other_core()),
                    pltpu.make_async_copy(self.src.at[form.full1(p, c)], self.own.at[p], self.lsem.at[p])]
        kind = self.STAGES.index(stage)
        out = []

        def add(src, dst, axis, k):
            out.append(rcopy(src, dst, self.send.at[kind, p, k - 1], self.recv.at[kind, p, k - 1], at.along(axis, k)))

        if stage == "swap":
            view = self.out.at[form.full1(p, c)]
            return [rcopy(view, view, self.send.at[kind, p, 0], self.recv.at[kind, p, 0], at.other_core())]
        steps = range(1, n)
        near = (1, n - 1) if self.relay else steps
        if stage == "pass":
            for i, k in enumerate(near):
                add(self.own.at[p].at[form.hin1(lax.rem(A1 + 2, n), i)], self.hold(p, i), a1, k)
        elif stage == "first":
            for k in near:
                add(self.own.at[p].at[form.in1(lax.rem(A1 + k, n))], self.buf1.at[p, k - 1], a1, k)
        elif stage == "second":
            for k in steps:
                add(self.acc1.at[p].at[form.in2(lax.rem(A2 + k, n))], self.buf2.at[p, k - 1], a2, k)
        elif stage == "third":
            for k in steps:
                add(self.buf3.at[p, A3], self.buf3.at[p, A3], a3, k)
        elif stage == "back2":
            view = self.out.at[form.full3(p, c, A1, A2)]
            for k in steps:
                add(view, view, a2, k)
        elif stage == "back1":
            view = self.out.at[form.full2(p, c, A1)]
            for k in near:
                add(view, view, a1, k)
        else:
            for i, k in enumerate(near):
                view = self.out.at[form.half2(p, c, lax.rem(A1 + n - k, n), i)]
                add(view, view, a1, k)
        return out

    def advance(self, step):
        form, n = self.form, self.n
        stage = self.stages[step] if step < len(self.stages) else None
        before = self.stages[step - 1]
        near = (0, n - 2) if self.relay else range(n - 1)
        for p in range(PARTS):
            A1, A2, A3 = self.spots(p)
            if step:
                for c in self.copies(before, p):
                    c.wait()
            own = self.own.at[p]
            if before == "core":
                own[...] += self.buf0[p]
            elif before == "pass":
                for i, k in enumerate((1, n - 1)):
                    own[form.hin1(lax.rem(A1 + k, n), i)] += self.hold(p, i)[...]
            elif before == "first":
                self.acc1[p] = functools.reduce(jnp.add, [own[form.in1(A1)]] + [self.buf1[p, k] for k in near])
            elif before == "second":
                self.buf3[p, A3] = functools.reduce(jnp.add, [self.acc1[(p,) + form.in2(A2)]] + [self.buf2[p, k] for k in range(n - 1)])
            elif before == "third":
                self.out[form.full3(p, self.at.core, A1, A2)] = functools.reduce(jnp.add, [self.buf3[p, k] for k in range(n)])
            if stage:
                for c in self.copies(stage, p):
                    c.start()

    def finish(self, step):
        for i in range(step, len(self.stages) + 1):
            self.advance(i)


REDUCE_REFS = 11


QB = 256


def aux_rows(rows, width):
    pad = jnp.zeros((64 - len(rows), width), F32)
    return jnp.concatenate(list(rows) + [pad], axis=0).astype(BF16)


def split3(v):
    hi = v.astype(BF16).astype(F32)
    mid = (v - hi).astype(BF16).astype(F32)
    lo = (v - hi - mid).astype(BF16).astype(F32)
    return [hi, mid, lo]


def blocks_loop(n, scatter, blocks, events):
    per = n * TILE // QB
    at = scatter.at

    def body(t, _):
        u = t // per
        k = scatter.visit(u // 2)
        near = lax.rem(u, 2)
        half = jnp.where(near == 1, at.core, 1 - at.core)
        inside = [scatter.chunk(p, k) * (n * TILE) + lax.rem(t, per) * QB for p in range(PARTS)]
        srcs = [pl.ds(pl.multiple_of(half * (n * n * TILE) + i, QB), QB) for i in inside]
        blocks(srcs, near, [pl.ds(pl.multiple_of(i, QB), QB) for i in inside])
        last = lax.rem(t, per) == per - 1

        @pl.when(last & (near == 0))
        def _():
            scatter.far_done(k)

        @pl.when(last & (near == 1))
        def _():
            scatter.near_done(k)

        for when, action in events:
            @pl.when(t == when)
            def _(action=action):
                action()
        return 0

    lax.fori_loop(0, 2 * n * per, body, 0)


def put(scatter, near, p, row, col, val):
    @pl.when(near == 1)
    def _():
        scatter.near[p, row, col] = val

    @pl.when(near == 0)
    def _():
        scatter.far[p, row, col] = val


def head(j):
    return slice(HALF * j, HALF * (j + 1))


def beside(j, block, other):
    return jnp.concatenate([block, other] if j == 0 else [other, block], axis=0)


def shrink(op, v, rows):
    while v.shape[0] > rows:
        h = v.shape[0] // 2
        v = op(v[:h], v[h:])
    return v


KC = 256


def fwd_kernel(n, x_ref, mem_ref, wk_ref, wv_ref, len_ref, o_ref, st_ref, *refs):
    saved, refs = refs[:SAVED], refs[SAVED:]
    kept, refs = refs[:SAVED], refs[SAVED:]
    q_ref, keep_ref, k_ref, v_ref, kt_ref = kept
    vt_ref, s_buf, msend, mrecv, save_sem, *refs = refs
    gbufs, bufs = refs[:GATHER_REFS], refs[GATHER_REFS:]
    keys = k_ref.shape[1]
    piece = keys // 3
    kc = min(KC, piece)
    chunks = keys // kc
    at = Place(n)
    at.barrier()
    quarter = at.quarter()

    size = piece // 2

    def donate(q, i):
        return rcopy(mem_ref.at[pl.ds(keys + i * size, size), :], keep_ref.at[pl.ds(q * piece + i * size, size), :],
                     msend.at[i], mrecv.at[q, i], at.mate(3))

    def give(i):
        for q in range(3):
            @pl.when(quarter == q)
            def _(q=q):
                donate(q, i).start()

    def saves():
        return [pltpu.make_async_copy(a, b, save_sem.at[i]) for i, (a, b) in enumerate(zip(kept, saved))]

    def project():
        @pl.when(quarter < 3)
        def _():
            keep_ref[...] = mem_ref[0:keys, :]

        @pl.when(quarter == 3)
        def _():
            for q in range(3):
                for i in range(2):
                    donate(q, i).wait_recv()

        lane = lax.broadcasted_iota(jnp.int32, (piece, TILE), 1)
        spot = lax.broadcasted_iota(jnp.int32, (piece, TILE), 0)
        low = lane < HALF
        lane = lane % HALF
        flag = jnp.where((lane > 0) & (lane < 4), 1.0, 0.0)
        for i in range(3):
            rows = pl.ds(i * piece, piece)
            m = keep_ref[rows, :]
            start = jnp.where(quarter == 3, at.mate(i) * (keys + piece) + keys, at.me * (keys + piece) + i * piece)
            bias = jnp.where(start + spot < len_ref[0], 0.0, NEG)
            aux_k = jnp.where(lane == 0, bias, flag)
            for w_ref, aux, a_ref, t_ref in ((wk_ref, aux_k, k_ref, kt_ref), (wv_ref, flag, v_ref, vt_ref)):
                for p in range(PARTS):
                    b = jnp.dot(m, w_ref[:, p * TILE:(p + 1) * TILE], preferred_element_type=F32).astype(BF16).astype(F32)
                    a_ref[2 * p, rows, :] = jnp.where(low, b, aux).astype(BF16)
                    a_ref[2 * p + 1, rows, :] = jnp.where(low, aux, b).astype(BF16)
                    t_ref[p, :, rows] = b.T.astype(BF16)

    run_gathers([Gather(n, at, x_ref, q_ref, gbufs)], [functools.partial(give, 0), functools.partial(give, 1), project])
    for q in range(3):
        @pl.when(quarter == q)
        def _(q=q):
            for i in range(2):
                donate(q, i).wait_send()
    for c in saves():
        c.start()
    aux = aux_rows([jnp.ones((1, QB), F32)], QB)
    scatter = Scatter(n, at, True, bufs)

    def blocks(srcs, near, dsts):
        heads = [(p, j) for p in range(PARTS) for j in range(2)]

        def score(i, c, run):
            p, j = heads[i]
            qa = beside(j, q_ref[p, head(j), srcs[p]], aux)
            s = jnp.dot(k_ref[i, c * kc:(c + 1) * kc, :], qa, preferred_element_type=F32)
            s_buf[i % 2, c * kc:(c + 1) * kc, :] = s
            top = shrink(jnp.maximum, s, 16)
            return top if run is None else jnp.maximum(run, top)

        run = None
        for c in range(chunks):
            run = score(0, c, run)
        done = []
        for i, (p, j) in enumerate(heads):
            m = jnp.max(run, axis=0, keepdims=True)
            run, total, out = None, None, None
            for c in range(chunks):
                if i + 1 < len(heads):
                    run = score(i + 1, c, run)
                e = jnp.exp(s_buf[i % 2, c * kc:(c + 1) * kc, :] - m)
                part = shrink(jnp.add, e, 16)
                total = part if total is None else total + part
                o = jnp.dot(vt_ref[p, head(j), c * kc:(c + 1) * kc], e.astype(BF16), preferred_element_type=F32)
                out = o if out is None else out + o
            done.append((out, m, jnp.sum(total, axis=0, keepdims=True)))
            if j == 1:
                (o0, m0, l0), (o1, m1, l1) = done[-2:]
                val = jnp.concatenate([o0, o1, m0, m1, l0, l1, jnp.zeros((4, QB), F32)], axis=0)
                put(scatter, near, p, ALL, dsts[p], val)

    blocks_loop(n, scatter, blocks, [])
    scatter.finish(o_ref, st_ref)
    for c in saves():
        c.wait()


SAVED = 5


def attention_fwd(n, cid, rows, memory, wk, wv, mem_len):
    total = 2 * n * n * TILE
    r = TILE // n
    m_rows, dim = memory.shape
    keys = m_rows * 3 // 4
    vm, hbm = pl.BlockSpec(memory_space=pltpu.VMEM), pl.BlockSpec(memory_space=pl.ANY)
    sem = pltpu.SemaphoreType.DMA
    shapes = ((PARTS, TILE, total), (keys, dim), (2 * PARTS, keys, TILE), (2 * PARTS, keys, TILE), (PARTS, TILE, keys))
    scratch = [pltpu.VMEM(v, BF16) for v in shapes] + [pltpu.VMEM(shapes[-1], BF16), pltpu.VMEM((2, keys, QB), F32),
                                                       sem((2,)), sem((3, 2)), sem((SAVED,))]
    return pl.pallas_call(
        functools.partial(fwd_kernel, n),
        out_shape=(jax.ShapeDtypeStruct((PARTS, r, TILE), F32),) * 2 + tuple(jax.ShapeDtypeStruct(v, BF16) for v in shapes),
        in_specs=[vm] * 4 + [pl.BlockSpec(memory_space=pltpu.SMEM)], out_specs=(vm,) * 2 + (hbm,) * SAVED, name="attention_fwd",
        scratch_shapes=scratch + Gather.scratch(n, BF16) + Scatter.scratch(n, TILE + 8, 2 * TILE),
        compiler_params=pltpu.CompilerParams(collective_id=cid, has_side_effects=True, vmem_limit_bytes=VMEM_LIMIT),
    )(rows, memory, wk, wv, mem_len)


SCATTER_REFS = 15


def bwd_kernel(n, forms, q_ref, x_ref, s_ref, k_ref, v_ref, kt_ref, *refs):
    count = len(forms)
    grads, refs = refs[:count], refs[count:]
    dq_ref, dk_ref, dv_ref, *refs = refs
    sums, refs = refs[:count], refs[count:]
    do_ref, st_ref, dk_acc, dv_acc, *refs = refs
    xbufs, refs = refs[:GATHER_REFS], refs[GATHER_REFS:]
    sbufs, refs = refs[:GATHER_REFS], refs[GATHER_REFS:]
    bufs, refs = refs[:SCATTER_REFS], refs[SCATTER_REFS:]
    one = jnp.ones((1, QB), F32)
    zero = jnp.zeros((1, QB), F32)
    blank = jnp.zeros((HALF, QB), BF16)
    nt = (((1,), (1,)), ((), ()))
    at = Place(n)
    at.barrier()
    scatter = Scatter(n, at, False, bufs)
    reduces = [Reduce(n, at, form, grads[i], sums[i], refs[REDUCE_REFS * i:REDUCE_REFS * (i + 1)], True)
               for i, form in enumerate(forms)]

    def advance(stage):
        for red in reduces:
            red.advance(stage)

    gathers = [Gather(n, at, s_ref, st_ref, sbufs), Gather(n, at, x_ref, do_ref, xbufs)]

    def clear():
        dk_acc[...] = jnp.zeros_like(dk_acc)
        dv_acc[...] = jnp.zeros_like(dv_acc)

    run_gathers(gathers, [functools.partial(advance, 0), clear, functools.partial(advance, 1)])

    def block(p, src, near, dst):
        probs, dscores, dos, qs, dqs = [], [], [], [], []
        for j in range(2):
            qh = q_ref[p, head(j), src]
            doh = do_ref[p, head(j), src]
            lse = st_ref[p, j:j + 1, src]
            delta = st_ref[p, 2 + j:3 + j, src]
            qa = beside(j, qh, aux_rows([one] + split3(-lse), QB))
            da = beside(j, doh, aux_rows([zero] + split3(-delta), QB))
            e = jnp.exp(jnp.dot(k_ref[2 * p + j], qa, preferred_element_type=F32))
            dp = jnp.dot(v_ref[2 * p + j], da, preferred_element_type=F32)
            ds = (e * dp).astype(BF16)
            probs.append(e.astype(BF16))
            dscores.append(ds)
            dos.append(beside(j, doh, blank))
            qs.append(beside(j, qh, blank))
            dqs.append(0.125 * jnp.dot(kt_ref[p, head(j), :], ds, preferred_element_type=F32))
        dv_acc[p] += (lax.dot_general(probs[0], dos[0], nt, preferred_element_type=F32)
                      + lax.dot_general(probs[1], dos[1], nt, preferred_element_type=F32))
        dk_acc[p] += (lax.dot_general(dscores[0], qs[0], nt, preferred_element_type=F32)
                      + lax.dot_general(dscores[1], qs[1], nt, preferred_element_type=F32))
        put(scatter, near, p, ALL, dst, jnp.concatenate(dqs, axis=0))

    trips = 2 * n * (n * TILE // QB)
    when = [min(w, trips - 1) for w in ((0, 3, 5, 7, 9, 12, 14) if reduces[0].relay else (3, 5, 7, 9, 13))]

    def blocks(srcs, near, dsts):
        for p in range(PARTS):
            block(p, srcs[p], near, dsts[p])

    blocks_loop(n, scatter, blocks, [(w, functools.partial(advance, i + 2)) for i, w in enumerate(when)])
    for p in range(PARTS):
        dk_ref[:, p * TILE:(p + 1) * TILE] = dk_acc[p].astype(BF16)
        dv_ref[:, p * TILE:(p + 1) * TILE] = dv_acc[p].astype(BF16)

    scatter.finish(dq_ref)
    for red in reduces:
        red.finish(2 + len(when))


def attention_bwd(n, cid, q_t, do_rows, stats_rows, k_aug, v_aug, k_t, wide, tall):
    total, keys = q_t.shape[2], k_aug.shape[1]
    r = TILE // n
    forms = [Wide(a.shape, n) for a in wide] + [Tall(a.shape, n) for a in tall]
    grads = list(wide) + list(tall)
    vm = pl.BlockSpec(memory_space=pltpu.VMEM)
    flat = jax.ShapeDtypeStruct((keys, PARTS * TILE), BF16)
    acc = pltpu.VMEM((PARTS, keys, TILE), F32)
    outs = [jax.ShapeDtypeStruct((PARTS, r, TILE), F32), flat, flat] + [jax.ShapeDtypeStruct(a.shape, F32) for a in grads]
    scratch = [pltpu.VMEM((PARTS, TILE, total), BF16), pltpu.VMEM((PARTS, 8, total), F32),
               acc, acc]
    scratch += Gather.scratch(n, BF16) + Gather.scratch(n, F32) + Scatter.scratch(n, TILE, TILE)
    for form in forms:
        scratch += Reduce.scratch(n, form)
    return pl.pallas_call(
        functools.partial(bwd_kernel, n, forms), out_shape=tuple(outs),
        in_specs=[vm] * 6 + [pl.BlockSpec(memory_space=pl.ANY)] * len(grads), out_specs=(vm,) * len(outs), name="attention_bwd",
        scratch_shapes=scratch,
        cost_estimate=pl.CostEstimate(flops=10 * 384 * total * keys, bytes_accessed=20_000_000, transcendentals=6 * total * keys),
        compiler_params=pltpu.CompilerParams(collective_id=cid, has_side_effects=True, vmem_limit_bytes=VMEM_LIMIT),
    )(q_t, do_rows, stats_rows, k_aug, v_aug, k_t, *grads)


BITS = 8


def reduce_kernel(n, form, src, small, dk_ref, dv_ref, wk_ref, wv_ref, out, small_out, dm_ref,
                  slots, pair, ssend, srecv, dm_buf, msend, mrecv, *bufs):
    at = Place(n)
    at.barrier()
    red = Reduce(n, at, form, src, out, bufs, False)
    keep = dk_ref.shape[0]
    piece = keep // 3
    quarter = at.quarter()
    nt = (((1,), (1,)), ((), ()))

    bit = piece // BITS

    def give_back(q, i):
        return rcopy(dm_buf.at[pl.ds(q * piece + i * bit, bit), :], dm_ref.at[pl.ds(keep + i * bit, bit), :],
                     msend.at[q, i], mrecv.at[i], at.mate(q))

    def give_bits(bits):
        @pl.when(quarter == 3)
        def _():
            for i in bits:
                for q in range(3):
                    give_back(q, i).start()

    def memory_grad():
        for i in range(3):
            rows = slice(i * piece, (i + 1) * piece)
            dm_buf[rows, :] = (lax.dot_general(dk_ref[rows, :], wk_ref[...], nt, preferred_element_type=F32)
                               + lax.dot_general(dv_ref[rows, :], wv_ref[...], nt, preferred_element_type=F32))

        @pl.when(quarter == 3)
        def _():
            dm_ref[...] = jnp.zeros_like(dm_ref)

        @pl.when(quarter < 3)
        def _():
            dm_ref[0:keep, :] = dm_buf[...]

    def small_copies(stage):
        if stage == 3:
            return [rcopy(pair.at[at.core], pair.at[at.core], ssend.at[3, 0], srecv.at[3, 0], at.other_core())]
        mine = slots.at[stage, at.coord[stage]]
        return [rcopy(mine, mine, ssend.at[stage, k - 1], srecv.at[stage, k - 1], at.along(stage, k)) for k in range(1, n)]

    red.advance(0)
    slots[0, at.coord[0]] = small[...]
    for c in small_copies(0):
        c.start()
    for stage in range(1, 8):
        red.advance(stage)
        if stage == 1:
            memory_grad()
        if stage < 7:
            give_bits([stage - 1] if stage < 5 else [2 * stage - 6, 2 * stage - 5])
        if stage < 5:
            for c in small_copies(stage - 1):
                c.wait()
            if stage < 4:
                val = functools.reduce(jnp.add, [slots[stage - 1, k] for k in range(n)])
                if stage < 3:
                    slots[stage, at.coord[stage]] = val
                else:
                    pair[at.core] = val
                for c in small_copies(stage):
                    c.start()
            else:
                small_out[...] = pair[0] + pair[1]

    @pl.when(quarter == 3)
    def _():
        for i in range(BITS):
            for q in range(3):
                give_back(q, i).wait_send()

    @pl.when(quarter < 3)
    def _():
        for i in range(BITS):
            give_back(0, i).wait_recv()


def all_reduce_late(n, cid, m_rows, stack, small, dk, dv, wk, wv):
    form = Stack(stack.shape, n)
    vm = pl.BlockSpec(memory_space=pltpu.VMEM)
    sem = pltpu.SemaphoreType.DMA
    return pl.pallas_call(
        functools.partial(reduce_kernel, n, form),
        out_shape=(jax.ShapeDtypeStruct(stack.shape, F32), jax.ShapeDtypeStruct(small.shape, F32),
                   jax.ShapeDtypeStruct((m_rows, wk.shape[0]), F32)),
        in_specs=[pl.BlockSpec(memory_space=pl.ANY)] + [vm] * 5, out_specs=(vm,) * 3, name="reduce_late",
        scratch_shapes=[pltpu.VMEM((3, n) + small.shape, F32), pltpu.VMEM((2,) + small.shape, F32),
                        sem((4, n - 1)), sem((4, n - 1)), pltpu.VMEM((dk.shape[0], wk.shape[0]), F32), sem((3, BITS)), sem((BITS,))]
        + Reduce.scratch(n, form),
        compiler_params=pltpu.CompilerParams(collective_id=cid, has_side_effects=True, vmem_limit_bytes=VMEM_LIMIT // 2),
    )(stack, small, dk, dv, wk, wv)


def solution(mesh):
    group = mesh.shape['seq']
    n = round((group // 2) ** (1 / 3))
    row_spec = P(('data', 'seq'), None)
    weight_spec = P()
    part_vec = P('data')
    part_mat = P('data', None)
    part_cube = P('data', None, None)

    def by_part(a):
        return jnp.transpose(a.reshape(a.shape[0], PARTS, TILE), (1, 0, 2))

    def by_row(a):
        return jnp.transpose(a, (1, 0, 2)).reshape(a.shape[1], PARTS * TILE)

    def device_step(dec_in, memory, mem_len, grad_out, norm_attn, wq_cross, wk_cross, wv_cross, wo_cross, norm_mlp, w_gate, w_up, w_down):
        q_rows, model_dim = dec_in.shape
        m_rows = memory.shape[0]
        heads, head_dim = wq_cross.shape[1], wq_cross.shape[2]
        wide = heads * head_dim
        wq, wk, wv = (w.reshape(model_dim, wide) for w in (wq_cross, wk_cross, wv_cross))
        wo = wo_cross.reshape(wide, model_dim)
        x_in = dec_in.astype(F32)
        normed_f, norm_pull = jax.vjp(rms_norm, x_in, norm_attn.astype(F32))
        normed = normed_f.astype(BF16)
        local_query = jnp.dot(normed, wq, preferred_element_type=F32).astype(BF16) * jnp.asarray(head_dim ** -0.5, BF16)
        out_parts, lse, q_t, kept, k_aug, v_aug, k_t = attention_fwd(
            n, 1, by_part(local_query), memory, wk, wv, mem_len)
        attended_f = by_row(out_parts)

        attended = attended_f.astype(BF16)
        hidden_f = x_in + jnp.dot(attended, wo, preferred_element_type=F32)
        hidden = hidden_f.astype(BF16)
        normed_mlp_f, mlp_norm_pull = jax.vjp(rms_norm, hidden.astype(F32), norm_mlp.astype(F32))
        normed_mlp = normed_mlp_f.astype(BF16)
        gate_pre = jnp.dot(normed_mlp, w_gate, preferred_element_type=F32)
        up_pre = jnp.dot(normed_mlp, w_up, preferred_element_type=F32)
        mlp_f, gated_pull = jax.vjp(gated_unit, gate_pre, up_pre)
        mlp_act = mlp_f.astype(BF16)

        grad_top = grad_out.astype(BF16)
        g_down = jnp.einsum('qf,qd->fd', mlp_act, grad_top, preferred_element_type=F32)
        grad_act = jnp.einsum('qd,fd->qf', grad_top, w_down, preferred_element_type=F32)
        grad_gate, grad_up = gated_pull(grad_act)
        grad_gate_b = grad_gate.astype(BF16)
        grad_up_b = grad_up.astype(BF16)
        g_gate = jnp.einsum('qd,qf->df', normed_mlp, grad_gate_b, preferred_element_type=F32)
        g_up = jnp.einsum('qd,qf->df', normed_mlp, grad_up_b, preferred_element_type=F32)
        grad_normed_mlp = (jnp.einsum('qf,df->qd', grad_gate_b, w_gate, preferred_element_type=F32)
                           + jnp.einsum('qf,df->qd', grad_up_b, w_up, preferred_element_type=F32))
        grad_hidden_norm, g_norm_mlp = mlp_norm_pull(grad_normed_mlp)
        grad_hidden = grad_out + grad_hidden_norm
        grad_hidden_b = grad_hidden.astype(BF16)
        g_wo = jnp.einsum('qe,qd->ed', attended, grad_hidden_b, preferred_element_type=F32)
        grad_attended = jnp.einsum('qd,ed->qe', grad_hidden_b, wo, preferred_element_type=F32)
        delta = jnp.sum((grad_attended * attended_f).reshape(q_rows, PARTS, 2, head_dim), axis=-1)
        delta = jnp.transpose(delta, (1, 0, 2))
        stats_in = jnp.concatenate([lse[:, :, 0:2], delta, jnp.zeros((PARTS, q_rows, TILE - 4), F32)], axis=2)

        dq_parts, dk_b, dv_b, g_gate, g_up, g_down = attention_bwd(
            n, 2, q_t, by_part(grad_attended.astype(BF16)), stats_in, k_aug, v_aug, k_t, (g_gate, g_up), (g_down,))
        grad_query_b = by_row(dq_parts).astype(BF16)

        g_wq = jnp.einsum('td,te->de', normed, grad_query_b, preferred_element_type=F32)
        grad_normed = jnp.einsum('te,de->td', grad_query_b, wq, preferred_element_type=F32)
        grad_x_norm, g_norm_attn = norm_pull(grad_normed)
        g_dec = grad_hidden + grad_x_norm
        g_wk = jnp.einsum('td,te->de', kept, dk_b, preferred_element_type=F32)
        g_wv = jnp.einsum('td,te->de', kept, dv_b, preferred_element_type=F32)
        small = jnp.concatenate([g_norm_attn[None], g_norm_mlp[None], jnp.zeros((6, model_dim), F32)], axis=0)
        late, small, g_mem = all_reduce_late(n, 3, m_rows, jnp.stack([g_wq, g_wk, g_wv, g_wo]), small, dk_b, dv_b, wk, wv)
        cube = (model_dim, heads, head_dim)
        g_wq, g_wk, g_wv = late[0], late[1], late[2]
        g_wo = late[3].reshape(heads, head_dim, model_dim)
        g_norm_attn, g_norm_mlp = small[0], small[1]
        return (g_dec, g_mem, g_norm_attn, g_wq.reshape(cube), g_wk.reshape(cube), g_wv.reshape(cube),
                g_wo, g_norm_mlp, g_gate, g_up, g_down)

    return jax.shard_map(device_step, mesh=mesh,
                         in_specs=(row_spec, row_spec, part_vec, row_spec) + (weight_spec,) * 9,
                         out_specs=(row_spec, row_spec, part_vec, part_cube, part_cube, part_cube, part_cube, part_vec, part_mat, part_mat, part_mat),
                         check_vma=False)
```

```python
import functools

import jax
import jax.numpy as jnp
from jax import lax
from jax.experimental import pallas as pl
from jax.experimental.pallas import tpu as pltpu
from jax.sharding import PartitionSpec as P

F32 = jnp.float32
BF16 = jnp.bfloat16
MESH = pl.DeviceIdType.MESH
VMEM_LIMIT = 62 * 1024 * 1024
NEG = -1e30
ORDERS = ((0, 1, 2), (2, 0, 1), (1, 2, 0))
PARTS = 3
TILE = 128
HALF = TILE // 2
ALL = slice(None)


def rms_norm(tensor, gain):
    mean_sq = jnp.mean(tensor * tensor, axis=-1, keepdims=True)
    return tensor * lax.rsqrt(mean_sq + 1e-6) * gain


def gated_unit(gate_pre, up_pre):
    return jax.nn.silu(gate_pre) * up_pre


class Place:
    def __init__(self, n):
        self.n = n
        me = lax.axis_index("seq")
        self.me = me
        self.core = lax.rem(me, 2)
        x = lax.rem(me // 2, n)
        y = lax.rem(me // (2 * n), n)
        z = me // (2 * n * n)
        self.coord = (z, y, x)
        self.stride = (2 * n * n, 2 * n, 2)

    def along(self, axis, k):
        here = self.coord[axis]
        return self.me + (lax.rem(here + k, self.n) - here) * self.stride[axis]

    def other_core(self):
        return self.me + 1 - 2 * self.core

    def quarter(self):
        return self.me // (self.n ** 3 // 2)

    def mate(self, q):
        size = self.n ** 3 // 2
        return q * size + lax.rem(self.me, size)

    def to(self, k):
        return {"seq": k}

    def barrier(self):
        sem = pltpu.get_barrier_semaphore()
        for axis in range(3):
            for k in range(1, self.n):
                pl.semaphore_signal(sem, inc=1, device_id=self.to(self.along(axis, k)), device_id_type=MESH)
        pl.semaphore_signal(sem, inc=1, device_id=self.to(self.other_core()), device_id_type=MESH)
        extra = 0
        if self.n < 4:
            for k in range(1, 4):
                pl.semaphore_signal(sem, inc=1, device_id=self.to(self.mate(lax.rem(self.quarter() + k, 4))), device_id_type=MESH)
            extra = 3
        pl.semaphore_wait(sem, 3 * (self.n - 1) + 1 + extra)


def rcopy(src, dst, send, recv, device):
    return pltpu.make_async_remote_copy(src_ref=src, dst_ref=dst, send_sem=send, recv_sem=recv,
                                        device_id={"seq": device}, device_id_type=MESH)


def lanes(start, size):
    return pl.ds(pl.multiple_of(start, TILE), size)


def rows_of(start, size):
    return pl.ds(pl.multiple_of(start, 8), size)


class Gather:
    def __init__(self, n, at, src, full, bufs):
        self.n, self.at, self.src, self.full = n, at, src, full
        self.rows, self.send, self.recv, self.csend, self.crecv = bufs
        self.copies = {}

    @staticmethod
    def scratch(n, dtype):
        sem = pltpu.SemaphoreType.DMA
        return [pltpu.VMEM((PARTS, TILE, TILE), dtype), sem((3, PARTS, n - 1)), sem((3, PARTS, n - 1)),
                sem((PARTS,)), sem((PARTS,))]

    def begin(self):
        n, at = self.n, self.at
        r = TILE // n
        for p in range(PARTS):
            a3 = ORDERS[p][2]
            mine = rows_of(at.coord[a3] * r, r)
            for k in range(1, n):
                c = rcopy(self.src.at[p], self.rows.at[p, mine, :], self.send.at[0, p, k - 1], self.recv.at[0, p, k - 1], at.along(a3, k))
                c.start()
                self.copies[0, p, k] = c
            self.rows[p, mine, :] = self.src[p]

    def turn(self):
        at, n = self.at, self.n
        for p in range(PARTS):
            a1, a2, _ = ORDERS[p]
            for k in range(1, n):
                self.copies[0, p, k].wait()
            block = self.rows[p].astype(F32).T
            base = ((at.core * n + at.coord[a1]) * n + at.coord[a2]) * TILE
            self.full[p, :, lanes(base, TILE)] = block[:self.full.shape[1]].astype(self.full.dtype)

    def place(self, stage, p, back):
        at, n = self.at, self.n
        a1, a2, _ = ORDERS[p]
        if stage == 1:
            spot = lax.rem(at.coord[a2] + n - back, n)
            return a2, lanes(((at.core * n + at.coord[a1]) * n + spot) * TILE, TILE)
        spot = lax.rem(at.coord[a1] + n - back, n)
        return a1, lanes((at.core * n + spot) * n * TILE, n * TILE)

    def spread(self, stage):
        n, at = self.n, self.at
        for p in range(PARTS):
            axis, cols = self.place(stage, p, 0)
            view = self.full.at[p, :, cols]
            for k in range(1, n):
                c = rcopy(view, view, self.send.at[stage, p, k - 1], self.recv.at[stage, p, k - 1], at.along(axis, k))
                c.start()
                self.copies[stage, p, k] = c

    def settle(self, stage):
        n = self.n
        for p in range(PARTS):
            for k in range(1, n):
                self.copies[stage, p, k].wait()

    def swap(self):
        n, at = self.n, self.at
        width = n * n * TILE
        out = []
        for p in range(PARTS):
            view = self.full.at[p, :, lanes(at.core * width, width)]
            c = rcopy(view, view, self.csend.at[p], self.crecv.at[p], at.other_core())
            c.start()
            out.append(c)
        return out


GATHER_REFS = 5


def run_gathers(gathers, hooks):
    for g in gathers:
        g.begin()
    hooks[0]()
    for g in gathers:
        g.turn()
        g.spread(1)
    hooks[1]()
    for g in gathers:
        g.settle(1)
        g.spread(2)
    hooks[2]()
    final = []
    for g in gathers:
        g.settle(2)
        final += g.swap()
    for c in final:
        c.wait()


def merge(blocks, rows_axis):
    take = (lambda b, i, j: b[i:j]) if rows_axis == 0 else (lambda b, i, j: b[:, i:j])
    outs, maxes, sums = [], [], []
    for h in range(2):
        ms = [take(b, TILE + h, TILE + h + 1) for b in blocks]
        m = functools.reduce(jnp.maximum, ms)
        ws = [jnp.exp(v - m) for v in ms]
        o = sum(take(b, HALF * h, HALF * h + HALF) * w for b, w in zip(blocks, ws))
        l = sum(take(b, TILE + 2 + h, TILE + 3 + h) * w for b, w in zip(blocks, ws))
        outs.append(o)
        maxes.append(m)
        sums.append(l)
    return outs, maxes + sums


class Scatter:
    def __init__(self, n, at, with_stats, bufs):
        self.n, self.at, self.with_stats = n, at, with_stats
        (self.far, self.near, self.buf0, self.buf1, self.acc1, self.buf2, self.acc2, self.buf3, self.pass_buf,
         self.csend, self.crecv, self.send, self.recv, self.psend, self.precv) = bufs
        self.relay = n == 4
        self.step = n * TILE

    @staticmethod
    def scratch(n, rows, wide):
        sem = pltpu.SemaphoreType.DMA
        half = n * n * TILE
        r = TILE // n
        return [
            pltpu.VMEM((PARTS, rows, half), F32), pltpu.VMEM((PARTS, rows, half), F32), pltpu.VMEM((PARTS, rows, half), F32),
            pltpu.VMEM((PARTS, n - 1, rows, n * TILE), F32), pltpu.VMEM((PARTS, rows, n * TILE), F32),
            pltpu.VMEM((PARTS, n - 1, rows, TILE), F32), pltpu.VMEM((PARTS, TILE, wide), F32),
            pltpu.VMEM((PARTS, n - 1, r, wide), F32), pltpu.VMEM((PARTS, 2, rows, n * HALF), F32),
            sem((PARTS, n)), sem((PARTS, n)), sem((3, PARTS, n - 1)), sem((3, PARTS, n - 1)), sem((PARTS, 2)), sem((PARTS, 2)),
        ]

    def visit(self, i):
        if self.relay:
            return jnp.where(i == 0, 2, jnp.where(i == 1, 3, jnp.where(i == 2, 1, 0)))
        return self.n - 1 - i

    def pass_copy(self, p, i):
        width = self.step // 2
        return rcopy(self.near.at[p, :, lanes(self.chunk(p, 2) * self.step + i * width, width)], self.pass_buf.at[p, i],
                     self.psend.at[p, i], self.precv.at[p, i], self.at.along(ORDERS[p][0], 1 + 2 * i))

    def take_over(self, p, i):
        self.pass_copy(p, i).wait_recv()
        width = self.step // 2
        for j in range(width // TILE):
            col = lanes(self.chunk(p, 1 + 2 * i) * self.step + i * width + j * TILE, TILE)
            self.combine(self.near, p, col, [self.near[p, :, col], self.pass_buf[p, i, :, j * TILE:(j + 1) * TILE]])
        self.first_copy(p, 1 + 2 * i).start()

    def chunk(self, p, k):
        return lax.rem(self.at.coord[ORDERS[p][0]] + k, self.n)

    def combine(self, dst, p, col, vals):
        if self.with_stats:
            outs, stats = merge(vals, 0)
            dst[p, 0:HALF, col] = outs[0]
            dst[p, HALF:TILE, col] = outs[1]
            dst[p, TILE:TILE + 8, col] = jnp.concatenate(stats + [jnp.zeros_like(stats[0])] * 4, axis=0)
        else:
            dst[p, :, col] = functools.reduce(jnp.add, vals)

    def core_copy(self, p, k):
        view = (p, ALL, lanes(self.chunk(p, k) * self.step, self.step))
        return rcopy(self.far.at[view], self.buf0.at[view], self.csend.at[p, k], self.crecv.at[p, k], self.at.other_core())

    def first_copy(self, p, k):
        return rcopy(self.near.at[p, :, lanes(self.chunk(p, k) * self.step, self.step)], self.buf1.at[p, k - 1],
                     self.send.at[0, p, k - 1], self.recv.at[0, p, k - 1], self.at.along(ORDERS[p][0], k))

    def far_done(self, k):
        for p in range(PARTS):
            self.core_copy(p, k).start()

    def near_done(self, k):
        for p in range(PARTS):
            self.core_copy(p, k).wait()

            def fold(j, _, p=p):
                col = lanes(self.chunk(p, k) * self.step + j * TILE, TILE)
                self.combine(self.near, p, col, [self.near[p, :, col], self.buf0[p, :, col]])
                return 0

            lax.fori_loop(0, self.n, fold, 0)

            if self.relay:
                @pl.when(k == 2)
                def _(p=p):
                    for i in range(2):
                        self.pass_copy(p, i).start()

                for i in range(2):
                    @pl.when(k == 1 + 2 * i)
                    def _(p=p, i=i):
                        self.take_over(p, i)
            else:
                @pl.when(k > 0)
                def _(p=p):
                    self.first_copy(p, k).start()

    def finish(self, o_ref, st_ref=None):
        n, at = self.n, self.at
        r = TILE // n
        copies = {}
        for p in range(PARTS):
            a1, a2, _ = ORDERS[p]
            direct = (1, 3) if self.relay else range(1, n)
            for k in direct:
                self.first_copy(p, k).wait()
            if self.relay:
                for i in range(2):
                    self.pass_copy(p, i).wait_send()
            mine = at.coord[a1] * n * TILE
            for j in range(n):
                col = slice(j * TILE, (j + 1) * TILE)
                self.combine(self.acc1, p, pl.ds(j * TILE, TILE),
                             [self.near[p, :, lanes(mine + j * TILE, TILE)]] + [self.buf1[p, k - 1, :, col] for k in direct])
            for k in range(1, n):
                there = lax.rem(at.coord[a2] + k, n)
                c = rcopy(self.acc1.at[p, :, lanes(there * TILE, TILE)], self.buf2.at[p, k - 1],
                          self.send.at[1, p, k - 1], self.recv.at[1, p, k - 1], at.along(a2, k))
                c.start()
                copies[1, p, k] = c
        for p in range(PARTS):
            _, a2, a3 = ORDERS[p]
            for k in range(1, n):
                copies[1, p, k].wait()
            blocks = [self.acc1[p, :, lanes(at.coord[a2] * TILE, TILE)]] + [self.buf2[p, k] for k in range(n - 1)]
            if self.with_stats:
                outs, stats = merge(blocks, 0)
                self.acc2[p, :, 0:TILE] = jnp.concatenate(outs, axis=0).T
                tail = jnp.concatenate(stats + [jnp.zeros((TILE - 4, TILE), F32)], axis=0)
                self.acc2[p, :, TILE:2 * TILE] = tail.T
            else:
                self.acc2[p] = functools.reduce(jnp.add, blocks).T
            for k in range(1, n):
                there = lax.rem(at.coord[a3] + k, n)
                c = rcopy(self.acc2.at[p, pl.ds(pl.multiple_of(there * r, r), r), :], self.buf3.at[p, k - 1],
                          self.send.at[2, p, k - 1], self.recv.at[2, p, k - 1], at.along(a3, k))
                c.start()
                copies[2, p, k] = c
        for p in range(PARTS):
            a3 = ORDERS[p][2]
            for k in range(1, n):
                copies[2, p, k].wait()
            blocks = [self.acc2[p, pl.ds(pl.multiple_of(at.coord[a3] * r, r), r), :]] + [self.buf3[p, k] for k in range(n - 1)]
            if self.with_stats:
                outs, (m0, m1, l0, l1) = merge(blocks, 1)
                o_ref[p] = jnp.concatenate([outs[0] / l0, outs[1] / l1], axis=1)
                col = lax.broadcasted_iota(jnp.int32, (r, TILE), 1)
                st_ref[p] = jnp.where(col == 0, m0 + jnp.log(l0), jnp.where(col == 1, m1 + jnp.log(l1), 0.0))
            else:
                o_ref[p] = functools.reduce(jnp.add, blocks)


class Wide:
    def __init__(self, shape, n):
        self.part, self.cols = shape[0] // PARTS, shape[1]
        self.r1, self.r2, self.c3 = self.part // 2, self.part // 2 // n, shape[1] // n
        self.l1, self.l2, self.l3 = (self.r1, self.cols), (self.r2, self.cols), (self.r2, self.c3)

    def row(self, p, c, a):
        return self.part * p + self.r1 * c + self.r2 * a

    def full1(self, p, c):
        return rows_of(self.part * p + self.r1 * c, self.r1), ALL

    def full2(self, p, c, a):
        return rows_of(self.row(p, c, a), self.r2), ALL

    def half2(self, p, c, a, i):
        size = self.r2 // 2
        return rows_of(self.row(p, c, a) + i * size, size), ALL

    def hin1(self, a, i):
        size = self.r2 // 2
        return rows_of(self.r2 * a + i * size, size), ALL

    def full3(self, p, c, a, b):
        return rows_of(self.row(p, c, a), self.r2), lanes(self.c3 * b, self.c3)

    def in1(self, a):
        return rows_of(self.r2 * a, self.r2), ALL

    def in2(self, b):
        return ALL, lanes(self.c3 * b, self.c3)


class Tall(Wide):
    def __init__(self, shape, n):
        super().__init__(shape, n)
        self.r3 = self.r2 // n
        self.l3 = (self.r3, self.cols)

    def full3(self, p, c, a, b):
        return rows_of(self.row(p, c, a) + self.r3 * b, self.r3), ALL

    def in2(self, b):
        return rows_of(self.r3 * b, self.r3), ALL


class Stack:
    def __init__(self, shape, n):
        w, rows, cols = shape
        self.part, self.w3 = rows // PARTS, w // n
        self.r1, self.r2 = self.part // 2, self.part // 2 // n
        self.l1, self.l2, self.l3 = (w, self.r1, cols), (w, self.r2, cols), (self.w3, self.r2, cols)

    def full1(self, p, c):
        return ALL, rows_of(self.part * p + self.r1 * c, self.r1), ALL

    def row(self, p, c, a):
        return self.part * p + self.r1 * c + self.r2 * a

    def full2(self, p, c, a):
        return ALL, rows_of(self.row(p, c, a), self.r2), ALL

    def full3(self, p, c, a, b):
        return pl.ds(self.w3 * b, self.w3), rows_of(self.row(p, c, a), self.r2), ALL

    def in1(self, a):
        return ALL, rows_of(self.r2 * a, self.r2), ALL

    def in2(self, b):
        return pl.ds(self.w3 * b, self.w3), ALL, ALL


class Reduce:
    STAGES = ("core", "pass", "first", "second", "third", "back2", "back1", "relay", "swap")

    def __init__(self, n, at, form, src, out, bufs, relay):
        self.n, self.at, self.form, self.src, self.out = n, at, form, src, out
        self.relay = relay and n == 4
        self.stages = [v for v in self.STAGES if self.relay or v not in ("pass", "relay")]
        (self.own, self.buf0, self.buf1, self.acc1, self.buf2, self.buf3, self.lsem,
         self.csend, self.crecv, self.send, self.recv) = bufs

    @staticmethod
    def scratch(n, form):
        sem = pltpu.SemaphoreType.DMA
        kinds = len(Reduce.STAGES)
        return [
            pltpu.VMEM((PARTS,) + form.l1, F32), pltpu.VMEM((PARTS,) + form.l1, F32),
            pltpu.VMEM((PARTS, n - 1) + form.l2, F32), pltpu.VMEM((PARTS,) + form.l2, F32),
            pltpu.VMEM((PARTS, n - 1) + form.l3, F32), pltpu.VMEM((PARTS, n) + form.l3, F32),
            sem((PARTS,)), sem((PARTS,)), sem((PARTS,)), sem((kinds, PARTS, n - 1)), sem((kinds, PARTS, n - 1)),
        ]

    def spots(self, p):
        return [self.at.coord[a] for a in ORDERS[p]]

    def hold(self, p, i):
        return self.buf1.at[(p, 1)].at[self.form.hin1(0, i)]

    def copies(self, stage, p):
        at, n, form = self.at, self.n, self.form
        A1, A2, A3 = self.spots(p)
        a1, a2, a3 = ORDERS[p]
        c = at.core
        if stage == "core":
            return [rcopy(self.src.at[form.full1(p, 1 - c)], self.buf0.at[p], self.csend.at[p], self.crecv.at[p], at.other_core()),
                    pltpu.make_async_copy(self.src.at[form.full1(p, c)], self.own.at[p], self.lsem.at[p])]
        kind = self.STAGES.index(stage)
        out = []

        def add(src, dst, axis, k):
            out.append(rcopy(src, dst, self.send.at[kind, p, k - 1], self.recv.at[kind, p, k - 1], at.along(axis, k)))

        if stage == "swap":
            view = self.out.at[form.full1(p, c)]
            return [rcopy(view, view, self.send.at[kind, p, 0], self.recv.at[kind, p, 0], at.other_core())]
        steps = range(1, n)
        near = (1, n - 1) if self.relay else steps
        if stage == "pass":
            for i, k in enumerate(near):
                add(self.own.at[p].at[form.hin1(lax.rem(A1 + 2, n), i)], self.hold(p, i), a1, k)
        elif stage == "first":
            for k in near:
                add(self.own.at[p].at[form.in1(lax.rem(A1 + k, n))], self.buf1.at[p, k - 1], a1, k)
        elif stage == "second":
            for k in steps:
                add(self.acc1.at[p].at[form.in2(lax.rem(A2 + k, n))], self.buf2.at[p, k - 1], a2, k)
        elif stage == "third":
            for k in steps:
                add(self.buf3.at[p, A3], self.buf3.at[p, A3], a3, k)
        elif stage == "back2":
            view = self.out.at[form.full3(p, c, A1, A2)]
            for k in steps:
                add(view, view, a2, k)
        elif stage == "back1":
            view = self.out.at[form.full2(p, c, A1)]
            for k in near:
                add(view, view, a1, k)
        else:
            for i, k in enumerate(near):
                view = self.out.at[form.half2(p, c, lax.rem(A1 + n - k, n), i)]
                add(view, view, a1, k)
        return out

    def advance(self, step):
        form, n = self.form, self.n
        stage = self.stages[step] if step < len(self.stages) else None
        before = self.stages[step - 1]
        near = (0, n - 2) if self.relay else range(n - 1)
        for p in range(PARTS):
            A1, A2, A3 = self.spots(p)
            if step:
                for c in self.copies(before, p):
                    c.wait()
            own = self.own.at[p]
            if before == "core":
                own[...] += self.buf0[p]
            elif before == "pass":
                for i, k in enumerate((1, n - 1)):
                    own[form.hin1(lax.rem(A1 + k, n), i)] += self.hold(p, i)[...]
            elif before == "first":
                self.acc1[p] = functools.reduce(jnp.add, [own[form.in1(A1)]] + [self.buf1[p, k] for k in near])
            elif before == "second":
                self.buf3[p, A3] = functools.reduce(jnp.add, [self.acc1[(p,) + form.in2(A2)]] + [self.buf2[p, k] for k in range(n - 1)])
            elif before == "third":
                self.out[form.full3(p, self.at.core, A1, A2)] = functools.reduce(jnp.add, [self.buf3[p, k] for k in range(n)])
            if stage:
                for c in self.copies(stage, p):
                    c.start()

    def finish(self, step):
        for i in range(step, len(self.stages) + 1):
            self.advance(i)


REDUCE_REFS = 11


QB = 256


def aux_rows(rows, width):
    pad = jnp.zeros((64 - len(rows), width), F32)
    return jnp.concatenate(list(rows) + [pad], axis=0).astype(BF16)


def split3(v):
    hi = v.astype(BF16).astype(F32)
    mid = (v - hi).astype(BF16).astype(F32)
    lo = (v - hi - mid).astype(BF16).astype(F32)
    return [hi, mid, lo]


def blocks_loop(n, scatter, blocks, events):
    per = n * TILE // QB
    at = scatter.at

    def body(t, _):
        u = t // per
        k = scatter.visit(u // 2)
        near = lax.rem(u, 2)
        half = jnp.where(near == 1, at.core, 1 - at.core)
        inside = [scatter.chunk(p, k) * (n * TILE) + lax.rem(t, per) * QB for p in range(PARTS)]
        srcs = [pl.ds(pl.multiple_of(half * (n * n * TILE) + i, QB), QB) for i in inside]
        blocks(srcs, near, [pl.ds(pl.multiple_of(i, QB), QB) for i in inside])
        last = lax.rem(t, per) == per - 1

        @pl.when(last & (near == 0))
        def _():
            scatter.far_done(k)

        @pl.when(last & (near == 1))
        def _():
            scatter.near_done(k)

        for when, action in events:
            @pl.when(t == when)
            def _(action=action):
                action()
        return 0

    lax.fori_loop(0, 2 * n * per, body, 0)


def put(scatter, near, p, row, col, val):
    @pl.when(near == 1)
    def _():
        scatter.near[p, row, col] = val

    @pl.when(near == 0)
    def _():
        scatter.far[p, row, col] = val


def head(j):
    return slice(HALF * j, HALF * (j + 1))


def beside(j, block, other):
    return jnp.concatenate([block, other] if j == 0 else [other, block], axis=0)


def shrink(op, v, rows):
    while v.shape[0] > rows:
        h = v.shape[0] // 2
        v = op(v[:h], v[h:])
    return v


KC = 256


def fwd_kernel(n, x_ref, mem_ref, wk_ref, wv_ref, len_ref, o_ref, st_ref, *refs):
    saved, refs = refs[:SAVED], refs[SAVED:]
    kept, refs = refs[:SAVED], refs[SAVED:]
    q_ref, keep_ref, k_ref, v_ref, kt_ref = kept
    vt_ref, s_buf, msend, mrecv, save_sem, *refs = refs
    gbufs, bufs = refs[:GATHER_REFS], refs[GATHER_REFS:]
    keys = k_ref.shape[1]
    piece = keys // 3
    kc = min(KC, piece)
    chunks = keys // kc
    at = Place(n)
    at.barrier()
    quarter = at.quarter()

    size = piece // 2

    def donate(q, i):
        return rcopy(mem_ref.at[pl.ds(keys + i * size, size), :], keep_ref.at[pl.ds(q * piece + i * size, size), :],
                     msend.at[i], mrecv.at[q, i], at.mate(3))

    def give(i):
        for q in range(3):
            @pl.when(quarter == q)
            def _(q=q):
                donate(q, i).start()

    def saves():
        return [pltpu.make_async_copy(a, b, save_sem.at[i]) for i, (a, b) in enumerate(zip(kept, saved))]

    def project():
        @pl.when(quarter < 3)
        def _():
            keep_ref[...] = mem_ref[0:keys, :]

        @pl.when(quarter == 3)
        def _():
            for q in range(3):
                for i in range(2):
                    donate(q, i).wait_recv()

        lane = lax.broadcasted_iota(jnp.int32, (piece, TILE), 1)
        spot = lax.broadcasted_iota(jnp.int32, (piece, TILE), 0)
        low = lane < HALF
        lane = lane % HALF
        flag = jnp.where((lane > 0) & (lane < 4), 1.0, 0.0)
        for i in range(3):
            rows = pl.ds(i * piece, piece)
            m = keep_ref[rows, :]
            start = jnp.where(quarter == 3, at.mate(i) * (keys + piece) + keys, at.me * (keys + piece) + i * piece)
            bias = jnp.where(start + spot < len_ref[0], 0.0, NEG)
            aux_k = jnp.where(lane == 0, bias, flag)
            for w_ref, aux, a_ref, t_ref in ((wk_ref, aux_k, k_ref, kt_ref), (wv_ref, flag, v_ref, vt_ref)):
                for p in range(PARTS):
                    b = jnp.dot(m, w_ref[:, p * TILE:(p + 1) * TILE], preferred_element_type=F32).astype(BF16).astype(F32)
                    a_ref[2 * p, rows, :] = jnp.where(low, b, aux).astype(BF16)
                    a_ref[2 * p + 1, rows, :] = jnp.where(low, aux, b).astype(BF16)
                    t_ref[p, :, rows] = b.T.astype(BF16)

    run_gathers([Gather(n, at, x_ref, q_ref, gbufs)], [functools.partial(give, 0), functools.partial(give, 1), project])
    for q in range(3):
        @pl.when(quarter == q)
        def _(q=q):
            for i in range(2):
                donate(q, i).wait_send()
    for c in saves():
        c.start()
    aux = aux_rows([jnp.ones((1, QB), F32)], QB)
    scatter = Scatter(n, at, True, bufs)

    def blocks(srcs, near, dsts):
        heads = [(p, j) for p in range(PARTS) for j in range(2)]

        def score(i, c, run):
            p, j = heads[i]
            qa = beside(j, q_ref[p, head(j), srcs[p]], aux)
            s = jnp.dot(k_ref[i, c * kc:(c + 1) * kc, :], qa, preferred_element_type=F32)
            s_buf[i % 2, c * kc:(c + 1) * kc, :] = s
            top = shrink(jnp.maximum, s, 16)
            return top if run is None else jnp.maximum(run, top)

        run = None
        for c in range(chunks):
            run = score(0, c, run)
        done = []
        for i, (p, j) in enumerate(heads):
            m = jnp.max(run, axis=0, keepdims=True)
            run, total, out = None, None, None
            for c in range(chunks):
                if i + 1 < len(heads):
                    run = score(i + 1, c, run)
                e = jnp.exp(s_buf[i % 2, c * kc:(c + 1) * kc, :] - m)
                part = shrink(jnp.add, e, 16)
                total = part if total is None else total + part
                o = jnp.dot(vt_ref[p, head(j), c * kc:(c + 1) * kc], e.astype(BF16), preferred_element_type=F32)
                out = o if out is None else out + o
            done.append((out, m, jnp.sum(total, axis=0, keepdims=True)))
            if j == 1:
                (o0, m0, l0), (o1, m1, l1) = done[-2:]
                val = jnp.concatenate([o0, o1, m0, m1, l0, l1, jnp.zeros((4, QB), F32)], axis=0)
                put(scatter, near, p, ALL, dsts[p], val)

    blocks_loop(n, scatter, blocks, [])
    scatter.finish(o_ref, st_ref)
    for c in saves():
        c.wait()


SAVED = 5


def attention_fwd(n, cid, rows, memory, wk, wv, mem_len):
    total = 2 * n * n * TILE
    r = TILE // n
    m_rows, dim = memory.shape
    keys = m_rows * 3 // 4
    vm, hbm = pl.BlockSpec(memory_space=pltpu.VMEM), pl.BlockSpec(memory_space=pl.ANY)
    sem = pltpu.SemaphoreType.DMA
    shapes = ((PARTS, TILE, total), (keys, dim), (2 * PARTS, keys, TILE), (2 * PARTS, keys, TILE), (PARTS, TILE, keys))
    scratch = [pltpu.VMEM(v, BF16) for v in shapes] + [pltpu.VMEM(shapes[-1], BF16), pltpu.VMEM((2, keys, QB), F32),
                                                       sem((2,)), sem((3, 2)), sem((SAVED,))]
    return pl.pallas_call(
        functools.partial(fwd_kernel, n),
        out_shape=(jax.ShapeDtypeStruct((PARTS, r, TILE), F32),) * 2 + tuple(jax.ShapeDtypeStruct(v, BF16) for v in shapes),
        in_specs=[vm] * 4 + [pl.BlockSpec(memory_space=pltpu.SMEM)], out_specs=(vm,) * 2 + (hbm,) * SAVED, name="attention_fwd",
        scratch_shapes=scratch + Gather.scratch(n, BF16) + Scatter.scratch(n, TILE + 8, 2 * TILE),
        compiler_params=pltpu.CompilerParams(collective_id=cid, has_side_effects=True, vmem_limit_bytes=VMEM_LIMIT),
    )(rows, memory, wk, wv, mem_len)


SCATTER_REFS = 15


def bwd_kernel(n, forms, x_ref, s_ref, q_hbm, k_hbm, v_hbm, kt_hbm, *refs):
    count = len(forms)
    grads, refs = refs[:count], refs[count:]
    dq_ref, dk_ref, dv_ref, *refs = refs
    sums, refs = refs[:count], refs[count:]
    do_ref, st_ref, dk_acc, dv_acc, q_ref, k_ref, v_ref, kt_ref, load_sem, *refs = refs
    xbufs, refs = refs[:GATHER_REFS], refs[GATHER_REFS:]
    sbufs, refs = refs[:GATHER_REFS], refs[GATHER_REFS:]
    bufs, refs = refs[:SCATTER_REFS], refs[SCATTER_REFS:]
    one = jnp.ones((1, QB), F32)
    zero = jnp.zeros((1, QB), F32)
    blank = jnp.zeros((HALF, QB), BF16)
    nt = (((1,), (1,)), ((), ()))
    at = Place(n)
    pairs = ((q_hbm, q_ref), (k_hbm, k_ref), (v_hbm, v_ref), (kt_hbm, kt_ref))
    loads = [pltpu.make_async_copy(a, b, load_sem.at[i]) for i, (a, b) in enumerate(pairs)]
    for c in loads:
        c.start()
    at.barrier()
    scatter = Scatter(n, at, False, bufs)
    reduces = [Reduce(n, at, form, grads[i], sums[i], refs[REDUCE_REFS * i:REDUCE_REFS * (i + 1)], True)
               for i, form in enumerate(forms)]

    def advance(stage):
        for red in reduces:
            red.advance(stage)

    gathers = [Gather(n, at, s_ref, st_ref, sbufs), Gather(n, at, x_ref, do_ref, xbufs)]

    def clear():
        dk_acc[...] = jnp.zeros_like(dk_acc)
        dv_acc[...] = jnp.zeros_like(dv_acc)

    run_gathers(gathers, [functools.partial(advance, 0), clear, functools.partial(advance, 1)])
    for c in loads:
        c.wait()

    def block(p, src, near, dst):
        probs, dscores, dos, qs, dqs = [], [], [], [], []
        for j in range(2):
            qh = q_ref[p, head(j), src]
            doh = do_ref[p, head(j), src]
            lse = st_ref[p, j:j + 1, src]
            delta = st_ref[p, 2 + j:3 + j, src]
            qa = beside(j, qh, aux_rows([one] + split3(-lse), QB))
            da = beside(j, doh, aux_rows([zero] + split3(-delta), QB))
            e = jnp.exp(jnp.dot(k_ref[2 * p + j], qa, preferred_element_type=F32))
            dp = jnp.dot(v_ref[2 * p + j], da, preferred_element_type=F32)
            ds = (e * dp).astype(BF16)
            probs.append(e.astype(BF16))
            dscores.append(ds)
            dos.append(beside(j, doh, blank))
            qs.append(beside(j, qh, blank))
            dqs.append(0.125 * jnp.dot(kt_ref[p, head(j), :], ds, preferred_element_type=F32))
        dv_acc[p] += (lax.dot_general(probs[0], dos[0], nt, preferred_element_type=F32)
                      + lax.dot_general(probs[1], dos[1], nt, preferred_element_type=F32))
        dk_acc[p] += (lax.dot_general(dscores[0], qs[0], nt, preferred_element_type=F32)
                      + lax.dot_general(dscores[1], qs[1], nt, preferred_element_type=F32))
        put(scatter, near, p, ALL, dst, jnp.concatenate(dqs, axis=0))

    trips = 2 * n * (n * TILE // QB)
    when = [min(w, trips - 1) for w in ((0, 3, 5, 7, 9, 12, 14) if reduces[0].relay else (3, 5, 7, 9, 13))]

    def blocks(srcs, near, dsts):
        for p in range(PARTS):
            block(p, srcs[p], near, dsts[p])

    blocks_loop(n, scatter, blocks, [(w, functools.partial(advance, i + 2)) for i, w in enumerate(when)])
    for p in range(PARTS):
        dk_ref[:, p * TILE:(p + 1) * TILE] = dk_acc[p].astype(BF16)
        dv_ref[:, p * TILE:(p + 1) * TILE] = dv_acc[p].astype(BF16)

    scatter.finish(dq_ref)
    for red in reduces:
        red.finish(2 + len(when))


def attention_bwd(n, cid, q_t, do_rows, stats_rows, k_aug, v_aug, k_t, wide, tall):
    total, keys = q_t.shape[2], k_aug.shape[1]
    r = TILE // n
    forms = [Wide(a.shape, n) for a in wide] + [Tall(a.shape, n) for a in tall]
    grads = list(wide) + list(tall)
    vm = pl.BlockSpec(memory_space=pltpu.VMEM)
    flat = jax.ShapeDtypeStruct((keys, PARTS * TILE), BF16)
    acc = pltpu.VMEM((PARTS, keys, TILE), F32)
    outs = [jax.ShapeDtypeStruct((PARTS, r, TILE), F32), flat, flat] + [jax.ShapeDtypeStruct(a.shape, F32) for a in grads]
    held = (q_t, k_aug, v_aug, k_t)
    scratch = [pltpu.VMEM((PARTS, TILE, total), BF16), pltpu.VMEM((PARTS, 8, total), F32),
               acc, acc] + [pltpu.VMEM(a.shape, BF16) for a in held] + [pltpu.SemaphoreType.DMA((len(held),))]
    scratch += Gather.scratch(n, BF16) + Gather.scratch(n, F32) + Scatter.scratch(n, TILE, TILE)
    for form in forms:
        scratch += Reduce.scratch(n, form)
    return pl.pallas_call(
        functools.partial(bwd_kernel, n, forms), out_shape=tuple(outs),
        in_specs=[vm] * 2 + [pl.BlockSpec(memory_space=pl.ANY)] * len(held + tuple(grads)), out_specs=(vm,) * len(outs), name="attention_bwd",
        scratch_shapes=scratch,
        cost_estimate=pl.CostEstimate(flops=10 * 384 * total * keys, bytes_accessed=20_000_000, transcendentals=6 * total * keys),
        compiler_params=pltpu.CompilerParams(collective_id=cid, has_side_effects=True, vmem_limit_bytes=VMEM_LIMIT),
    )(do_rows, stats_rows, *held, *grads)


BITS = 8


def reduce_kernel(n, form, src, small, dk_ref, dv_ref, wk_ref, wv_ref, out, small_out, dm_ref,
                  slots, pair, ssend, srecv, dm_buf, msend, mrecv, *bufs):
    at = Place(n)
    at.barrier()
    red = Reduce(n, at, form, src, out, bufs, False)
    keep = dk_ref.shape[0]
    piece = keep // 3
    quarter = at.quarter()
    nt = (((1,), (1,)), ((), ()))

    bit = piece // BITS

    def give_back(q, i):
        return rcopy(dm_buf.at[pl.ds(q * piece + i * bit, bit), :], dm_ref.at[pl.ds(keep + i * bit, bit), :],
                     msend.at[q, i], mrecv.at[i], at.mate(q))

    def give_bits(bits):
        @pl.when(quarter == 3)
        def _():
            for i in bits:
                for q in range(3):
                    give_back(q, i).start()

    def memory_grad():
        for i in range(3):
            rows = slice(i * piece, (i + 1) * piece)
            dm_buf[rows, :] = (lax.dot_general(dk_ref[rows, :], wk_ref[...], nt, preferred_element_type=F32)
                               + lax.dot_general(dv_ref[rows, :], wv_ref[...], nt, preferred_element_type=F32))

        @pl.when(quarter == 3)
        def _():
            dm_ref[...] = jnp.zeros_like(dm_ref)

        @pl.when(quarter < 3)
        def _():
            dm_ref[0:keep, :] = dm_buf[...]

    def small_copies(stage):
        if stage == 3:
            return [rcopy(pair.at[at.core], pair.at[at.core], ssend.at[3, 0], srecv.at[3, 0], at.other_core())]
        mine = slots.at[stage, at.coord[stage]]
        return [rcopy(mine, mine, ssend.at[stage, k - 1], srecv.at[stage, k - 1], at.along(stage, k)) for k in range(1, n)]

    red.advance(0)
    slots[0, at.coord[0]] = small[...]
    for c in small_copies(0):
        c.start()
    for stage in range(1, 8):
        red.advance(stage)
        if stage == 1:
            memory_grad()
        if stage < 7:
            give_bits([stage - 1] if stage < 5 else [2 * stage - 6, 2 * stage - 5])
        if stage < 5:
            for c in small_copies(stage - 1):
                c.wait()
            if stage < 4:
                val = functools.reduce(jnp.add, [slots[stage - 1, k] for k in range(n)])
                if stage < 3:
                    slots[stage, at.coord[stage]] = val
                else:
                    pair[at.core] = val
                for c in small_copies(stage):
                    c.start()
            else:
                small_out[...] = pair[0] + pair[1]

    @pl.when(quarter == 3)
    def _():
        for i in range(BITS):
            for q in range(3):
                give_back(q, i).wait_send()

    @pl.when(quarter < 3)
    def _():
        for i in range(BITS):
            give_back(0, i).wait_recv()


def all_reduce_late(n, cid, m_rows, stack, small, dk, dv, wk, wv):
    form = Stack(stack.shape, n)
    vm = pl.BlockSpec(memory_space=pltpu.VMEM)
    sem = pltpu.SemaphoreType.DMA
    return pl.pallas_call(
        functools.partial(reduce_kernel, n, form),
        out_shape=(jax.ShapeDtypeStruct(stack.shape, F32), jax.ShapeDtypeStruct(small.shape, F32),
                   jax.ShapeDtypeStruct((m_rows, wk.shape[0]), F32)),
        in_specs=[pl.BlockSpec(memory_space=pl.ANY)] + [vm] * 5, out_specs=(vm,) * 3, name="reduce_late",
        scratch_shapes=[pltpu.VMEM((3, n) + small.shape, F32), pltpu.VMEM((2,) + small.shape, F32),
                        sem((4, n - 1)), sem((4, n - 1)), pltpu.VMEM((dk.shape[0], wk.shape[0]), F32), sem((3, BITS)), sem((BITS,))]
        + Reduce.scratch(n, form),
        compiler_params=pltpu.CompilerParams(collective_id=cid, has_side_effects=True, vmem_limit_bytes=VMEM_LIMIT // 2),
    )(stack, small, dk, dv, wk, wv)


def solution(mesh):
    group = mesh.shape['seq']
    n = round((group // 2) ** (1 / 3))
    row_spec = P(('data', 'seq'), None)
    weight_spec = P()
    part_vec = P('data')
    part_mat = P('data', None)
    part_cube = P('data', None, None)

    def by_part(a):
        return jnp.transpose(a.reshape(a.shape[0], PARTS, TILE), (1, 0, 2))

    def by_row(a):
        return jnp.transpose(a, (1, 0, 2)).reshape(a.shape[1], PARTS * TILE)

    def device_step(dec_in, memory, mem_len, grad_out, norm_attn, wq_cross, wk_cross, wv_cross, wo_cross, norm_mlp, w_gate, w_up, w_down):
        q_rows, model_dim = dec_in.shape
        m_rows = memory.shape[0]
        heads, head_dim = wq_cross.shape[1], wq_cross.shape[2]
        wide = heads * head_dim
        wq, wk, wv = (w.reshape(model_dim, wide) for w in (wq_cross, wk_cross, wv_cross))
        wo = wo_cross.reshape(wide, model_dim)
        x_in = dec_in.astype(F32)
        normed_f, norm_pull = jax.vjp(rms_norm, x_in, norm_attn.astype(F32))
        normed = normed_f.astype(BF16)
        local_query = jnp.dot(normed, wq, preferred_element_type=F32).astype(BF16) * jnp.asarray(head_dim ** -0.5, BF16)
        out_parts, lse, q_t, kept, k_aug, v_aug, k_t = attention_fwd(
            n, 1, by_part(local_query), memory, wk, wv, mem_len)
        attended_f = by_row(out_parts)

        attended = attended_f.astype(BF16)
        hidden_f = x_in + jnp.dot(attended, wo, preferred_element_type=F32)
        hidden = hidden_f.astype(BF16)
        normed_mlp_f, mlp_norm_pull = jax.vjp(rms_norm, hidden.astype(F32), norm_mlp.astype(F32))
        normed_mlp = normed_mlp_f.astype(BF16)
        gate_pre = jnp.dot(normed_mlp, w_gate, preferred_element_type=F32)
        up_pre = jnp.dot(normed_mlp, w_up, preferred_element_type=F32)
        mlp_f, gated_pull = jax.vjp(gated_unit, gate_pre, up_pre)
        mlp_act = mlp_f.astype(BF16)

        grad_top = grad_out.astype(BF16)
        g_down = jnp.einsum('qf,qd->fd', mlp_act, grad_top, preferred_element_type=F32)
        grad_act = jnp.einsum('qd,fd->qf', grad_top, w_down, preferred_element_type=F32)
        grad_gate, grad_up = gated_pull(grad_act)
        grad_gate_b = grad_gate.astype(BF16)
        grad_up_b = grad_up.astype(BF16)
        g_gate = jnp.einsum('qd,qf->df', normed_mlp, grad_gate_b, preferred_element_type=F32)
        g_up = jnp.einsum('qd,qf->df', normed_mlp, grad_up_b, preferred_element_type=F32)
        grad_normed_mlp = (jnp.einsum('qf,df->qd', grad_gate_b, w_gate, preferred_element_type=F32)
                           + jnp.einsum('qf,df->qd', grad_up_b, w_up, preferred_element_type=F32))
        grad_hidden_norm, g_norm_mlp = mlp_norm_pull(grad_normed_mlp)
        grad_hidden = grad_out + grad_hidden_norm
        grad_hidden_b = grad_hidden.astype(BF16)
        g_wo = jnp.einsum('qe,qd->ed', attended, grad_hidden_b, preferred_element_type=F32)
        grad_attended = jnp.einsum('qd,ed->qe', grad_hidden_b, wo, preferred_element_type=F32)
        delta = jnp.sum((grad_attended * attended_f).reshape(q_rows, PARTS, 2, head_dim), axis=-1)
        delta = jnp.transpose(delta, (1, 0, 2))
        stats_in = jnp.concatenate([lse[:, :, 0:2], delta, jnp.zeros((PARTS, q_rows, TILE - 4), F32)], axis=2)

        dq_parts, dk_b, dv_b, g_gate, g_up, g_down = attention_bwd(
            n, 2, q_t, by_part(grad_attended.astype(BF16)), stats_in, k_aug, v_aug, k_t, (g_gate, g_up), (g_down,))
        grad_query_b = by_row(dq_parts).astype(BF16)

        g_wq = jnp.einsum('td,te->de', normed, grad_query_b, preferred_element_type=F32)
        grad_normed = jnp.einsum('te,de->td', grad_query_b, wq, preferred_element_type=F32)
        grad_x_norm, g_norm_attn = norm_pull(grad_normed)
        g_dec = grad_hidden + grad_x_norm
        g_wk = jnp.einsum('td,te->de', kept, dk_b, preferred_element_type=F32)
        g_wv = jnp.einsum('td,te->de', kept, dv_b, preferred_element_type=F32)
        small = jnp.concatenate([g_norm_attn[None], g_norm_mlp[None], jnp.zeros((6, model_dim), F32)], axis=0)
        late, small, g_mem = all_reduce_late(n, 3, m_rows, jnp.stack([g_wq, g_wk, g_wv, g_wo]), small, dk_b, dv_b, wk, wv)
        cube = (model_dim, heads, head_dim)
        g_wq, g_wk, g_wv = late[0], late[1], late[2]
        g_wo = late[3].reshape(heads, head_dim, model_dim)
        g_norm_attn, g_norm_mlp = small[0], small[1]
        return (g_dec, g_mem, g_norm_attn, g_wq.reshape(cube), g_wk.reshape(cube), g_wv.reshape(cube),
                g_wo, g_norm_mlp, g_gate, g_up, g_down)

    return jax.shard_map(device_step, mesh=mesh,
                         in_specs=(row_spec, row_spec, part_vec, row_spec) + (weight_spec,) * 9,
                         out_specs=(row_spec, row_spec, part_vec, part_cube, part_cube, part_cube, part_cube, part_vec, part_mat, part_mat, part_mat),
                         check_vma=False)
```
